32 devices in a mesh: fsdp: 4 (over z), ctx: 4 (over x, core), tp: 2 (over y).
Axes of the slice: x: 2, y: 2, z: 4, core: 2. Of those that a mesh axis runs over, the one named last changes fastest.
Arguments:
- hidden_in: bfloat16 [4, 2048, 2048], P('fsdp', 'ctx'), may hold values from -6 to 6
- out_grad: bfloat16 [4, 2048, 2048], P('fsdp', 'ctx'), may hold values from -6 to 6
- segment_ids: int32 [4, 2048], P('fsdp', 'ctx'), may hold values from 0 to 3, never falling along the last dimension, each value on 1 to 1024 neighbouring positions
- attn_gain: bfloat16 [2048], P('fsdp'), may hold values from 0.5 to 1.5
- w_query: bfloat16 [2048, 2048], P('fsdp', 'tp'), may hold values from -0.125 to 0.125
- w_key: bfloat16 [2048, 2048], P('fsdp', 'tp'), may hold values from -0.125 to 0.125
- w_value: bfloat16 [2048, 2048], P('fsdp', 'tp'), may hold values from -0.125 to 0.125
- w_out: bfloat16 [2048, 2048], P('tp', 'fsdp'), may hold values from -1 to 1
- mlp_gain: bfloat16 [2048], P('fsdp'), may hold values from 0.5 to 1.5
- w_gate: bfloat16 [2048, 8192], P('fsdp', 'tp'), may hold values from -0.125 to 0.125
- w_up: bfloat16 [2048, 8192], P('fsdp', 'tp'), may hold values from -0.125 to 0.125
- w_down: bfloat16 [8192, 2048], P('tp', 'fsdp'), may hold values from -0.0625 to 0.0625
Outputs:
- output: bfloat16 [4, 2048, 2048], P('fsdp', 'ctx')
- input_grad: bfloat16 [4, 2048, 2048], P('fsdp', 'ctx')
- attn_gain_grad: float32 [2048], P('fsdp')
- query_grad: float32 [2048, 2048], P('fsdp', 'tp')
- key_grad: float32 [2048, 2048], P('fsdp', 'tp')
- value_grad: float32 [2048, 2048], P('fsdp', 'tp')
- out_proj_grad: float32 [2048, 2048], P('tp', 'fsdp')
- mlp_gain_grad: float32 [2048], P('fsdp')
- gate_grad: float32 [2048, 8192], P('fsdp', 'tp')
- up_grad: float32 [2048, 8192], P('fsdp', 'tp')
- down_grad: float32 [8192, 2048], P('tp', 'fsdp')
The draws below stay inside these ranges and needn't reach their ends.
Inputs may be any that keep to these rules, and one draw needn't show every extreme that they name: `segment_ids`: along each sequence the document numbers never fall; a document is a run of 1 to 1024 tokens of one number.
All inputs are finite; a program needn't handle non-finite values.
Results may differ from the reference program's by a relative error of at most 0.024.
Values may be sent and summed in bfloat16 or wider, within the bound.
A program may use at most 384 MiB of HBM per device.

```python
import math
import jax
import jax.numpy as jnp
import numpy as np
from jax import lax

D = 2048
HEADS = 32
HEAD_DIM = 64
FF = 8192
SEQ = 2048
SEQS = 4


def block_scale(rng, dims, shards, smallest, largest):
    loudness = 1.0
    for axis_at, shards_of in shards:
        steps = jax.random.uniform(jax.random.fold_in(jax.random.fold_in(rng, 6), axis_at), (shards_of,), jnp.float32, smallest / len(shards), largest / len(shards))
        loudness = loudness * jnp.repeat(jnp.exp(steps), dims[axis_at] // shards_of).reshape((-1,) + (1,) * (len(dims) - 1 - axis_at))
    return loudness


def split_up(number_of, total, bound, slope):
    loads = [(1 << 20) // math.isqrt(grade ** slope) + 1 for grade in range(2, number_of + 1)]
    rest, counts = total - bound - (number_of - 1), [1] * (number_of - 1)
    while rest > 0:
        movable = [i for i in range(number_of - 1) if counts[i] < bound]
        pool, budget = sum([loads[i] for i in movable]), rest
        for i in movable:
            addition = min(bound - counts[i], max(1, budget * loads[i] // pool), rest)
            counts[i] = counts[i] + addition
            rest = rest - addition
    return np.array([bound] + counts)


def uneven(rng, amount, total, bound, slope):
    if amount == 2:
        one = jax.random.randint(rng, (), max(1, total - bound), min(bound, total - 1) + 1)
        return jnp.stack([one, total - one])
    tallies = jnp.asarray(split_up(amount, total, bound, slope), jnp.int32)
    couples = (amount - 1) // 2
    giver, taker = tallies[1:1 + 2 * couples:2], tallies[2:2 + 2 * couples:2]
    slack = jnp.minimum(giver - 1, bound - taker)
    shifted = jax.random.randint(jax.random.fold_in(rng, 1), (couples,), 0, 1 << 20) % (slack + 1)
    tallies = tallies.at[1:1 + 2 * couples:2].set(giver - shifted).at[2:2 + 2 * couples:2].set(taker + shifted)
    return tallies[jax.random.permutation(jax.random.fold_in(rng, 2), amount)]


def noise(rng, shape, deviation, reach, split=(), held_as=jnp.bfloat16):
    gain = block_scale(rng, shape, split, -0.22, 0.18) if split else 1.0
    values = jax.random.normal(rng, shape, jnp.float32) * deviation * gain
    return jnp.minimum(jnp.maximum(values, -reach), reach).astype(held_as)


def setup_inputs(seed: int = 0) -> dict:
    seeds = jax.random.split(jax.random.key(seed), 13)
    return {
        "hidden_in": noise(seeds[0], (SEQS, SEQ, D), 1.0, 6.0, ((0, 4), (1, 4))),
        "out_grad": noise(seeds[1], (SEQS, SEQ, D), 1.0, 6.0, ((0, 4), (1, 4))),
        "segment_ids": jax.vmap(lambda own: jnp.searchsorted(jnp.cumsum(uneven(own, max(SEQ // 512, 4), SEQ, SEQ // 2, 1)), jnp.arange(SEQ), side="right"))(jax.random.split(seeds[2], SEQS)).reshape((SEQS, SEQ)).astype(jnp.int32),
        "attn_gain": jnp.clip(1.0 + 0.1 * jax.random.normal(seeds[3], (D,), jnp.float32), 0.5, 1.5).astype(jnp.bfloat16),
        "w_query": noise(seeds[4], (D, D), D ** -0.5, 0.125, ((0, 4), (1, 2))),
        "w_key": noise(seeds[5], (D, D), D ** -0.5, 0.125, ((0, 4), (1, 2))),
        "w_value": noise(seeds[6], (D, D), D ** -0.5, 0.125, ((0, 4), (1, 2))),
        "w_out": noise(seeds[7], (D, D), (D // 64) ** -0.5, 1.0, ((0, 2), (1, 4))),
        "mlp_gain": jnp.clip(1.0 + 0.1 * jax.random.normal(seeds[8], (D,), jnp.float32), 0.5, 1.5).astype(jnp.bfloat16),
        "w_gate": noise(seeds[9], (D, FF), D ** -0.5, 0.125, ((0, 4), (1, 2))),
        "w_up": noise(seeds[10], (D, FF), D ** -0.5, 0.125, ((0, 4), (1, 2))),
        "w_down": noise(seeds[11], (FF, D), FF ** -0.5, 0.0625, ((0, 2), (1, 4))),
    }


@jax.custom_vjp
def low(v):
    return lax.optimization_barrier(v.astype(jnp.bfloat16)).astype(jnp.float32)

@jax.custom_vjp
def low_back(v):
    return v

def low_keep(v):
    return (low(v), None)

def low_pass(kept, grad):
    return (grad,)

def back_keep(v):
    return (v, None)

def back_low(kept, grad):
    return (low(grad),)
low.defvjp(low_keep, low_pass)
low_back.defvjp(back_keep, back_low)
EPS = 1e-05
ROPE_BASE = 130000.0
MASKED = -1e+30
HIGH = lax.Precision.HIGHEST

def normalize(tok_rows, gain_vec):
    return tok_rows * lax.rsqrt(lax.optimization_barrier(jnp.mean(tok_rows * tok_rows, axis=-1, keepdims=True)) + EPS) * gain_vec

def rotate(head_rows, cosine, sine_table):
    half_dim = head_rows.shape[-1] // 2
    turned = jnp.concatenate([-head_rows[..., half_dim:], head_rows[..., :half_dim]], axis=-1)
    return head_rows * cosine + turned * sine_table

def angle_tables(positions):
    exponents = jnp.arange(0, HEAD_DIM, 2).astype(jnp.float32) / HEAD_DIM
    inverse = jnp.float32(ROPE_BASE) ** (-exponents)
    angles = positions.astype(jnp.float32)[:, None] * inverse[None, :]
    angles = jnp.concatenate([angles, angles], axis=-1)
    return (jnp.cos(angles)[:, None, :], jnp.sin(angles)[:, None, :])

def matmul(first_op, second_op):
    return jnp.dot(first_op, second_op, precision=HIGH)

def attention(queries, key_rows, value_rows, segments):
    length = queries.shape[0]
    block_len = min(512, length)
    block_count = length // block_len
    score_scale = HEAD_DIM ** (-0.5)
    positions = jnp.arange(length).astype(jnp.int32)

    def one_block(block_item):
        query_block, segment_block, position_block = block_item
        scores = jnp.einsum('qhd,khd->hqk', query_block, key_rows, precision=HIGH) * score_scale
        scores = low_back(scores)
        allowed = (segment_block[:, None] == segments[None, :]) & (positions[None, :] <= position_block[:, None])
        scores = jnp.where(allowed[None], scores, MASKED)
        row_best = lax.optimization_barrier(jnp.max(scores, axis=-1, keepdims=True))
        exp_scores = jnp.exp(scores - row_best)
        probs = exp_scores / lax.optimization_barrier(jnp.sum(exp_scores, axis=-1, keepdims=True))
        return jnp.einsum('hqk,khd->qhd', low(probs), value_rows, precision=HIGH)
    block_items = (queries.reshape(block_count, block_len, HEADS, HEAD_DIM), segments.reshape(block_count, block_len), positions.reshape(block_count, block_len))
    mixed = lax.map(jax.checkpoint(one_block), block_items)
    return mixed.reshape(length, HEADS * HEAD_DIM)

def one_layer(tok_rows, segments, attn_gain, w_query, w_key, w_value, w_out, mlp_gain, w_gate, w_up, w_down):
    length = tok_rows.shape[0]
    cosine, sine_table = angle_tables(jnp.arange(length).astype(jnp.int32))

    def shaped(matrix):
        return matrix.reshape(length, HEADS, HEAD_DIM)
    attn_in = low(normalize(tok_rows, attn_gain))
    queries = low(rotate(shaped(low_back(matmul(attn_in, w_query))), cosine, sine_table))
    key_rows = low(rotate(shaped(low_back(matmul(attn_in, w_key))), cosine, sine_table))
    value_rows = shaped(low_back(low(matmul(attn_in, w_value))))
    mixed = low_back(low(attention(queries, key_rows, value_rows, segments)))
    resid = tok_rows + low_back(matmul(mixed, w_out))
    mlp_in = low(normalize(resid, mlp_gain))
    gate_act = low_back(matmul(mlp_in, w_gate))
    up_act = low_back(matmul(mlp_in, w_up))
    hidden = low(gate_act * jax.nn.sigmoid(gate_act) * up_act)
    return resid + low_back(matmul(hidden, w_down))

def reference(hidden_in, out_grad, segment_ids, attn_gain, w_query, w_key, w_value, w_out, mlp_gain, w_gate, w_up, w_down):
    weights = tuple((weight.astype(jnp.float32) for weight in (attn_gain, w_query, w_key, w_value, w_out, mlp_gain, w_gate, w_up, w_down)))

    def one_sequence(totals, seq_item):
        tok_rows, segments, grad_rows = seq_item

        def forward(rows_in, *params):
            return one_layer(rows_in, segments, *params)
        result, pull_back = jax.vjp(forward, tok_rows, *weights)
        gradients = pull_back(grad_rows)
        totals = tuple((total + grad_in for total, grad_in in zip(totals, gradients[1:])))
        return (totals, (result.astype(jnp.bfloat16), gradients[0].astype(jnp.bfloat16)))
    start_sums = tuple((jnp.zeros(weight.shape, jnp.float32) for weight in weights))
    totals, outputs = lax.scan(one_sequence, start_sums, (hidden_in.astype(jnp.float32), segment_ids.astype(jnp.int32), out_grad.astype(jnp.float32)))
    return (outputs[0], outputs[1], totals[0], totals[1], totals[2], totals[3], totals[4], totals[5], totals[6], totals[7], totals[8])
```

```python
import functools

import jax
import jax.numpy as jnp
from jax import lax
from jax.experimental import pallas as pl
from jax.experimental.pallas import tpu as pltpu
from jax.sharding import PartitionSpec as P

HEAD_DIM = 64
EPS = 1e-05
ROPE_BASE = 130000.0
MASKED = -1e30
PAIR = 2 * HEAD_DIM
BLOCK = 512
VMEM_LIMIT = 60 * 1024 * 1024


def low(values):
    return values.astype(jnp.bfloat16)


def wide(values):
    return values.astype(jnp.float32)


def product(a, b):
    return jnp.dot(a, b, preferred_element_type=jnp.float32)


def contract_rows(a, b):
    return lax.dot_general(a, b, (((0,), (0,)), ((), ())), preferred_element_type=jnp.float32)


def contract_cols(a, b):
    return lax.dot_general(a, b, (((1,), (1,)), ((), ())), preferred_element_type=jnp.float32)


def first_head():
    return lax.broadcasted_iota(jnp.int32, (1, PAIR), 1) < HEAD_DIM


def split_heads(rows):
    zero = jnp.zeros_like(rows)
    mask = first_head()
    return jnp.where(mask, rows, zero), jnp.where(mask, zero, rows)


def turn(rows, sign):
    half = HEAD_DIM // 2
    lanes = lax.broadcasted_iota(jnp.int32, (1, PAIR), 1)
    up = pltpu.roll(rows, PAIR - half, 1)
    down = pltpu.roll(rows, half, 1)
    return jnp.where(lanes % HEAD_DIM < half, -sign * up, sign * down)


def forward_kernel(info, qkv_ref, cos_ref, sin_ref, seg_col, seg_row, rot_ref, out_ref, wide_ref, lse_ref, best, total, acc):
    blocks = qkv_ref.shape[0] // BLOCK

    def prepare(n, _):
        rows = pl.ds(pl.multiple_of(n * BLOCK, BLOCK), BLOCK)
        cos, sin = cos_ref[rows, :], sin_ref[rows, :]
        q = qkv_ref[rows, :PAIR]
        k = qkv_ref[rows, PAIR : 2 * PAIR]
        rot_ref[rows, :PAIR] = low(low(q * cos + turn(q, 1.0) * sin) * jnp.bfloat16(HEAD_DIM**-0.5))
        rot_ref[rows, PAIR : 2 * PAIR] = low(k * cos + turn(k, 1.0) * sin)
        rot_ref[rows, 2 * PAIR :] = low(qkv_ref[rows, 2 * PAIR :])
        return 0

    lax.fori_loop(0, blocks, prepare, 0)

    def visit(i, j, diagonal):
        rows = pl.ds(pl.multiple_of(i * BLOCK, BLOCK), BLOCK)
        cols = pl.ds(pl.multiple_of(j * BLOCK, BLOCK), BLOCK)
        allowed = seg_col[rows, :1] == seg_row[:1, cols]
        if diagonal:
            at = lax.broadcasted_iota(jnp.int32, (BLOCK, BLOCK), 0)
            allowed = allowed & (at >= lax.broadcasted_iota(jnp.int32, (BLOCK, BLOCK), 1))
        keys = rot_ref[cols, PAIR : 2 * PAIR]
        values = rot_ref[cols, 2 * PAIR :]
        for h, q in enumerate(split_heads(rot_ref[rows, :PAIR])):
            scores = jnp.where(allowed, contract_cols(q, keys), MASKED)
            top = jnp.max(scores, axis=1, keepdims=True)
            if diagonal:
                p = jnp.exp(scores - top)
                best[h] = jnp.broadcast_to(top, (BLOCK, PAIR))
                total[h] = jnp.broadcast_to(jnp.sum(p, axis=1, keepdims=True), (BLOCK, PAIR))
                acc[h] = product(low(p), values)
            else:
                old = best[h][:, :1]
                new = jnp.maximum(old, top)
                fade = jnp.exp(old - new)
                p = jnp.exp(scores - new)
                best[h] = jnp.broadcast_to(new, (BLOCK, PAIR))
                total[h] = total[h] * fade + jnp.sum(p, axis=1, keepdims=True)
                acc[h] = acc[h] * fade + product(low(p), values)

    def one_row(i, _):
        rows = pl.ds(pl.multiple_of(i * BLOCK, BLOCK), BLOCK)
        visit(i, i, True)

        def one_col(j, _):
            @pl.when((info[0, j] < info[0, i]) & (info[2, j] >= info[1, i]))
            def _():
                visit(i, j, False)

            return 0

        lax.fori_loop(0, blocks, one_col, 0)
        mixed = jnp.where(first_head(), acc[0] / total[0], acc[1] / total[1])
        out_ref[rows, :] = low(mixed)
        wide_ref[rows, :] = mixed
        for h in range(2):
            lse_ref[0, h : h + 1, rows] = (best[h] + jnp.log(total[h])).T[:1, :]
        return 0

    lax.fori_loop(0, blocks, one_row, 0)


def backward_kernel(info, rot_ref, cos_ref, sin_ref, seg_col, seg_row, cot_ref, wide_ref, lse_ref, out_ref, delta, dq):
    blocks = rot_ref.shape[0] // BLOCK
    scale = HEAD_DIM**-0.5

    def prepare(n, _):
        rows = pl.ds(pl.multiple_of(n * BLOCK, BLOCK), BLOCK)
        terms = (wide(cot_ref[rows, :]) * wide_ref[rows, :]).T
        delta[0:1, rows] = jnp.sum(terms[:HEAD_DIM], axis=0, keepdims=True)
        delta[1:2, rows] = jnp.sum(terms[HEAD_DIM:], axis=0, keepdims=True)
        dq[rows, :] = jnp.zeros((BLOCK, PAIR), jnp.float32)
        return 0

    lax.fori_loop(0, blocks, prepare, 0)

    def visit(i, j, diagonal, dk, dv):
        rows = pl.ds(pl.multiple_of(i * BLOCK, BLOCK), BLOCK)
        cols = pl.ds(pl.multiple_of(j * BLOCK, BLOCK), BLOCK)
        allowed = seg_col[cols, :1] == seg_row[:1, rows]
        if diagonal:
            at = lax.broadcasted_iota(jnp.int32, (BLOCK, BLOCK), 0)
            allowed = allowed & (at <= lax.broadcasted_iota(jnp.int32, (BLOCK, BLOCK), 1))
        queries, cots = rot_ref[rows, :PAIR], cot_ref[rows, :]
        query_heads, cot_heads = split_heads(queries), split_heads(cots)
        key_heads = split_heads(rot_ref[cols, PAIR : 2 * PAIR])
        value_heads = split_heads(rot_ref[cols, 2 * PAIR :])
        total = dq[rows, :]
        for h in range(2):
            scores = contract_cols(key_heads[h], queries)
            probs = jnp.where(allowed, jnp.exp(scores - lse_ref[0, h : h + 1, rows]), 0.0)
            dv = dv + product(low(probs), cot_heads[h])
            prob_cot = contract_cols(value_heads[h], cots)
            score_cot = low(probs * (prob_cot - delta[h : h + 1, rows]))
            dk = dk + product(score_cot, query_heads[h])
            total = total + contract_rows(score_cot, key_heads[h])
        dq[rows, :] = total
        return dk, dv

    def unturn(grad, rows):
        return low(grad * cos_ref[rows, :] + turn(grad * sin_ref[rows, :], -1.0))

    def one_col(j, _):
        cols = pl.ds(pl.multiple_of(j * BLOCK, BLOCK), BLOCK)
        zero = jnp.zeros((BLOCK, PAIR), jnp.float32)
        dk, dv = visit(j, j, True, zero, zero)

        def one_row(i, state):
            return lax.cond(
                (info[0, j] < info[0, i]) & (info[2, j] >= info[1, i]),
                lambda state: visit(i, j, False, *state),
                lambda state: state,
                state,
            )

        dk, dv = lax.fori_loop(0, blocks, one_row, (dk, dv))
        out_ref[cols, PAIR : 2 * PAIR] = unturn(dk, cols)
        out_ref[cols, 2 * PAIR :] = low(dv)
        return 0

    lax.fori_loop(0, blocks, one_col, 0)

    def finish(n, _):
        rows = pl.ds(pl.multiple_of(n * BLOCK, BLOCK), BLOCK)
        out_ref[rows, :PAIR] = unturn(dq[rows, :] * scale, rows)
        return 0

    lax.fori_loop(0, blocks, finish, 0)


def attention_forward(info, qkv, cos, sin, seg_col, seg_row):
    tokens, width = qkv.shape
    pairs = width // (3 * PAIR)
    whole = lambda p, info: (0, 0)
    return pl.pallas_call(
        forward_kernel,
        grid_spec=pltpu.PrefetchScalarGridSpec(
            num_scalar_prefetch=1,
            grid=(pairs,),
            in_specs=[
                pl.BlockSpec((tokens, 3 * PAIR), lambda p, info: (0, p)),
                pl.BlockSpec((tokens, PAIR), whole),
                pl.BlockSpec((tokens, PAIR), whole),
                pl.BlockSpec((tokens, 1), whole),
                pl.BlockSpec((1, tokens), whole),
            ],
            out_specs=[
                pl.BlockSpec((tokens, 3 * PAIR), lambda p, info: (0, p)),
                pl.BlockSpec((tokens, PAIR), lambda p, info: (0, p)),
                pl.BlockSpec((tokens, PAIR), lambda p, info: (0, p)),
                pl.BlockSpec((1, 2, tokens), lambda p, info: (p, 0, 0)),
            ],
            scratch_shapes=[
                pltpu.VMEM((2, BLOCK, PAIR), jnp.float32),
                pltpu.VMEM((2, BLOCK, PAIR), jnp.float32),
                pltpu.VMEM((2, BLOCK, PAIR), jnp.float32),
            ],
        ),
        out_shape=[
            jax.ShapeDtypeStruct((tokens, width), jnp.bfloat16),
            jax.ShapeDtypeStruct((tokens, pairs * PAIR), jnp.bfloat16),
            jax.ShapeDtypeStruct((tokens, pairs * PAIR), jnp.float32),
            jax.ShapeDtypeStruct((pairs, 2, tokens), jnp.float32),
        ],
        compiler_params=pltpu.CompilerParams(vmem_limit_bytes=VMEM_LIMIT),
        cost_estimate=pl.CostEstimate(flops=tokens * tokens * width, bytes_accessed=10 * tokens * width, transcendentals=tokens * tokens * 2 * pairs),
    )(info, qkv, cos, sin, seg_col, seg_row)


def attention_backward(info, rot, cos, sin, seg_col, seg_row, cot, mixed, lse):
    tokens, width = rot.shape
    pairs = width // (3 * PAIR)
    whole = lambda p, info: (0, 0)
    return pl.pallas_call(
        backward_kernel,
        grid_spec=pltpu.PrefetchScalarGridSpec(
            num_scalar_prefetch=1,
            grid=(pairs,),
            in_specs=[
                pl.BlockSpec((tokens, 3 * PAIR), lambda p, info: (0, p)),
                pl.BlockSpec((tokens, PAIR), whole),
                pl.BlockSpec((tokens, PAIR), whole),
                pl.BlockSpec((tokens, 1), whole),
                pl.BlockSpec((1, tokens), whole),
                pl.BlockSpec((tokens, PAIR), lambda p, info: (0, p)),
                pl.BlockSpec((tokens, PAIR), lambda p, info: (0, p)),
                pl.BlockSpec((1, 2, tokens), lambda p, info: (p, 0, 0)),
            ],
            out_specs=pl.BlockSpec((tokens, 3 * PAIR), lambda p, info: (0, p)),
            scratch_shapes=[
                pltpu.VMEM((2, tokens), jnp.float32),
                pltpu.VMEM((tokens, PAIR), jnp.float32),
            ],
        ),
        out_shape=jax.ShapeDtypeStruct((tokens, width), jnp.bfloat16),
        compiler_params=pltpu.CompilerParams(vmem_limit_bytes=VMEM_LIMIT),
        cost_estimate=pl.CostEstimate(flops=3 * tokens * tokens * width, bytes_accessed=10 * tokens * width, transcendentals=tokens * tokens * 2 * pairs),
    )(info, rot, cos, sin, seg_col, seg_row, cot, mixed, lse)


def swap(values, axis, mask):
    size = lax.axis_size(axis)
    return lax.ppermute(values, axis, [(i, i ^ mask) for i in range(size)])


def masks(size):
    return [1 << n for n in reversed(range(size.bit_length() - 1))]


def offsets(size):
    held = [0]
    for mask in masks(size):
        held = held + [at ^ mask for at in held]
    return held


def gather_rows(rows, axis):
    for mask in masks(lax.axis_size(axis)):
        rows = jnp.concatenate([rows, swap(rows, axis, mask)], axis=0)
    return rows


def scatter_rows(make, count, axis):
    todo = list(reversed(masks(lax.axis_size(axis))))
    half = count // 2
    there = swap(low(make(half, count)), axis, todo[0])
    rows = make(0, half) + wide(there)
    for mask in todo[1:]:
        half = rows.shape[0] // 2
        rows = rows[:half] + wide(swap(low(rows[half:]), axis, mask))
    return rows


def scatter_both(make, count):
    rows = scatter_rows(make, count, "ctx")
    size = lax.axis_size("tp")
    me = lax.axis_index("tp")
    for mask in masks(size):
        half = rows.shape[0] // 2
        upper = (me & mask) != 0
        mine = jnp.where(upper, rows[half:], rows[:half])
        other = jnp.where(upper, rows[:half], rows[half:])
        rows = mine + wide(swap(low(other), "tp", mask))
    return rows


def join_tp(rows):
    size = lax.axis_size("tp")
    me = lax.axis_index("tp")
    for mask in reversed(masks(size)):
        upper = (me & mask) != 0
        other = swap(rows, "tp", mask)
        rows = jnp.where(upper, jnp.concatenate([other, rows], 0), jnp.concatenate([rows, other], 0))
    return rows


def own_part(rows):
    size = lax.axis_size("tp")
    count = rows.shape[0] // size
    return lax.dynamic_slice_in_dim(rows, lax.axis_index("tp") * count, count, 0)


def local(
    hidden_in,
    out_grad,
    segment_ids,
    attn_gain,
    w_query,
    w_key,
    w_value,
    w_out,
    mlp_gain,
    w_gate,
    w_up,
    w_down,
):
    group = lax.axis_size("ctx")
    me = lax.axis_index("ctx")
    local_rows = hidden_in.shape[1]
    tokens = local_rows * group
    head_cols = w_query.shape[1] // group
    pairs = head_cols // PAIR
    ff_cols = w_gate.shape[1] // group

    def my_cols(weight, count):
        return lax.dynamic_slice_in_dim(weight, me * count, count, 1)

    def my_rows(weight, count):
        return lax.dynamic_slice_in_dim(weight, me * count, count, 0)

    def interleave(q, k, v):
        parts = []
        for p in range(pairs):
            parts += [x[:, p * PAIR : (p + 1) * PAIR] for x in (q, k, v)]
        return jnp.concatenate(parts, axis=1)

    def gather(weight, axis):
        return lax.all_gather(weight, "fsdp", axis=axis, tiled=True)

    w_qkv = gather(interleave(*[my_cols(w, head_cols) for w in (w_query, w_key, w_value)]), 0)
    gains = gather(jnp.stack([attn_gain, mlp_gain]), 1)
    full_out = gather(my_rows(w_out, head_cols), 1)
    full_gate = gather(my_cols(w_gate, ff_cols), 0)
    full_up = gather(my_cols(w_up, ff_cols), 0)
    full_down = gather(my_rows(w_down, ff_cols), 1)

    gain_one, gain_two = wide(gains[0]), wide(gains[1])

    rows_in = wide(hidden_in[0])
    r1 = lax.rsqrt(jnp.mean(rows_in * rows_in, axis=-1, keepdims=True) + EPS)
    attn_in = gather_rows(low(rows_in * r1 * gain_one), "ctx")
    segments = gather_rows(segment_ids[0], "ctx")
    branch_cot = gather_rows(out_grad[0], "ctx")

    firsts = jnp.stack([(me ^ at) * local_rows for at in offsets(group)])
    positions = (firsts[:, None] + jnp.arange(local_rows, dtype=jnp.int32)[None, :]).reshape(tokens)
    exponents = jnp.arange(0, HEAD_DIM, 2).astype(jnp.float32) / HEAD_DIM
    inverse = jnp.float32(ROPE_BASE) ** (-exponents)
    angles = positions.astype(jnp.float32)[:, None] * inverse[None, :]
    cos = jnp.tile(jnp.cos(angles), (1, 4))
    sin = jnp.tile(jnp.sin(angles), (1, 4))
    info = jnp.stack([positions[::BLOCK], segments[::BLOCK], segments[BLOCK - 1 :: BLOCK]])
    seg_col, seg_row = segments[:, None], segments[None, :]

    qkv = product(attn_in, w_qkv)
    rot, mixed, mixed_wide, lse = attention_forward(info, qkv, cos, sin, seg_col, seg_row)

    part = scatter_both(lambda lo, hi: product(mixed[lo:hi], full_out), tokens)
    own_in = wide(own_part(hidden_in[0]))
    resid = own_in + part
    r2 = lax.rsqrt(jnp.mean(resid * resid, axis=-1, keepdims=True) + EPS)
    mlp_in = gather_rows(join_tp(low(resid * r2 * gain_two)), "ctx")
    gate_act = product(mlp_in, full_gate)
    up_act = product(mlp_in, full_up)
    sigmoid = jax.nn.sigmoid(gate_act)
    hidden = low(gate_act * sigmoid * up_act)
    down_part = low(contract_rows(hidden, branch_cot))

    hidden_cot = contract_cols(branch_cot, full_down)
    gate_cot = low(hidden_cot * up_act * sigmoid * (1.0 + gate_act * (1.0 - sigmoid)))
    up_cot = low(hidden_cot * gate_act * sigmoid)
    mlp_in_cot = scatter_both(
        lambda lo, hi: contract_cols(gate_cot[lo:hi], full_gate) + contract_cols(up_cot[lo:hi], full_up), tokens
    )
    gate_part = low(contract_rows(mlp_in, gate_cot))
    up_part = low(contract_rows(mlp_in, up_cot))

    out_sum = scatter_both(lambda lo, hi: product(hidden[lo:hi], full_down), tokens)
    output = join_tp(low(resid + out_sum))

    own_grad = wide(own_part(out_grad[0]))
    scaled = mlp_in_cot * gain_two
    gain_two_part = jnp.sum(mlp_in_cot * (resid * r2), axis=0)
    resid_cot = own_grad + r2 * scaled - resid * (r2 * r2 * r2) * jnp.mean(resid * scaled, axis=-1, keepdims=True)
    attn_cot = gather_rows(join_tp(low(resid_cot)), "ctx")
    mixed_cot = low(contract_cols(attn_cot, full_out))
    out_part = low(contract_rows(mixed, attn_cot))
    cots = attention_backward(info, rot, cos, sin, seg_col, seg_row, mixed_cot, mixed_wide, lse)
    qkv_part = low(contract_rows(attn_in, cots))
    attn_in_cot = scatter_both(lambda lo, hi: contract_cols(cots[lo:hi], w_qkv), tokens)
    own_r1 = own_part(r1)
    scaled = attn_in_cot * gain_one
    gain_one_part = jnp.sum(attn_in_cot * (own_in * own_r1), axis=0)
    input_grad = resid_cot + own_r1 * scaled - own_in * (own_r1 * own_r1 * own_r1) * jnp.mean(own_in * scaled, axis=-1, keepdims=True)
    input_grad = join_tp(low(input_grad))

    def settle(part, axis):
        return lax.psum_scatter(part, "fsdp", scatter_dimension=axis, tiled=True)

    def spread(block, axis):
        return wide(lax.all_gather(block, "ctx", axis=axis, tiled=True))

    down_own = settle(down_part, 1)
    gate_own = settle(gate_part, 0)
    up_own = settle(up_part, 0)
    out_own = settle(out_part, 1)
    qkv_own = settle(qkv_part, 0)

    def pick(n):
        return jnp.concatenate([qkv_own[:, (3 * p + n) * PAIR : (3 * p + n + 1) * PAIR] for p in range(pairs)], axis=1)

    gain_sums = lax.psum(jnp.stack([gain_one_part, gain_two_part]), ("fsdp", "ctx", "tp"))
    gain_sums = lax.dynamic_slice_in_dim(gain_sums, lax.axis_index("fsdp") * attn_gain.shape[0], attn_gain.shape[0], 1)
    return (
        output[None],
        input_grad[None],
        gain_sums[0],
        spread(pick(0), 1),
        spread(pick(1), 1),
        spread(pick(2), 1),
        spread(out_own, 0),
        gain_sums[1],
        spread(gate_own, 1),
        spread(up_own, 1),
        spread(down_own, 0),
    )


def solution(mesh):
    weight, gain = P("fsdp", "tp"), P("fsdp")
    rows = P("fsdp", "ctx", None)
    in_specs = (rows, rows, P("fsdp", "ctx"), gain, weight, weight, weight, P("tp", "fsdp"), gain, weight, weight, P("tp", "fsdp"))
    out_specs = (rows, rows, gain, weight, weight, weight, P("tp", "fsdp"), gain, weight, weight, P("tp", "fsdp"))
    return jax.shard_map(local, mesh=mesh, in_specs=in_specs, out_specs=out_specs, check_vma=False)
```

```python
import functools

import jax
import jax.numpy as jnp
from jax import lax
from jax.experimental import pallas as pl
from jax.experimental.pallas import tpu as pltpu
from jax.sharding import PartitionSpec as P

HEAD_DIM = 64
EPS = 1e-05
ROPE_BASE = 130000.0
MASKED = -1e30
PAIR = 2 * HEAD_DIM
BLOCK = 512
VMEM_LIMIT = 60 * 1024 * 1024


def low(values):
    return values.astype(jnp.bfloat16)


def wide(values):
    return values.astype(jnp.float32)


def product(a, b):
    return jnp.dot(a, b, preferred_element_type=jnp.float32)


def contract_rows(a, b):
    return lax.dot_general(a, b, (((0,), (0,)), ((), ())), preferred_element_type=jnp.float32)


def contract_cols(a, b):
    return lax.dot_general(a, b, (((1,), (1,)), ((), ())), preferred_element_type=jnp.float32)


def first_head():
    return lax.broadcasted_iota(jnp.int32, (1, PAIR), 1) < HEAD_DIM


def split_heads(rows):
    zero = jnp.zeros_like(rows)
    mask = first_head()
    return jnp.where(mask, rows, zero), jnp.where(mask, zero, rows)


def turn(rows, sign):
    half = HEAD_DIM // 2
    lanes = lax.broadcasted_iota(jnp.int32, (1, PAIR), 1)
    up = pltpu.roll(rows, PAIR - half, 1)
    down = pltpu.roll(rows, half, 1)
    return jnp.where(lanes % HEAD_DIM < half, -sign * up, sign * down)


def forward_kernel(info, qkv_ref, cos_ref, sin_ref, seg_col, seg_row, rot_ref, out_ref, wide_ref, lse_ref, best, total, acc):
    blocks = qkv_ref.shape[0] // BLOCK

    def prepare(n, _):
        rows = pl.ds(pl.multiple_of(n * BLOCK, BLOCK), BLOCK)
        cos, sin = cos_ref[rows, :], sin_ref[rows, :]
        q = qkv_ref[rows, :PAIR]
        k = qkv_ref[rows, PAIR : 2 * PAIR]
        rot_ref[rows, :PAIR] = low(low(q * cos + turn(q, 1.0) * sin) * jnp.bfloat16(HEAD_DIM**-0.5))
        rot_ref[rows, PAIR : 2 * PAIR] = low(k * cos + turn(k, 1.0) * sin)
        rot_ref[rows, 2 * PAIR :] = low(qkv_ref[rows, 2 * PAIR :])
        return 0

    lax.fori_loop(0, blocks, prepare, 0)

    def visit(i, j, diagonal):
        rows = pl.ds(pl.multiple_of(i * BLOCK, BLOCK), BLOCK)
        cols = pl.ds(pl.multiple_of(j * BLOCK, BLOCK), BLOCK)
        allowed = seg_col[rows, :1] == seg_row[:1, cols]
        if diagonal:
            at = lax.broadcasted_iota(jnp.int32, (BLOCK, BLOCK), 0)
            allowed = allowed & (at >= lax.broadcasted_iota(jnp.int32, (BLOCK, BLOCK), 1))
        keys = rot_ref[cols, PAIR : 2 * PAIR]
        values = rot_ref[cols, 2 * PAIR :]
        for h, q in enumerate(split_heads(rot_ref[rows, :PAIR])):
            scores = jnp.where(allowed, contract_cols(q, keys), MASKED)
            top = jnp.max(scores, axis=1, keepdims=True)
            if diagonal:
                p = jnp.exp(scores - top)
                best[h] = jnp.broadcast_to(top, (BLOCK, PAIR))
                total[h] = jnp.broadcast_to(jnp.sum(p, axis=1, keepdims=True), (BLOCK, PAIR))
                acc[h] = product(low(p), values)
            else:
                old = best[h][:, :1]
                new = jnp.maximum(old, top)
                fade = jnp.exp(old - new)
                p = jnp.exp(scores - new)
                best[h] = jnp.broadcast_to(new, (BLOCK, PAIR))
                total[h] = total[h] * fade + jnp.sum(p, axis=1, keepdims=True)
                acc[h] = acc[h] * fade + product(low(p), values)

    def one_row(i, _):
        rows = pl.ds(pl.multiple_of(i * BLOCK, BLOCK), BLOCK)
        visit(i, i, True)

        def one_col(j, _):
            @pl.when((info[0, j] < info[0, i]) & (info[2, j] >= info[1, i]))
            def _():
                visit(i, j, False)

            return 0

        lax.fori_loop(0, blocks, one_col, 0)
        mixed = jnp.where(first_head(), acc[0] / total[0], acc[1] / total[1])
        out_ref[rows, :] = low(mixed)
        wide_ref[rows, :] = mixed
        for h in range(2):
            lse_ref[0, h : h + 1, rows] = (best[h] + jnp.log(total[h])).T[:1, :]
        return 0

    lax.fori_loop(0, blocks, one_row, 0)


def backward_kernel(info, rot_ref, cos_ref, sin_ref, seg_col, seg_row, cot_ref, wide_ref, lse_ref, out_ref, delta, dq):
    blocks = rot_ref.shape[0] // BLOCK
    scale = HEAD_DIM**-0.5

    def prepare(n, _):
        rows = pl.ds(pl.multiple_of(n * BLOCK, BLOCK), BLOCK)
        terms = (wide(cot_ref[rows, :]) * wide_ref[rows, :]).T
        delta[0:1, rows] = jnp.sum(terms[:HEAD_DIM], axis=0, keepdims=True)
        delta[1:2, rows] = jnp.sum(terms[HEAD_DIM:], axis=0, keepdims=True)
        dq[rows, :] = jnp.zeros((BLOCK, PAIR), jnp.float32)
        return 0

    lax.fori_loop(0, blocks, prepare, 0)

    def visit(i, j, diagonal, dk, dv):
        rows = pl.ds(pl.multiple_of(i * BLOCK, BLOCK), BLOCK)
        cols = pl.ds(pl.multiple_of(j * BLOCK, BLOCK), BLOCK)
        allowed = seg_col[cols, :1] == seg_row[:1, rows]
        if diagonal:
            at = lax.broadcasted_iota(jnp.int32, (BLOCK, BLOCK), 0)
            allowed = allowed & (at <= lax.broadcasted_iota(jnp.int32, (BLOCK, BLOCK), 1))
        queries, cots = rot_ref[rows, :PAIR], cot_ref[rows, :]
        query_heads, cot_heads = split_heads(queries), split_heads(cots)
        key_heads = split_heads(rot_ref[cols, PAIR : 2 * PAIR])
        value_heads = split_heads(rot_ref[cols, 2 * PAIR :])
        total = dq[rows, :]
        for h in range(2):
            scores = contract_cols(key_heads[h], queries)
            probs = jnp.where(allowed, jnp.exp(scores - lse_ref[0, h : h + 1, rows]), 0.0)
            dv = dv + product(low(probs), cot_heads[h])
            prob_cot = contract_cols(value_heads[h], cots)
            score_cot = low(probs * (prob_cot - delta[h : h + 1, rows]))
            dk = dk + product(score_cot, query_heads[h])
            total = total + contract_rows(score_cot, key_heads[h])
        dq[rows, :] = total
        return dk, dv

    def unturn(grad, rows):
        return low(grad * cos_ref[rows, :] + turn(grad * sin_ref[rows, :], -1.0))

    def one_col(j, _):
        cols = pl.ds(pl.multiple_of(j * BLOCK, BLOCK), BLOCK)
        zero = jnp.zeros((BLOCK, PAIR), jnp.float32)
        dk, dv = visit(j, j, True, zero, zero)

        def one_row(i, state):
            return lax.cond(
                (info[0, j] < info[0, i]) & (info[2, j] >= info[1, i]),
                lambda state: visit(i, j, False, *state),
                lambda state: state,
                state,
            )

        dk, dv = lax.fori_loop(0, blocks, one_row, (dk, dv))
        out_ref[cols, PAIR : 2 * PAIR] = unturn(dk, cols)
        out_ref[cols, 2 * PAIR :] = low(dv)
        return 0

    lax.fori_loop(0, blocks, one_col, 0)

    def finish(n, _):
        rows = pl.ds(pl.multiple_of(n * BLOCK, BLOCK), BLOCK)
        out_ref[rows, :PAIR] = unturn(dq[rows, :] * scale, rows)
        return 0

    lax.fori_loop(0, blocks, finish, 0)


def attention_forward(info, qkv, cos, sin, seg_col, seg_row):
    tokens, width = qkv.shape
    pairs = width // (3 * PAIR)
    whole = lambda p, info: (0, 0)
    return pl.pallas_call(
        forward_kernel,
        grid_spec=pltpu.PrefetchScalarGridSpec(
            num_scalar_prefetch=1,
            grid=(pairs,),
            in_specs=[
                pl.BlockSpec((tokens, 3 * PAIR), lambda p, info: (0, p)),
                pl.BlockSpec((tokens, PAIR), whole),
                pl.BlockSpec((tokens, PAIR), whole),
                pl.BlockSpec((tokens, 1), whole),
                pl.BlockSpec((1, tokens), whole),
            ],
            out_specs=[
                pl.BlockSpec((tokens, 3 * PAIR), lambda p, info: (0, p)),
                pl.BlockSpec((tokens, PAIR), lambda p, info: (0, p)),
                pl.BlockSpec((tokens, PAIR), lambda p, info: (0, p)),
                pl.BlockSpec((1, 2, tokens), lambda p, info: (p, 0, 0)),
            ],
            scratch_shapes=[
                pltpu.VMEM((2, BLOCK, PAIR), jnp.float32),
                pltpu.VMEM((2, BLOCK, PAIR), jnp.float32),
                pltpu.VMEM((2, BLOCK, PAIR), jnp.float32),
            ],
        ),
        out_shape=[
            jax.ShapeDtypeStruct((tokens, width), jnp.bfloat16),
            jax.ShapeDtypeStruct((tokens, pairs * PAIR), jnp.bfloat16),
            jax.ShapeDtypeStruct((tokens, pairs * PAIR), jnp.float32),
            jax.ShapeDtypeStruct((pairs, 2, tokens), jnp.float32),
        ],
        compiler_params=pltpu.CompilerParams(vmem_limit_bytes=VMEM_LIMIT),
        cost_estimate=pl.CostEstimate(flops=tokens * tokens * width, bytes_accessed=10 * tokens * width, transcendentals=tokens * tokens * 2 * pairs),
    )(info, qkv, cos, sin, seg_col, seg_row)


def attention_backward(info, rot, cos, sin, seg_col, seg_row, cot, mixed, lse):
    tokens, width = rot.shape
    pairs = width // (3 * PAIR)
    whole = lambda p, info: (0, 0)
    return pl.pallas_call(
        backward_kernel,
        grid_spec=pltpu.PrefetchScalarGridSpec(
            num_scalar_prefetch=1,
            grid=(pairs,),
            in_specs=[
                pl.BlockSpec((tokens, 3 * PAIR), lambda p, info: (0, p)),
                pl.BlockSpec((tokens, PAIR), whole),
                pl.BlockSpec((tokens, PAIR), whole),
                pl.BlockSpec((tokens, 1), whole),
                pl.BlockSpec((1, tokens), whole),
                pl.BlockSpec((tokens, PAIR), lambda p, info: (0, p)),
                pl.BlockSpec((tokens, PAIR), lambda p, info: (0, p)),
                pl.BlockSpec((1, 2, tokens), lambda p, info: (p, 0, 0)),
            ],
            out_specs=pl.BlockSpec((tokens, 3 * PAIR), lambda p, info: (0, p)),
            scratch_shapes=[
                pltpu.VMEM((2, tokens), jnp.float32),
                pltpu.VMEM((tokens, PAIR), jnp.float32),
            ],
        ),
        out_shape=jax.ShapeDtypeStruct((tokens, width), jnp.bfloat16),
        compiler_params=pltpu.CompilerParams(vmem_limit_bytes=VMEM_LIMIT),
        cost_estimate=pl.CostEstimate(flops=3 * tokens * tokens * width, bytes_accessed=10 * tokens * width, transcendentals=tokens * tokens * 2 * pairs),
    )(info, rot, cos, sin, seg_col, seg_row, cot, mixed, lse)


def swap(values, axis, mask):
    size = lax.axis_size(axis)
    return lax.ppermute(values, axis, [(i, i ^ mask) for i in range(size)])


def masks(size):
    return [1 << n for n in reversed(range(size.bit_length() - 1))]


def offsets(size):
    held = [0]
    for mask in masks(size):
        held = held + [at ^ mask for at in held]
    return held


def gather_rows(rows, axis):
    for mask in masks(lax.axis_size(axis)):
        rows = jnp.concatenate([rows, swap(rows, axis, mask)], axis=0)
    return rows


def scatter_rows(make, count, axis):
    todo = list(reversed(masks(lax.axis_size(axis))))
    half = count // 2
    there = swap(low(make(half, count)), axis, todo[0])
    rows = make(0, half) + wide(there)
    for mask in todo[1:]:
        half = rows.shape[0] // 2
        rows = rows[:half] + wide(swap(low(rows[half:]), axis, mask))
    return rows


def scatter_both(make, count):
    rows = scatter_rows(make, count, "ctx")
    size = lax.axis_size("tp")
    me = lax.axis_index("tp")
    for mask in masks(size):
        half = rows.shape[0] // 2
        upper = (me & mask) != 0
        mine = jnp.where(upper, rows[half:], rows[:half])
        other = jnp.where(upper, rows[:half], rows[half:])
        rows = mine + wide(swap(low(other), "tp", mask))
    return rows


def join_tp(rows):
    size = lax.axis_size("tp")
    me = lax.axis_index("tp")
    for mask in reversed(masks(size)):
        upper = (me & mask) != 0
        other = swap(rows, "tp", mask)
        rows = jnp.where(upper, jnp.concatenate([other, rows], 0), jnp.concatenate([rows, other], 0))
    return rows


def own_part(rows):
    size = lax.axis_size("tp")
    count = rows.shape[0] // size
    return lax.dynamic_slice_in_dim(rows, lax.axis_index("tp") * count, count, 0)


def place_kernel(at, *refs):
    out = refs[-1]
    for n, piece in enumerate(refs[:-1]):

        @pl.when(pl.program_id(0) == n)
        def _():
            out[...] = wide(piece[...])


def spread(block, axis):
    pieces = [block]
    for mask in masks(lax.axis_size("ctx")):
        there = swap(jnp.stack(pieces) if len(pieces) > 1 else pieces[0], "ctx", mask)
        pieces = pieces + ([there[n] for n in range(len(pieces))] if len(pieces) > 1 else [there])
    at = lax.axis_index("ctx") ^ jnp.array(offsets(lax.axis_size("ctx")), jnp.int32)
    shape = list(block.shape)
    shape[axis] *= len(pieces)
    return pl.pallas_call(
        place_kernel,
        grid_spec=pltpu.PrefetchScalarGridSpec(
            num_scalar_prefetch=1,
            grid=(len(pieces),),
            in_specs=[pl.BlockSpec(block.shape, lambda n, at: (0, 0))] * len(pieces),
            out_specs=pl.BlockSpec(block.shape, lambda n, at: (at[n], 0) if axis == 0 else (0, at[n])),
        ),
        out_shape=jax.ShapeDtypeStruct(shape, jnp.float32),
        compiler_params=pltpu.CompilerParams(vmem_limit_bytes=VMEM_LIMIT),
        cost_estimate=pl.CostEstimate(flops=0, bytes_accessed=6 * block.size * len(pieces), transcendentals=0),
    )(at, *pieces)


MESH = pl.DeviceIdType.MESH
TILE = 512


def fits_kernels():
    return lax.axis_size("ctx") == 4 and lax.axis_size("tp") == 2


class Place:
    def __init__(self):
        me = lax.axis_index("ctx")
        x, core = me // 2, me % 2
        self.tp = lax.axis_index("tp")
        self.x = {"ctx": (1 - x) * 2 + core}
        self.core = {"ctx": x * 2 + 1 - core}
        self.cross = {"ctx": (1 - x) * 2 + 1 - core}
        self.y = {"tp": 1 - self.tp}

    def others(self, axis):
        size, me = lax.axis_size(axis), lax.axis_index(axis)
        return [{axis: (me + n) % size} for n in range(1, size)]


def meet(devices):
    barrier = pltpu.get_barrier_semaphore()
    for device in devices:
        pl.semaphore_signal(barrier, inc=1, device_id=device, device_id_type=MESH)
    pl.semaphore_wait(barrier, len(devices))


class Links:
    def __init__(self, send, recv):
        self.send, self.recv, self.count, self.sent = send, recv, 0, []

    def copy(self, src, dst, device, at=None):
        n = self.count
        self.count += 1
        made = pltpu.make_async_remote_copy(src, dst, self.send.at[n], self.recv.at[n], device_id=device, device_id_type=MESH)
        self.sent.append(made)
        return made

    def drain(self):
        for made in self.sent:
            made.wait_send()


def aligned(start, count):
    return pl.ds(pl.multiple_of(start, count), count)


def start_kernel(hidden, grads, segs, gains, attn_in, cot, segs_out, gains_out, hbuf, nbuf, gbuf, gain_row, send, recv, local_sem):
    place, links = Place(), Links(send, recv)
    rows = hidden.shape[0]
    half, quarter = rows // 2, rows // 4
    z = lax.axis_index("fsdp")
    near = [place.x, place.core, place.cross, place.y]
    far = place.others("fsdp")
    meet(near + far)

    def span(block, part, chunk=None):
        if chunk is None:
            return aligned(block * rows + part * half, half)
        return aligned(block * rows + part * half + chunk * quarter, quarter)

    mine, other = place.tp, 1 - place.tp
    tiny = [links.copy(gains, gains_out.at[z], device) for device in far]
    tiny_segs = [links.copy(segs, segs_out.at[n + 1], device) for n, device in enumerate(near[:3])]
    for made in tiny + tiny_segs:
        made.start()
    over_x = {}
    for name, src, dst in (("h", hidden, hbuf), ("g", grads, gbuf)):
        for q in range(2):
            over_x[name, q] = links.copy(src.at[span(0, mine, q)], dst.at[span(1, mine, q)], place.x)
    over_core = {name: links.copy(src, dst.at[aligned(2 * rows, rows)], place.core) for name, src, dst in (("h", hidden, hbuf), ("g", grads, gbuf))}
    for key in (("h", 0), ("h", 1)):
        over_x[key].start()
    over_core["h"].start()
    for key in (("g", 0), ("g", 1)):
        over_x[key].start()
    over_core["g"].start()
    kept = []

    def keep(src, dst):
        made = pltpu.make_async_copy(src, dst, local_sem.at[len(kept)])
        made.start()
        kept.append(made)

    keep(grads, cot.at[aligned(0, rows)])
    gains_out[z] = gains[...]
    segs_out[0] = segs[...]
    for made in tiny:
        made.wait_recv()
    lanes = 128
    groups = gains.shape[0] // 2
    for device in range(gains_out.shape[0]):
        for row in range(groups):
            gain_row[:, pl.ds((device * groups + row) * lanes, lanes)] = gains_out[device, row : row + 1, :]

    def normalize(src, at, block, count):
        def some(n, _):
            there = aligned(at + n * 64, 64)
            values = wide(src[there, :])
            scale = lax.rsqrt(jnp.mean(values * values, axis=1, keepdims=True) + EPS)
            nbuf[aligned(block + n * 64, 64), :] = low(values * scale * gain_row[...])
            return 0

        lax.fori_loop(0, count // 64, some, 0)
        keep(nbuf.at[pl.ds(block, count)], attn_in.at[pl.ds(block, count)])

    normalize(hidden, 0, 0, rows)
    over_y, across, last = {}, {}, {}

    def pass_on(name, buf):
        for q in range(2):
            over_x[name, q].wait_recv()
            over_y[name, q] = links.copy(buf.at[span(1, mine, q)], buf.at[span(1, mine, q)], place.y)
            across[name, q] = links.copy(buf.at[span(1, mine, q)], buf.at[span(3, mine, q)], place.core)
            over_y[name, q].start()
            across[name, q].start()

    def finish(name, buf):
        for q in range(2):
            over_y[name, q].wait_recv()
            last[name, q] = links.copy(buf.at[span(1, other, q)], buf.at[span(3, other, q)], place.core)
            last[name, q].start()

    pass_on("h", hbuf)
    over_core["h"].wait_recv()
    normalize(hbuf, 2 * rows, 2 * rows, rows)
    finish("h", hbuf)
    normalize(hbuf, rows, rows, rows)
    pass_on("g", gbuf)
    for q in range(2):
        across["h", q].wait_recv()
        last["h", q].wait_recv()
    normalize(hbuf, 3 * rows, 3 * rows, rows)
    over_core["g"].wait_recv()
    keep(gbuf.at[aligned(2 * rows, rows)], cot.at[aligned(2 * rows, rows)])
    finish("g", gbuf)
    keep(gbuf.at[aligned(rows, rows)], cot.at[aligned(rows, rows)])
    for q in range(2):
        across["g", q].wait_recv()
        last["g", q].wait_recv()
    keep(gbuf.at[aligned(3 * rows, rows)], cot.at[aligned(3 * rows, rows)])
    for made in tiny_segs:
        made.wait_recv()
    links.drain()
    for made in kept:
        made.wait()


def start_exchange(hidden, grads, segments, attn_gain, mlp_gain):
    rows, width = hidden.shape
    fsdp = lax.axis_size("fsdp")
    segs = jnp.concatenate([segments.reshape(-1, 128), jnp.zeros((8 - rows // 128, 128), jnp.int32)], axis=0)
    gains = wide(jnp.concatenate([attn_gain, mlp_gain])).reshape(-1, 128)
    vmem = pl.BlockSpec(memory_space=pltpu.VMEM)
    hbm = pl.BlockSpec(memory_space=pl.ANY)
    tokens = 4 * rows
    attn_in, cot, segs, gains = pl.pallas_call(
        start_kernel,
        in_specs=[vmem] * 4,
        out_specs=[hbm, hbm, vmem, vmem],
        out_shape=[
            jax.ShapeDtypeStruct((tokens, width), jnp.bfloat16),
            jax.ShapeDtypeStruct((tokens, width), jnp.bfloat16),
            jax.ShapeDtypeStruct((4, 8, 128), jnp.int32),
            jax.ShapeDtypeStruct((fsdp,) + gains.shape, jnp.float32),
        ],
        scratch_shapes=[
            pltpu.VMEM((tokens, width), jnp.bfloat16),
            pltpu.VMEM((tokens, width), jnp.bfloat16),
            pltpu.VMEM((tokens, width), jnp.bfloat16),
            pltpu.VMEM((1, width), jnp.float32),
            pltpu.SemaphoreType.DMA((fsdp + 32,)),
            pltpu.SemaphoreType.DMA((fsdp + 32,)),
            pltpu.SemaphoreType.DMA((8,)),
        ],
        compiler_params=pltpu.CompilerParams(collective_id=0, has_side_effects=True, vmem_limit_bytes=VMEM_LIMIT),
        cost_estimate=pl.CostEstimate(flops=0, bytes_accessed=200_000_000, transcendentals=0),
    )(hidden, grads, segs, gains)
    segs = segs[:, : rows // 128].reshape(tokens)
    gains = jnp.transpose(gains.reshape(fsdp, 2, -1), (1, 0, 2)).reshape(2, width)
    return attn_in, cot, segs, gains


def scatter_scratch(rows, width):
    part, half = rows // 8, width // 2
    return [
        pltpu.VMEM((4, part, width), jnp.bfloat16),
        pltpu.VMEM((4, part, width), jnp.bfloat16),
        pltpu.VMEM((6, part, half), jnp.bfloat16),
        pltpu.VMEM((6, part, half), jnp.bfloat16),
        pltpu.VMEM((2, part, half), jnp.float32),
        pltpu.VMEM((part, width), jnp.float32),
        pltpu.SemaphoreType.DMA((10,)),
        pltpu.SemaphoreType.DMA((10,)),
    ]


class Scatter:
    def __init__(self, place, make, count, refs):
        self.place, self.make = place, make
        self.hi, self.core_in, self.out, self.come, self.wait, self.total, send, recv = refs
        self.part = count // 8
        self.half = self.total.shape[1] // 2
        links = Links(send, recv)
        self.links = links
        self.core = [links.copy(self.hi.at[n], self.core_in.at[n], place.core) for n in range(4)]
        self.send = [links.copy(self.out.at[n], self.come.at[n], place.x if n in (0, 1, 5) else place.y) for n in range(6)]

    def rows(self, n):
        tp = self.place.tp
        part = (1 - tp) + (n % 2) * (2 * tp - 1)
        return ((1 - n // 2) * 2 + part) * self.part

    def columns(self, side, each):
        tiles = self.half // TILE

        def one(n, _):
            each(aligned(side * self.half + n * TILE, TILE), aligned(n * TILE, TILE))
            return 0

        lax.fori_loop(0, tiles, one, 0)

    def to_core(self):
        for n in range(4):
            rows = aligned(4 * self.part + self.rows(n), self.part)
            for side in range(2):

                def each(cols, _):
                    self.hi[n, :, cols] = low(self.make(rows, cols))

                self.columns(side, each)
            self.core[n].start()

    def to_links(self):
        away = {(0, 0): 0, (1, 0): 1, (0, 1): 2, (2, 1): 3}
        for n in range(4):
            rows = aligned(self.rows(n), self.part)
            self.core[n].wait_recv()
            for side in range(2):

                def each(cols, at):
                    value = self.make(rows, cols) + wide(self.core_in[n, :, cols])
                    if (n, side) in away:
                        self.out[away[n, side], :, at] = low(value)
                    elif n == 3:
                        self.total[:, cols] = value
                    else:
                        self.wait[side, :, at] = value

                self.columns(side, each)
                if (n, side) in away:
                    self.send[away[n, side]].start()

    def turn(self):
        for side, came, goes in ((1, 2, 5), (0, 0, 4)):
            self.send[came].wait_recv()

            def each(_, at):
                self.out[goes, :, at] = low(self.wait[side, :, at] + wide(self.come[came, :, at]))

            self.columns(side, each)
            self.send[goes].start()

    def finish(self):
        for n in (1, 3, 4, 5):
            self.send[n].wait_recv()
        left, right = pl.ds(0, self.half), pl.ds(self.half, self.half)
        self.total[:, left] = self.total[:, left] + wide(self.come[1]) + wide(self.come[4])
        self.total[:, right] = self.total[:, right] + wide(self.come[3]) + wide(self.come[5])
        self.links.drain()


def gather_plane(place, links, mine, full, part):
    half = mine.shape[1] // 2
    left, right = pl.ds(0, half), pl.ds(half, half)
    own, other = place.tp, 1 - place.tp

    def rows(block, tp):
        return aligned((block * 2 + tp) * part, part)

    y_left = links.copy(mine.at[:, left], full.at[rows(0, own), left], place.y)
    x_right = links.copy(mine.at[:, right], full.at[rows(1, own), right], place.x)
    y_right = links.copy(mine.at[:, right], full.at[rows(0, own), right], place.y)
    x_left = links.copy(mine.at[:, left], full.at[rows(1, own), left], place.x)
    core = [links.copy(mine, full.at[rows(2, own)], place.core)]
    for made in (y_left, x_right, y_right, x_left, core[0]):
        made.start()
    waits = []

    def relay(come, block, tp, cols, onward=None):
        come.wait_recv()
        here = full.at[rows(block, tp), cols]
        if onward == "x":
            made = links.copy(here, full.at[rows(1, tp), cols], place.x)
        elif onward == "y":
            made = links.copy(here, full.at[rows(block, tp), cols], place.y)
        if onward:
            made.start()
        over = links.copy(here, full.at[rows(block + 2, tp), cols], place.core)
        over.start()
        core.append(over)
        return made if onward else None

    far_left = relay(y_left, 0, other, left, "x")
    far_right = relay(x_right, 1, own, right, "y")
    relay(y_right, 0, other, right)
    relay(x_left, 1, own, left)
    relay(far_left, 1, other, left)
    relay(far_right, 1, other, right)
    for made in core:
        made.wait_recv()


def own_rows_of(ref, place, part):
    return ref[aligned(place.tp * part, part), :]


def forward_mid_kernel(mixed, weight, hidden, gain, full, resid_out, mine, *refs):
    place = Place()
    scatter_refs, (send, recv, local_sem) = refs[:-3], refs[-3:]
    count = mixed.shape[0]
    part = count // 8
    meet([place.x, place.core, place.y])
    scatter = Scatter(place, lambda rows, cols: product(mixed[rows, :], weight[:, cols]), count, scatter_refs)
    scatter.to_core()
    scatter.to_links()
    scatter.turn()
    scatter.finish()
    step = 64

    def some(n, _):
        rows = aligned(n * step, step)
        values = wide(hidden[aligned(place.tp * part + n * step, step), :]) + scatter.total[rows, :]
        resid_out[rows, :] = values
        scale = lax.rsqrt(jnp.mean(values * values, axis=1, keepdims=True) + EPS)
        mine[rows, :] = low(values * scale * gain[...])
        return 0

    lax.fori_loop(0, part // step, some, 0)
    stay = pltpu.make_async_copy(mine, full.at[aligned(place.tp * part, part)], local_sem)
    stay.start()
    links = Links(send, recv)
    gather_plane(place, links, mine, full, part)
    links.drain()
    stay.wait()


def mid_scratch(count, width):
    return [pltpu.VMEM((count // 8, width), jnp.bfloat16)] + scatter_scratch(count, width) + [
        pltpu.SemaphoreType.DMA((16,)),
        pltpu.SemaphoreType.DMA((16,)),
        pltpu.SemaphoreType.DMA,
    ]


def forward_mid(mixed, weight, hidden, gain):
    count, width = mixed.shape[0], weight.shape[1]
    vmem = pl.BlockSpec(memory_space=pltpu.VMEM)
    return pl.pallas_call(
        forward_mid_kernel,
        in_specs=[vmem] * 4,
        out_specs=[pl.BlockSpec(memory_space=pl.ANY), vmem],
        out_shape=[jax.ShapeDtypeStruct((count, width), jnp.bfloat16), jax.ShapeDtypeStruct((count // 8, width), jnp.float32)],
        scratch_shapes=mid_scratch(count, width),
        compiler_params=pltpu.CompilerParams(collective_id=1, has_side_effects=True, vmem_limit_bytes=VMEM_LIMIT),
        cost_estimate=pl.CostEstimate(flops=0, bytes_accessed=300_000_000, transcendentals=0),
    )(mixed, weight, hidden, gain[None, :])


def norm_back(values, scale, gain, cot):
    scaled = cot * gain
    lean = jnp.mean(values * scaled, axis=1, keepdims=True)
    return scale * scaled - values * (scale * scale * scale) * lean, cot * (values * scale)


def backward_mid_kernel(gate_cot, gate, up_cot, up, resid, grads, gain, full, cot_out, gain_out, mine, *refs):
    place = Place()
    scatter_refs, (send, recv, local_sem) = refs[:-3], refs[-3:]
    count = gate_cot.shape[0]
    part = count // 8
    meet([place.x, place.core, place.y])

    def make(rows, cols):
        return contract_cols(gate_cot[rows, :], gate[cols, :]) + contract_cols(up_cot[rows, :], up[cols, :])

    scatter = Scatter(place, make, count, scatter_refs)
    scatter.to_core()
    scatter.to_links()
    scatter.turn()
    scatter.finish()
    step = 32

    def some(n, sums):
        rows = aligned(n * step, step)
        values = resid[rows, :]
        scale = lax.rsqrt(jnp.mean(values * values, axis=1, keepdims=True) + EPS)
        back, terms = norm_back(values, scale, gain[...], scatter.total[rows, :])
        cot = wide(grads[aligned(place.tp * part + n * step, step), :]) + back
        cot_out[rows, :] = cot
        mine[rows, :] = low(cot)
        return sums + jnp.sum(terms, axis=0, keepdims=True)

    gain_out[...] = lax.fori_loop(0, part // step, some, jnp.zeros(gain.shape, jnp.float32))
    stay = pltpu.make_async_copy(mine, full.at[aligned(place.tp * part, part)], local_sem)
    stay.start()
    links = Links(send, recv)
    gather_plane(place, links, mine, full, part)
    links.drain()
    stay.wait()


def backward_mid(gate_cot, gate, up_cot, up, resid, grads, gain):
    count, width = gate_cot.shape[0], gate.shape[0]
    vmem = pl.BlockSpec(memory_space=pltpu.VMEM)
    return pl.pallas_call(
        backward_mid_kernel,
        in_specs=[vmem] * 7,
        out_specs=[pl.BlockSpec(memory_space=pl.ANY), vmem, vmem],
        out_shape=[
            jax.ShapeDtypeStruct((count, width), jnp.bfloat16),
            jax.ShapeDtypeStruct((count // 8, width), jnp.float32),
            jax.ShapeDtypeStruct((1, width), jnp.float32),
        ],
        scratch_shapes=mid_scratch(count, width),
        compiler_params=pltpu.CompilerParams(collective_id=2, has_side_effects=True, vmem_limit_bytes=VMEM_LIMIT),
        cost_estimate=pl.CostEstimate(flops=0, bytes_accessed=300_000_000, transcendentals=0),
    )(gate_cot, gate, up_cot, up, resid, grads, gain[None, :])


def finish_kernel(hidden_act, down, cots, w_qkv, resid, resid_cot, hidden, gain, gain_two, out, grad_out, gains_out, mine, sums, come, *refs):
    place = Place()
    (send, recv, local_sem), refs = refs[-3:], refs[:-3]
    count = hidden_act.shape[0]
    part = count // 8
    z = [{"fsdp": device} for device in ()]
    meet([place.x, place.core, place.y] + place.others("fsdp"))
    each = len(refs) // 2
    first = Scatter(place, lambda rows, cols: contract_cols(cots[rows, :], w_qkv[cols, :]), count, refs[:each])
    second = Scatter(place, lambda rows, cols: product(hidden_act[rows, :], down[:, cols]), count, refs[each:])
    links = Links(send, recv)
    own = aligned(place.tp * part, part)
    first.to_core()
    first.to_links()
    second.to_core()
    first.turn()
    second.to_links()
    first.finish()
    step = 32

    def some(n, total):
        rows = aligned(n * step, step)
        values = wide(hidden[aligned(place.tp * part + n * step, step), :])
        scale = lax.rsqrt(jnp.mean(values * values, axis=1, keepdims=True) + EPS)
        back, terms = norm_back(values, scale, gain[...], first.total[rows, :])
        mine[0, rows, :] = low(resid_cot[rows, :] + back)
        return total + jnp.sum(terms, axis=0, keepdims=True)

    sums[0, 0:1, :] = lax.fori_loop(0, part // step, some, jnp.zeros(gain.shape, jnp.float32))
    sums[0, 1:2, :] = gain_two[...]
    grad_y = links.copy(mine.at[0], grad_out.at[own], place.y)
    grad_y.start()
    stay = [pltpu.make_async_copy(mine.at[0], grad_out.at[own], local_sem.at[0])]
    stay[0].start()
    second.turn()
    near = [place.x, place.core, place.y]
    for n, device in enumerate(near):
        made = links.copy(sums.at[n], come.at[n], device)
        made.start()
        made.wait_recv()
        sums[n + 1] = sums[n] + come[n]
    at = len(near)
    far = [links.copy(sums.at[at], come.at[at + n], device) for n, device in enumerate(place.others("fsdp"))]
    for made in far:
        made.start()
    second.finish()

    def more(n, _):
        rows = aligned(n * step, step)
        mine[1, rows, :] = low(resid[rows, :] + second.total[rows, :])
        return 0

    lax.fori_loop(0, part // step, more, 0)
    out_y = links.copy(mine.at[1], out.at[own], place.y)
    out_y.start()
    stay.append(pltpu.make_async_copy(mine.at[1], out.at[own], local_sem.at[1]))
    stay[1].start()
    total = sums[at]
    for n, made in enumerate(far):
        made.wait_recv()
        total = total + come[at + n]
    gains_out[...] = total
    grad_y.wait_recv()
    out_y.wait_recv()
    links.drain()
    for made in stay:
        made.wait()


def finish_exchange(hidden_act, down, cots, w_qkv, resid, resid_cot, hidden, gain, gain_two):
    count, width = hidden_act.shape[0], down.shape[1]
    fsdp = lax.axis_size("fsdp")
    vmem = pl.BlockSpec(memory_space=pltpu.VMEM)
    hbm = pl.BlockSpec(memory_space=pl.ANY)
    return pl.pallas_call(
        finish_kernel,
        in_specs=[vmem] * 9,
        out_specs=[hbm, hbm, vmem],
        out_shape=[
            jax.ShapeDtypeStruct((count // 4, width), jnp.bfloat16),
            jax.ShapeDtypeStruct((count // 4, width), jnp.bfloat16),
            jax.ShapeDtypeStruct((2, width), jnp.float32),
        ],
        scratch_shapes=[
            pltpu.VMEM((2, count // 8, width), jnp.bfloat16),
            pltpu.VMEM((4, 2, width), jnp.float32),
            pltpu.VMEM((2 + fsdp, 2, width), jnp.float32),
        ]
        + scatter_scratch(count, width) * 2
        + [pltpu.SemaphoreType.DMA((5 + fsdp,)), pltpu.SemaphoreType.DMA((5 + fsdp,)), pltpu.SemaphoreType.DMA((2,))],
        compiler_params=pltpu.CompilerParams(collective_id=3, has_side_effects=True, vmem_limit_bytes=VMEM_LIMIT),
        cost_estimate=pl.CostEstimate(flops=0, bytes_accessed=300_000_000, transcendentals=0),
    )(hidden_act, down, cots, w_qkv, resid, resid_cot, hidden, gain[None, :], gain_two)


def local(
    hidden_in,
    out_grad,
    segment_ids,
    attn_gain,
    w_query,
    w_key,
    w_value,
    w_out,
    mlp_gain,
    w_gate,
    w_up,
    w_down,
):
    group = lax.axis_size("ctx")
    me = lax.axis_index("ctx")
    local_rows = hidden_in.shape[1]
    tokens = local_rows * group
    head_cols = w_query.shape[1] // group
    pairs = head_cols // PAIR
    ff_cols = w_gate.shape[1] // group

    def my_cols(weight, count):
        return lax.dynamic_slice_in_dim(weight, me * count, count, 1)

    def my_rows(weight, count):
        return lax.dynamic_slice_in_dim(weight, me * count, count, 0)

    def interleave(q, k, v):
        parts = []
        for p in range(pairs):
            parts += [x[:, p * PAIR : (p + 1) * PAIR] for x in (q, k, v)]
        return jnp.concatenate(parts, axis=1)

    def gather(weight, axis):
        return lax.all_gather(weight, "fsdp", axis=axis, tiled=True)

    w_qkv = gather(interleave(*[my_cols(w, head_cols) for w in (w_query, w_key, w_value)]), 0)
    full_out = gather(my_rows(w_out, head_cols), 1)
    full_gate = gather(my_cols(w_gate, ff_cols), 0)
    full_up = gather(my_cols(w_up, ff_cols), 0)
    full_down = gather(my_rows(w_down, ff_cols), 1)


    kernels = fits_kernels()
    if kernels:
        attn_in, branch_cot, segments, gains = start_exchange(hidden_in[0], out_grad[0], segment_ids[0], attn_gain, mlp_gain)
        gain_one, gain_two = gains[0], gains[1]
    else:
        gains = wide(gather(jnp.stack([attn_gain, mlp_gain]), 1))
        gain_one, gain_two = gains[0], gains[1]
        rows_in = wide(hidden_in[0])
        r1 = lax.rsqrt(jnp.mean(rows_in * rows_in, axis=-1, keepdims=True) + EPS)
        attn_in = gather_rows(low(rows_in * r1 * gain_one), "ctx")
        segments = gather_rows(segment_ids[0], "ctx")
        branch_cot = gather_rows(out_grad[0], "ctx")

    firsts = jnp.stack([(me ^ at) * local_rows for at in offsets(group)])
    positions = (firsts[:, None] + jnp.arange(local_rows, dtype=jnp.int32)[None, :]).reshape(tokens)
    exponents = jnp.arange(0, HEAD_DIM, 2).astype(jnp.float32) / HEAD_DIM
    inverse = jnp.float32(ROPE_BASE) ** (-exponents)
    angles = positions.astype(jnp.float32)[:, None] * inverse[None, :]
    cos = jnp.tile(jnp.cos(angles), (1, 4))
    sin = jnp.tile(jnp.sin(angles), (1, 4))
    info = jnp.stack([positions[::BLOCK], segments[::BLOCK], segments[BLOCK - 1 :: BLOCK]])
    seg_col, seg_row = segments[:, None], segments[None, :]

    qkv = product(attn_in, w_qkv)
    rot, mixed, mixed_wide, lse = attention_forward(info, qkv, cos, sin, seg_col, seg_row)

    own_in = wide(own_part(hidden_in[0]))
    if kernels:
        mlp_in, resid = forward_mid(mixed, full_out, hidden_in[0], gain_two)
    else:
        part = scatter_both(lambda lo, hi: product(mixed[lo:hi], full_out), tokens)
        resid = own_in + part
        r2 = lax.rsqrt(jnp.mean(resid * resid, axis=-1, keepdims=True) + EPS)
        mlp_in = gather_rows(join_tp(low(resid * r2 * gain_two)), "ctx")
    gate_act = product(mlp_in, full_gate)
    up_act = product(mlp_in, full_up)
    sigmoid = jax.nn.sigmoid(gate_act)
    hidden = low(gate_act * sigmoid * up_act)
    down_part = low(contract_rows(hidden, branch_cot))

    hidden_cot = contract_cols(branch_cot, full_down)
    gate_cot = low(hidden_cot * up_act * sigmoid * (1.0 + gate_act * (1.0 - sigmoid)))
    up_cot = low(hidden_cot * gate_act * sigmoid)
    gate_part = low(contract_rows(mlp_in, gate_cot))
    up_part = low(contract_rows(mlp_in, up_cot))
    if kernels:
        gate_cot, up_cot, gate_part, up_part, down_part = lax.optimization_barrier((gate_cot, up_cot, gate_part, up_part, down_part))
        attn_cot, resid_cot, gain_two_part = backward_mid(gate_cot, full_gate, up_cot, full_up, resid, out_grad[0], gain_two)
    else:
        mlp_in_cot = scatter_both(
            lambda lo, hi: contract_cols(gate_cot[lo:hi], full_gate) + contract_cols(up_cot[lo:hi], full_up), tokens
        )
        back, terms = norm_back(resid, r2, gain_two, mlp_in_cot)
        gain_two_part = jnp.sum(terms, axis=0, keepdims=True)
        resid_cot = wide(own_part(out_grad[0])) + back
        attn_cot = gather_rows(join_tp(low(resid_cot)), "ctx")
    mixed_cot = low(contract_cols(attn_cot, full_out))
    out_part = low(contract_rows(mixed, attn_cot))
    cots = attention_backward(info, rot, cos, sin, seg_col, seg_row, mixed_cot, mixed_wide, lse)
    qkv_part = low(contract_rows(attn_in, cots))
    if kernels:
        cots, qkv_part, out_part = lax.optimization_barrier((cots, qkv_part, out_part))
        output, input_grad, gain_sums = finish_exchange(hidden, full_down, cots, w_qkv, resid, resid_cot, hidden_in[0], gain_one, gain_two_part)
    else:
        out_sum = scatter_both(lambda lo, hi: product(hidden[lo:hi], full_down), tokens)
        output = join_tp(low(resid + out_sum))
        attn_in_cot = scatter_both(lambda lo, hi: contract_cols(cots[lo:hi], w_qkv), tokens)
        back, terms = norm_back(own_in, own_part(r1), gain_one, attn_in_cot)
        input_grad = join_tp(low(resid_cot + back))
        gain_sums = lax.psum(jnp.concatenate([jnp.sum(terms, axis=0, keepdims=True), gain_two_part]), ("fsdp", "ctx", "tp"))

    def settle(part, axis):
        return lax.psum_scatter(part, "fsdp", scatter_dimension=axis, tiled=True)

    down_grad = spread(settle(down_part, 1), 0)
    gate_grad = spread(settle(gate_part, 0), 1)
    up_grad = spread(settle(up_part, 0), 1)
    out_proj_grad = spread(settle(out_part, 1), 0)
    qkv_own = settle(qkv_part, 0)

    def pick(n):
        return jnp.concatenate([qkv_own[:, (3 * p + n) * PAIR : (3 * p + n + 1) * PAIR] for p in range(pairs)], axis=1)

    gain_sums = lax.dynamic_slice_in_dim(gain_sums, lax.axis_index("fsdp") * attn_gain.shape[0], attn_gain.shape[0], 1)
    return (
        output[None],
        input_grad[None],
        gain_sums[0],
        spread(pick(0), 1),
        spread(pick(1), 1),
        spread(pick(2), 1),
        out_proj_grad,
        gain_sums[1],
        gate_grad,
        up_grad,
        down_grad,
    )


def solution(mesh):
    weight, gain = P("fsdp", "tp"), P("fsdp")
    rows = P("fsdp", "ctx", None)
    in_specs = (rows, rows, P("fsdp", "ctx"), gain, weight, weight, weight, P("tp", "fsdp"), gain, weight, weight, P("tp", "fsdp"))
    out_specs = (rows, rows, gain, weight, weight, weight, P("tp", "fsdp"), gain, weight, weight, P("tp", "fsdp"))
    return jax.shard_map(local, mesh=mesh, in_specs=in_specs, out_specs=out_specs, check_vma=False)
```

```python
import math

import jax
import jax.numpy as jnp
from jax import lax
from jax.experimental import pallas as pl
from jax.experimental.pallas import tpu as pltpu
from jax.sharding import PartitionSpec as P

HEAD_DIM = 64
EPS = 1e-05
ROPE_BASE = 130000.0
MASKED = -1e30
PAIR = 2 * HEAD_DIM
BLOCK = 512
VMEM_LIMIT = 60 * 1024 * 1024


def low(values):
    return values.astype(jnp.bfloat16)


def wide(values):
    return values.astype(jnp.float32)


def product(a, b):
    return jnp.dot(a, b, preferred_element_type=jnp.float32)


def contract_rows(a, b):
    return lax.dot_general(a, b, (((0,), (0,)), ((), ())), preferred_element_type=jnp.float32)


def contract_cols(a, b):
    return lax.dot_general(a, b, (((1,), (1,)), ((), ())), preferred_element_type=jnp.float32)


def first_head():
    return lax.broadcasted_iota(jnp.int32, (1, PAIR), 1) < HEAD_DIM


def split_heads(rows):
    zero = jnp.zeros_like(rows)
    mask = first_head()
    return jnp.where(mask, rows, zero), jnp.where(mask, zero, rows)


def turn(rows, sign):
    half = HEAD_DIM // 2
    lanes = lax.broadcasted_iota(jnp.int32, (1, PAIR), 1)
    up = pltpu.roll(rows, PAIR - half, 1)
    down = pltpu.roll(rows, half, 1)
    return jnp.where(lanes % HEAD_DIM < half, -sign * up, sign * down)


def forward_kernel(info, qkv_ref, cos_ref, sin_ref, seg_col, seg_row, rot_ref, out_ref, wide_ref, lse_ref, best, total, acc):
    blocks = qkv_ref.shape[0] // BLOCK

    def prepare(n, _):
        rows = pl.ds(pl.multiple_of(n * BLOCK, BLOCK), BLOCK)
        cos, sin = cos_ref[rows, :], sin_ref[rows, :]
        q = qkv_ref[rows, :PAIR]
        k = qkv_ref[rows, PAIR : 2 * PAIR]
        rot_ref[rows, :PAIR] = low(low(q * cos + turn(q, 1.0) * sin) * jnp.bfloat16(HEAD_DIM**-0.5))
        rot_ref[rows, PAIR : 2 * PAIR] = low(k * cos + turn(k, 1.0) * sin)
        rot_ref[rows, 2 * PAIR :] = low(qkv_ref[rows, 2 * PAIR :])
        return 0

    lax.fori_loop(0, blocks, prepare, 0)

    def visit(i, j, diagonal):
        rows = pl.ds(pl.multiple_of(i * BLOCK, BLOCK), BLOCK)
        cols = pl.ds(pl.multiple_of(j * BLOCK, BLOCK), BLOCK)
        allowed = seg_col[rows, :1] == seg_row[:1, cols]
        if diagonal:
            at = lax.broadcasted_iota(jnp.int32, (BLOCK, BLOCK), 0)
            allowed = allowed & (at >= lax.broadcasted_iota(jnp.int32, (BLOCK, BLOCK), 1))
        keys = rot_ref[cols, PAIR : 2 * PAIR]
        values = rot_ref[cols, 2 * PAIR :]
        for h, q in enumerate(split_heads(rot_ref[rows, :PAIR])):
            scores = jnp.where(allowed, contract_cols(q, keys), MASKED)
            top = jnp.max(scores, axis=1, keepdims=True)
            if diagonal:
                p = jnp.exp(scores - top)
                best[h] = jnp.broadcast_to(top, (BLOCK, PAIR))
                total[h] = jnp.broadcast_to(jnp.sum(p, axis=1, keepdims=True), (BLOCK, PAIR))
                acc[h] = product(low(p), values)
            else:
                old = best[h][:, :1]
                new = jnp.maximum(old, top)
                fade = jnp.exp(old - new)
                p = jnp.exp(scores - new)
                best[h] = jnp.broadcast_to(new, (BLOCK, PAIR))
                total[h] = total[h] * fade + jnp.sum(p, axis=1, keepdims=True)
                acc[h] = acc[h] * fade + product(low(p), values)

    def one_row(i, _):
        rows = pl.ds(pl.multiple_of(i * BLOCK, BLOCK), BLOCK)
        visit(i, i, True)

        def one_col(j, _):
            @pl.when((info[0, j] < info[0, i]) & (info[2, j] >= info[1, i]))
            def _():
                visit(i, j, False)

            return 0

        lax.fori_loop(0, blocks, one_col, 0)
        mixed = jnp.where(first_head(), acc[0] / total[0], acc[1] / total[1])
        out_ref[rows, :] = low(mixed)
        wide_ref[rows, :] = mixed
        for h in range(2):
            lse_ref[0, h : h + 1, rows] = (best[h] + jnp.log(total[h])).T[:1, :]
        return 0

    lax.fori_loop(0, blocks, one_row, 0)


def backward_kernel(info, rot_ref, cos_ref, sin_ref, seg_col, seg_row, cot_ref, wide_ref, lse_ref, out_ref, delta, dq):
    blocks = rot_ref.shape[0] // BLOCK
    scale = HEAD_DIM**-0.5

    def prepare(n, _):
        rows = pl.ds(pl.multiple_of(n * BLOCK, BLOCK), BLOCK)
        terms = (wide(cot_ref[rows, :]) * wide_ref[rows, :]).T
        delta[0:1, rows] = jnp.sum(terms[:HEAD_DIM], axis=0, keepdims=True)
        delta[1:2, rows] = jnp.sum(terms[HEAD_DIM:], axis=0, keepdims=True)
        dq[rows, :] = jnp.zeros((BLOCK, PAIR), jnp.float32)
        return 0

    lax.fori_loop(0, blocks, prepare, 0)

    def visit(row, rows_count, col, cols_count, diagonal, dk, dv):
        rows, cols = aligned(row, rows_count), aligned(col, cols_count)
        allowed = seg_col[cols, :1] == seg_row[:1, rows]
        if diagonal:
            at = lax.broadcasted_iota(jnp.int32, (cols_count, rows_count), 0)
            allowed = allowed & (at <= lax.broadcasted_iota(jnp.int32, (cols_count, rows_count), 1))
        queries, cots = rot_ref[rows, :PAIR], cot_ref[rows, :]
        query_heads, cot_heads = split_heads(queries), split_heads(cots)
        key_heads = split_heads(rot_ref[cols, PAIR : 2 * PAIR])
        value_heads = split_heads(rot_ref[cols, 2 * PAIR :])
        total = dq[rows, :]
        for h in range(2):
            scores = contract_cols(key_heads[h], queries)
            probs = jnp.where(allowed, jnp.exp(scores - lse_ref[0, h : h + 1, rows]), 0.0)
            dv = dv + product(low(probs), cot_heads[h])
            prob_cot = contract_cols(value_heads[h], cots)
            score_cot = low(probs * (prob_cot - delta[h : h + 1, rows]))
            dk = dk + product(score_cot, query_heads[h])
            total = total + contract_rows(score_cot, key_heads[h])
        dq[rows, :] = total
        return dk, dv

    def unturn(grad, rows):
        return low(grad * cos_ref[rows, :] + turn(grad * sin_ref[rows, :], -1.0))

    def one_col(j, _):
        cols = pl.ds(pl.multiple_of(j * BLOCK, BLOCK), BLOCK)
        zero = jnp.zeros((BLOCK // 2, PAIR), jnp.float32)
        start, half = j * BLOCK, BLOCK // 2
        halves = [
            visit(start, BLOCK, start, half, True, zero, zero),
            visit(start + half, half, start + half, half, True, zero, zero),
        ]
        dk, dv = [jnp.concatenate(pair, axis=0) for pair in zip(*halves)]

        def one_row(i, state):
            return lax.cond(
                (info[0, j] < info[0, i]) & (info[2, j] >= info[1, i]),
                lambda state: visit(i * BLOCK, BLOCK, start, BLOCK, False, *state),
                lambda state: state,
                state,
            )

        dk, dv = lax.fori_loop(0, blocks, one_row, (dk, dv))
        out_ref[cols, PAIR : 2 * PAIR] = unturn(dk, cols)
        out_ref[cols, 2 * PAIR :] = low(dv)
        return 0

    lax.fori_loop(0, blocks, one_col, 0)

    def finish(n, _):
        rows = pl.ds(pl.multiple_of(n * BLOCK, BLOCK), BLOCK)
        out_ref[rows, :PAIR] = unturn(dq[rows, :] * scale, rows)
        return 0

    lax.fori_loop(0, blocks, finish, 0)


def attention_forward(info, qkv, cos, sin, seg_col, seg_row):
    tokens, width = qkv.shape
    pairs = width // (3 * PAIR)
    whole = lambda p, info: (0, 0)
    return pl.pallas_call(
        forward_kernel,
        grid_spec=pltpu.PrefetchScalarGridSpec(
            num_scalar_prefetch=1,
            grid=(pairs,),
            in_specs=[
                pl.BlockSpec((tokens, 3 * PAIR), lambda p, info: (0, p)),
                pl.BlockSpec((tokens, PAIR), whole),
                pl.BlockSpec((tokens, PAIR), whole),
                pl.BlockSpec((tokens, 1), whole),
                pl.BlockSpec((1, tokens), whole),
            ],
            out_specs=[
                pl.BlockSpec((tokens, 3 * PAIR), lambda p, info: (0, p)),
                pl.BlockSpec((tokens, PAIR), lambda p, info: (0, p)),
                pl.BlockSpec((tokens, PAIR), lambda p, info: (0, p)),
                pl.BlockSpec((1, 2, tokens), lambda p, info: (p, 0, 0)),
            ],
            scratch_shapes=[
                pltpu.VMEM((2, BLOCK, PAIR), jnp.float32),
                pltpu.VMEM((2, BLOCK, PAIR), jnp.float32),
                pltpu.VMEM((2, BLOCK, PAIR), jnp.float32),
            ],
        ),
        out_shape=[
            jax.ShapeDtypeStruct((tokens, width), jnp.bfloat16),
            jax.ShapeDtypeStruct((tokens, pairs * PAIR), jnp.bfloat16),
            jax.ShapeDtypeStruct((tokens, pairs * PAIR), jnp.float32),
            jax.ShapeDtypeStruct((pairs, 2, tokens), jnp.float32),
        ],
        compiler_params=pltpu.CompilerParams(vmem_limit_bytes=VMEM_LIMIT),
        cost_estimate=pl.CostEstimate(flops=tokens * tokens * width, bytes_accessed=10 * tokens * width, transcendentals=tokens * tokens * 2 * pairs),
    )(info, qkv, cos, sin, seg_col, seg_row)


def attention_backward(info, rot, cos, sin, seg_col, seg_row, cot, mixed, lse):
    tokens, width = rot.shape
    pairs = width // (3 * PAIR)
    whole = lambda p, info: (0, 0)
    return pl.pallas_call(
        backward_kernel,
        grid_spec=pltpu.PrefetchScalarGridSpec(
            num_scalar_prefetch=1,
            grid=(pairs,),
            in_specs=[
                pl.BlockSpec((tokens, 3 * PAIR), lambda p, info: (0, p)),
                pl.BlockSpec((tokens, PAIR), whole),
                pl.BlockSpec((tokens, PAIR), whole),
                pl.BlockSpec((tokens, 1), whole),
                pl.BlockSpec((1, tokens), whole),
                pl.BlockSpec((tokens, PAIR), lambda p, info: (0, p)),
                pl.BlockSpec((tokens, PAIR), lambda p, info: (0, p)),
                pl.BlockSpec((1, 2, tokens), lambda p, info: (p, 0, 0)),
            ],
            out_specs=pl.BlockSpec((tokens, 3 * PAIR), lambda p, info: (0, p)),
            scratch_shapes=[
                pltpu.VMEM((2, tokens), jnp.float32),
                pltpu.VMEM((tokens, PAIR), jnp.float32),
            ],
        ),
        out_shape=jax.ShapeDtypeStruct((tokens, width), jnp.bfloat16),
        compiler_params=pltpu.CompilerParams(vmem_limit_bytes=VMEM_LIMIT),
        cost_estimate=pl.CostEstimate(flops=3 * tokens * tokens * width, bytes_accessed=10 * tokens * width, transcendentals=tokens * tokens * 2 * pairs),
    )(info, rot, cos, sin, seg_col, seg_row, cot, mixed, lse)


def swap(values, axis, mask):
    size = lax.axis_size(axis)
    return lax.ppermute(values, axis, [(i, i ^ mask) for i in range(size)])


def masks(size):
    return [1 << n for n in reversed(range(size.bit_length() - 1))]


def offsets(size):
    held = [0]
    for mask in masks(size):
        held = held + [at ^ mask for at in held]
    return held


def gather_rows(rows, axis):
    for mask in masks(lax.axis_size(axis)):
        rows = jnp.concatenate([rows, swap(rows, axis, mask)], axis=0)
    return rows


def scatter_rows(make, count, axis):
    todo = list(reversed(masks(lax.axis_size(axis))))
    half = count // 2
    there = swap(low(make(half, count)), axis, todo[0])
    rows = make(0, half) + wide(there)
    for mask in todo[1:]:
        half = rows.shape[0] // 2
        rows = rows[:half] + wide(swap(low(rows[half:]), axis, mask))
    return rows


def scatter_both(make, count):
    rows = scatter_rows(make, count, "ctx")
    size = lax.axis_size("tp")
    me = lax.axis_index("tp")
    for mask in masks(size):
        half = rows.shape[0] // 2
        upper = (me & mask) != 0
        mine = jnp.where(upper, rows[half:], rows[:half])
        other = jnp.where(upper, rows[:half], rows[half:])
        rows = mine + wide(swap(low(other), "tp", mask))
    return rows


def join_tp(rows):
    size = lax.axis_size("tp")
    me = lax.axis_index("tp")
    for mask in reversed(masks(size)):
        upper = (me & mask) != 0
        other = swap(rows, "tp", mask)
        rows = jnp.where(upper, jnp.concatenate([other, rows], 0), jnp.concatenate([rows, other], 0))
    return rows


def own_part(rows):
    size = lax.axis_size("tp")
    count = rows.shape[0] // size
    return lax.dynamic_slice_in_dim(rows, lax.axis_index("tp") * count, count, 0)


MESH = pl.DeviceIdType.MESH
TILE = 512


def fits_kernels():
    return lax.axis_size("ctx") == 4 and lax.axis_size("tp") == 2


class Place:
    def __init__(self):
        me = lax.axis_index("ctx")
        x, core = me // 2, me % 2
        self.tp = lax.axis_index("tp")
        self.x = {"ctx": (1 - x) * 2 + core}
        self.core = {"ctx": x * 2 + 1 - core}
        self.cross = {"ctx": (1 - x) * 2 + 1 - core}
        self.y = {"tp": 1 - self.tp}

    def others(self, axis):
        size, me = lax.axis_size(axis), lax.axis_index(axis)
        return [{axis: (me + n) % size} for n in range(1, size)]


def meet(devices):
    barrier = pltpu.get_barrier_semaphore()
    for device in devices:
        pl.semaphore_signal(barrier, inc=1, device_id=device, device_id_type=MESH)
    pl.semaphore_wait(barrier, len(devices))


class Links:
    def __init__(self, send, recv):
        self.send, self.recv, self.count, self.sent = send, recv, 0, []

    def copy(self, src, dst, device, at=None):
        n = self.count
        self.count += 1
        made = pltpu.make_async_remote_copy(src, dst, self.send.at[n], self.recv.at[n], device_id=device, device_id_type=MESH)
        self.sent.append(made)
        return made

    def drain(self):
        for made in self.sent:
            made.wait_send()


def aligned(start, count):
    return pl.ds(pl.multiple_of(start, count), count)


def start_kernel(hidden, grads, segs, gains, attn_in, cot, segs_out, gains_out, hbuf, nbuf, gbuf, gain_row, send, recv, local_sem):
    place, links = Place(), Links(send, recv)
    rows = hidden.shape[0]
    half, quarter = rows // 2, rows // 4
    z = lax.axis_index("fsdp")
    near = [place.x, place.core, place.cross, place.y]
    far = place.others("fsdp")
    meet(near + far)

    def span(block, part, chunk=None):
        if chunk is None:
            return aligned(block * rows + part * half, half)
        return aligned(block * rows + part * half + chunk * quarter, quarter)

    mine, other = place.tp, 1 - place.tp
    tiny = [links.copy(gains, gains_out.at[z], device) for device in far]
    tiny_segs = [links.copy(segs, segs_out.at[n + 1], device) for n, device in enumerate(near[:3])]
    for made in tiny + tiny_segs:
        made.start()
    over_x = {}
    for name, src, dst in (("h", hidden, hbuf), ("g", grads, gbuf)):
        for q in range(2):
            over_x[name, q] = links.copy(src.at[span(0, mine, q)], dst.at[span(1, mine, q)], place.x)
    over_core = {name: links.copy(src, dst.at[aligned(2 * rows, rows)], place.core) for name, src, dst in (("h", hidden, hbuf), ("g", grads, gbuf))}
    for key in (("h", 0), ("h", 1)):
        over_x[key].start()
    over_core["h"].start()
    for key in (("g", 0), ("g", 1)):
        over_x[key].start()
    over_core["g"].start()
    kept = []

    def keep(src, dst):
        made = pltpu.make_async_copy(src, dst, local_sem.at[len(kept)])
        made.start()
        kept.append(made)

    keep(grads, cot.at[aligned(0, rows)])
    gains_out[z] = gains[...]
    segs_out[0] = segs[...]
    for made in tiny:
        made.wait_recv()
    lanes = 128
    groups = gains.shape[0] // 2
    for device in range(gains_out.shape[0]):
        for row in range(groups):
            gain_row[:, pl.ds((device * groups + row) * lanes, lanes)] = gains_out[device, row : row + 1, :]

    def normalize(src, at, block, count):
        def some(n, _):
            there = aligned(at + n * 64, 64)
            values = wide(src[there, :])
            scale = lax.rsqrt(jnp.mean(values * values, axis=1, keepdims=True) + EPS)
            nbuf[aligned(block + n * 64, 64), :] = low(values * scale * gain_row[...])
            return 0

        lax.fori_loop(0, count // 64, some, 0)
        keep(nbuf.at[pl.ds(block, count)], attn_in.at[pl.ds(block, count)])

    normalize(hidden, 0, 0, rows)
    over_y, across, last = {}, {}, {}

    def pass_on(name, buf):
        for q in range(2):
            over_x[name, q].wait_recv()
            over_y[name, q] = links.copy(buf.at[span(1, mine, q)], buf.at[span(1, mine, q)], place.y)
            across[name, q] = links.copy(buf.at[span(1, mine, q)], buf.at[span(3, mine, q)], place.core)
            over_y[name, q].start()
            across[name, q].start()

    def finish(name, buf):
        for q in range(2):
            over_y[name, q].wait_recv()
            last[name, q] = links.copy(buf.at[span(1, other, q)], buf.at[span(3, other, q)], place.core)
            last[name, q].start()

    pass_on("h", hbuf)
    over_core["h"].wait_recv()
    normalize(hbuf, 2 * rows, 2 * rows, rows)
    finish("h", hbuf)
    normalize(hbuf, rows, rows, rows)
    pass_on("g", gbuf)
    for q in range(2):
        across["h", q].wait_recv()
        last["h", q].wait_recv()
    normalize(hbuf, 3 * rows, 3 * rows, rows)
    over_core["g"].wait_recv()
    keep(gbuf.at[aligned(2 * rows, rows)], cot.at[aligned(2 * rows, rows)])
    finish("g", gbuf)
    keep(gbuf.at[aligned(rows, rows)], cot.at[aligned(rows, rows)])
    for q in range(2):
        across["g", q].wait_recv()
        last["g", q].wait_recv()
    keep(gbuf.at[aligned(3 * rows, rows)], cot.at[aligned(3 * rows, rows)])
    for made in tiny_segs:
        made.wait_recv()
    links.drain()
    for made in kept:
        made.wait()


def start_exchange(hidden, grads, segments, attn_gain, mlp_gain):
    rows, width = hidden.shape
    fsdp = lax.axis_size("fsdp")
    segs = jnp.concatenate([segments.reshape(-1, 128), jnp.zeros((8 - rows // 128, 128), jnp.int32)], axis=0)
    gains = wide(jnp.concatenate([attn_gain, mlp_gain])).reshape(-1, 128)
    vmem = pl.BlockSpec(memory_space=pltpu.VMEM)
    hbm = pl.BlockSpec(memory_space=pl.ANY)
    tokens = 4 * rows
    attn_in, cot, segs, gains = pl.pallas_call(
        start_kernel,
        in_specs=[vmem] * 4,
        out_specs=[hbm, hbm, vmem, vmem],
        out_shape=[
            jax.ShapeDtypeStruct((tokens, width), jnp.bfloat16),
            jax.ShapeDtypeStruct((tokens, width), jnp.bfloat16),
            jax.ShapeDtypeStruct((4, 8, 128), jnp.int32),
            jax.ShapeDtypeStruct((fsdp,) + gains.shape, jnp.float32),
        ],
        scratch_shapes=[
            pltpu.VMEM((tokens, width), jnp.bfloat16),
            pltpu.VMEM((tokens, width), jnp.bfloat16),
            pltpu.VMEM((tokens, width), jnp.bfloat16),
            pltpu.VMEM((1, width), jnp.float32),
            pltpu.SemaphoreType.DMA((fsdp + 32,)),
            pltpu.SemaphoreType.DMA((fsdp + 32,)),
            pltpu.SemaphoreType.DMA((8,)),
        ],
        compiler_params=pltpu.CompilerParams(collective_id=0, has_side_effects=True, vmem_limit_bytes=VMEM_LIMIT),
        cost_estimate=pl.CostEstimate(flops=0, bytes_accessed=200_000_000, transcendentals=0),
    )(hidden, grads, segs, gains)
    segs = segs[:, : rows // 128].reshape(tokens)
    gains = jnp.transpose(gains.reshape(fsdp, 2, -1), (1, 0, 2)).reshape(2, width)
    return attn_in, cot, segs, gains


def scatter_scratch(rows, width):
    part, half = rows // 8, width // 2
    return [
        pltpu.VMEM((4, part, width), jnp.bfloat16),
        pltpu.VMEM((4, part, width), jnp.bfloat16),
        pltpu.VMEM((6, part, half), jnp.bfloat16),
        pltpu.VMEM((6, part, half), jnp.bfloat16),
        pltpu.VMEM((2, part, half), jnp.float32),
        pltpu.VMEM((part, width), jnp.float32),
        pltpu.SemaphoreType.DMA((14,)),
        pltpu.SemaphoreType.DMA((14,)),
    ]


class Scatter:
    def __init__(self, place, make, count, refs, first=("x", "y")):
        self.place, self.make = place, make
        self.hi, self.core_in, self.out, self.come, self.wait, self.total, send, recv = refs
        self.part = count // 8
        self.half = self.total.shape[1] // 2
        self.links = Links(send, recv)
        self.core = {}
        for side in range(2):
            cols = pl.ds(side * self.half, self.half)
            for n in range(4):
                self.core[n, side] = self.links.copy(self.hi.at[n, :, cols], self.core_in.at[n, :, cols], place.core)
        self.send, self.away, self.stays = [], {}, {}
        for side, link in enumerate(first):
            to, then = (place.x, place.y) if link == "x" else (place.y, place.x)
            for n, device in enumerate((to, to, then)):
                at = 3 * side + n
                self.send.append(self.links.copy(self.out.at[at], self.come.at[at], device))
            second, stay = (1, 2) if link == "x" else (2, 1)
            self.away[0, side], self.away[second, side] = 3 * side, 3 * side + 1
            self.stays[side] = stay

    def rows(self, n):
        tp = self.place.tp
        part = (1 - tp) + (n % 2) * (2 * tp - 1)
        return ((1 - n // 2) * 2 + part) * self.part

    def columns(self, side, each):
        tiles = self.half // TILE

        def one(n, _):
            each(aligned(side * self.half + n * TILE, TILE), aligned(n * TILE, TILE))
            return 0

        lax.fori_loop(0, tiles, one, 0)

    def to_core(self, n, side):
        rows = aligned(4 * self.part + self.rows(n), self.part)

        def each(cols, _):
            self.hi[n, :, cols] = low(self.make(rows, cols))

        self.columns(side, each)
        self.core[n, side].start()

    def to_links(self, n, side):
        rows = aligned(self.rows(n), self.part)
        self.core[n, side].wait_recv()

        def each(cols, at):
            value = self.make(rows, cols) + wide(self.core_in[n, :, cols])
            if (n, side) in self.away:
                self.out[self.away[n, side], :, at] = low(value)
            elif n == 3:
                self.total[:, cols] = value
            else:
                self.wait[side, :, at] = value

        self.columns(side, each)
        if (n, side) in self.away:
            self.send[self.away[n, side]].start()

    def units(self):
        return (
            [(0, side) for side in range(2)]
            + [(n, side) for n in (1, 2) for side in range(2) if (n, side) in self.away]
            + [(self.stays[side], side) for side in range(2)]
            + [(3, side) for side in range(2)]
        )

    def start(self):
        units = self.units()
        ahead = 2
        for unit in units[:ahead]:
            self.to_core(*unit)
        for at, unit in enumerate(units):
            self.to_links(*unit)
            if at + ahead < len(units):
                self.to_core(*units[at + ahead])

    def turn(self):
        for side in range(2):
            came, goes = 3 * side, 3 * side + 2
            self.send[came].wait_recv()

            def each(_, at):
                self.out[goes, :, at] = low(self.wait[side, :, at] + wide(self.come[came, :, at]))

            self.columns(side, each)
            self.send[goes].start()

    def finish(self):
        for side in range(2):
            for n in (1, 2):
                self.send[3 * side + n].wait_recv()
            cols = pl.ds(side * self.half, self.half)
            self.total[:, cols] = self.total[:, cols] + wide(self.come[3 * side + 1]) + wide(self.come[3 * side + 2])
        self.links.drain()


def gather_plane(place, links, mine, full, part):
    half = mine.shape[1] // 2
    left, right = pl.ds(0, half), pl.ds(half, half)
    own, other = place.tp, 1 - place.tp

    def rows(block, tp):
        return aligned((block * 2 + tp) * part, part)

    y_left = links.copy(mine.at[:, left], full.at[rows(0, own), left], place.y)
    x_right = links.copy(mine.at[:, right], full.at[rows(1, own), right], place.x)
    y_right = links.copy(mine.at[:, right], full.at[rows(0, own), right], place.y)
    x_left = links.copy(mine.at[:, left], full.at[rows(1, own), left], place.x)
    core = [links.copy(mine, full.at[rows(2, own)], place.core)]
    for made in (y_left, x_right, y_right, x_left, core[0]):
        made.start()
    waits = []

    def relay(come, block, tp, cols, onward=None):
        come.wait_recv()
        here = full.at[rows(block, tp), cols]
        if onward == "x":
            made = links.copy(here, full.at[rows(1, tp), cols], place.x)
        elif onward == "y":
            made = links.copy(here, full.at[rows(block, tp), cols], place.y)
        if onward:
            made.start()
        over = links.copy(here, full.at[rows(block + 2, tp), cols], place.core)
        over.start()
        core.append(over)
        return made if onward else None

    far_left = relay(y_left, 0, other, left, "x")
    far_right = relay(x_right, 1, own, right, "y")
    relay(y_right, 0, other, right)
    relay(x_left, 1, own, left)
    relay(far_left, 1, other, left)
    relay(far_right, 1, other, right)
    for made in core:
        made.wait_recv()


def own_rows_of(ref, place, part):
    return ref[aligned(place.tp * part, part), :]


def forward_mid_kernel(mixed, weight, hidden, gain, full, resid_out, mine, *refs):
    place = Place()
    scatter_refs, (send, recv, local_sem) = refs[:-3], refs[-3:]
    count = mixed.shape[0]
    part = count // 8
    meet([place.x, place.core, place.y])
    scatter = Scatter(place, lambda rows, cols: contract_cols(mixed[rows, :], weight[cols, weight.shape[1] - mixed.shape[1] :]), count, scatter_refs)
    scatter.start()
    scatter.turn()
    scatter.finish()
    step = 64

    def some(n, _):
        rows = aligned(n * step, step)
        values = wide(hidden[aligned(place.tp * part + n * step, step), :]) + scatter.total[rows, :]
        resid_out[rows, :] = values
        scale = lax.rsqrt(jnp.mean(values * values, axis=1, keepdims=True) + EPS)
        mine[rows, :] = low(values * scale * gain[...])
        return 0

    lax.fori_loop(0, part // step, some, 0)
    stay = pltpu.make_async_copy(mine, full.at[aligned(place.tp * part, part)], local_sem)
    stay.start()
    links = Links(send, recv)
    gather_plane(place, links, mine, full, part)
    links.drain()
    stay.wait()


def mid_scratch(count, width):
    return [pltpu.VMEM((count // 8, width), jnp.bfloat16)] + scatter_scratch(count, width) + [
        pltpu.SemaphoreType.DMA((16,)),
        pltpu.SemaphoreType.DMA((16,)),
        pltpu.SemaphoreType.DMA,
    ]


def forward_mid(mixed, weight, hidden, gain):
    count, width = mixed.shape[0], weight.shape[0]
    vmem = pl.BlockSpec(memory_space=pltpu.VMEM)
    return pl.pallas_call(
        forward_mid_kernel,
        in_specs=[vmem] * 4,
        out_specs=[pl.BlockSpec(memory_space=pl.ANY), vmem],
        out_shape=[jax.ShapeDtypeStruct((count, width), jnp.bfloat16), jax.ShapeDtypeStruct((count // 8, width), jnp.float32)],
        scratch_shapes=mid_scratch(count, width),
        compiler_params=pltpu.CompilerParams(collective_id=1, has_side_effects=True, vmem_limit_bytes=VMEM_LIMIT),
        cost_estimate=pl.CostEstimate(flops=0, bytes_accessed=300_000_000, transcendentals=0),
    )(mixed, weight, hidden, gain[None, :])


def norm_back(values, scale, gain, cot):
    scaled = cot * gain
    lean = jnp.mean(values * scaled, axis=1, keepdims=True)
    return scale * scaled - values * (scale * scale * scale) * lean, cot * (values * scale)


def backward_mid_kernel(gate_cot, up_cot, weights, resid, grads, gain, full, cot_out, gain_out, mine, *refs):
    place = Place()
    scatter_refs, (send, recv, local_sem) = refs[:-3], refs[-3:]
    count, hidden_cols = gate_cot.shape
    part = count // 8
    meet([place.x, place.core, place.y])

    def make(rows, cols):
        return contract_cols(gate_cot[rows, :], weights[cols, :hidden_cols]) + contract_cols(up_cot[rows, :], weights[cols, hidden_cols:])

    scatter = Scatter(place, make, count, scatter_refs)
    scatter.start()
    scatter.turn()
    scatter.finish()
    step = 32

    def some(n, sums):
        rows = aligned(n * step, step)
        values = resid[rows, :]
        scale = lax.rsqrt(jnp.mean(values * values, axis=1, keepdims=True) + EPS)
        back, terms = norm_back(values, scale, gain[...], scatter.total[rows, :])
        cot = wide(grads[aligned(place.tp * part + n * step, step), :]) + back
        cot_out[rows, :] = cot
        mine[rows, :] = low(cot)
        return sums + jnp.sum(terms, axis=0, keepdims=True)

    gain_out[...] = lax.fori_loop(0, part // step, some, jnp.zeros(gain.shape, jnp.float32))
    stay = pltpu.make_async_copy(mine, full.at[aligned(place.tp * part, part)], local_sem)
    stay.start()
    links = Links(send, recv)
    gather_plane(place, links, mine, full, part)
    links.drain()
    stay.wait()


def backward_mid(gate_cot, up_cot, weights, resid, grads, gain):
    count, width = gate_cot.shape[0], weights.shape[0]
    vmem = pl.BlockSpec(memory_space=pltpu.VMEM)
    return pl.pallas_call(
        backward_mid_kernel,
        in_specs=[vmem] * 6,
        out_specs=[pl.BlockSpec(memory_space=pl.ANY), vmem, vmem],
        out_shape=[
            jax.ShapeDtypeStruct((count, width), jnp.bfloat16),
            jax.ShapeDtypeStruct((count // 8, width), jnp.float32),
            jax.ShapeDtypeStruct((1, width), jnp.float32),
        ],
        scratch_shapes=mid_scratch(count, width),
        compiler_params=pltpu.CompilerParams(collective_id=2, has_side_effects=True, vmem_limit_bytes=VMEM_LIMIT),
        cost_estimate=pl.CostEstimate(flops=0, bytes_accessed=300_000_000, transcendentals=0),
    )(gate_cot, up_cot, weights, resid, grads, gain[None, :])


def finish_kernel(cots, weights, hidden_act, down, resid, resid_cot, hidden, gain, gain_two, out, grad_out, gains_out, mine, sums, come, *refs):
    place = Place()
    (send, recv, local_sem), refs = refs[-3:], refs[:-3]
    count = cots.shape[0]
    part = count // 8
    each = len(refs) // 2
    meet([place.x, place.core, place.y] + place.others("fsdp"))
    first = Scatter(place, lambda rows, cols: contract_cols(cots[rows, :], weights[cols, : cots.shape[1]]), count, refs[:each])
    second = Scatter(place, lambda rows, cols: product(hidden_act[rows, :], down[:, cols]), count, refs[each:])
    links = Links(send, recv)
    own = aligned(place.tp * part, part)
    step = 32
    first.start()
    first.turn()
    second.start()
    first.finish()

    def some(n, total):
        rows = aligned(n * step, step)
        values = wide(hidden[aligned(place.tp * part + n * step, step), :])
        scale = lax.rsqrt(jnp.mean(values * values, axis=1, keepdims=True) + EPS)
        back, terms = norm_back(values, scale, gain[...], first.total[rows, :])
        mine[0, rows, :] = low(resid_cot[rows, :] + back)
        return total + jnp.sum(terms, axis=0, keepdims=True)

    sums[0, 0:1, :] = lax.fori_loop(0, part // step, some, jnp.zeros(gain.shape, jnp.float32))
    sums[0, 1:2, :] = gain_two[...]
    near = [place.x, place.core, place.y]
    near_sums = [links.copy(sums.at[n], come.at[n], device) for n, device in enumerate(near)]
    near_sums[0].start()
    second.turn()
    grad_y = links.copy(mine.at[0], grad_out.at[own], place.y)
    grad_y.start()
    stay = [pltpu.make_async_copy(mine.at[0], grad_out.at[own], local_sem.at[0])]
    stay[0].start()
    for n in range(len(near)):
        near_sums[n].wait_recv()
        sums[n + 1] = sums[n] + come[n]
        if n + 1 < len(near):
            near_sums[n + 1].start()
    at = len(near)
    far = [links.copy(sums.at[at], come.at[at + n], device) for n, device in enumerate(place.others("fsdp"))]
    for made in far:
        made.start()
    second.finish()
    mine[1] = low(resid[...] + second.total[...])
    out_y = links.copy(mine.at[1], out.at[own], place.y)
    out_y.start()
    stay.append(pltpu.make_async_copy(mine.at[1], out.at[own], local_sem.at[1]))
    stay[1].start()
    total = sums[at]
    for n, made in enumerate(far):
        made.wait_recv()
        total = total + come[at + n]
    gains_out[...] = total
    grad_y.wait_recv()
    out_y.wait_recv()
    links.drain()
    for made in stay:
        made.wait()


def finish_exchange(cots, weights, hidden_act, down, resid, resid_cot, hidden, gain, gain_two):
    count, width = cots.shape[0], weights.shape[0]
    fsdp = lax.axis_size("fsdp")
    vmem = pl.BlockSpec(memory_space=pltpu.VMEM)
    hbm = pl.BlockSpec(memory_space=pl.ANY)
    return pl.pallas_call(
        finish_kernel,
        in_specs=[vmem] * 9,
        out_specs=[hbm, hbm, vmem],
        out_shape=[jax.ShapeDtypeStruct((count // 4, width), jnp.bfloat16)] * 2 + [jax.ShapeDtypeStruct((2, width), jnp.float32)],
        scratch_shapes=[
            pltpu.VMEM((2, count // 8, width), jnp.bfloat16),
            pltpu.VMEM((4, 2, width), jnp.float32),
            pltpu.VMEM((2 + fsdp, 2, width), jnp.float32),
        ]
        + scatter_scratch(count, width) * 2
        + [pltpu.SemaphoreType.DMA((5 + fsdp,)), pltpu.SemaphoreType.DMA((5 + fsdp,)), pltpu.SemaphoreType.DMA((2,))],
        compiler_params=pltpu.CompilerParams(collective_id=3, has_side_effects=True, vmem_limit_bytes=VMEM_LIMIT),
        cost_estimate=pl.CostEstimate(flops=0, bytes_accessed=300_000_000, transcendentals=0),
    )(cots, weights, hidden_act, down, resid, resid_cot, hidden, gain[None, :], gain_two)


def take_attention_kernel(at, query, key, value, out, taken):
    pairs = query.shape[1] // PAIR
    for p in range(pairs):
        for n, part in enumerate((query, key, value)):
            taken[:, (3 * p + n) * PAIR : (3 * p + n + 1) * PAIR] = part[:, p * PAIR : (p + 1) * PAIR]
    taken[:, 3 * pairs * PAIR :] = out[...].T


def take_attention(me, query, key, value, out, count):
    depth = query.shape[0]
    block = pl.BlockSpec((depth, count), lambda n, at: (0, at[0]))
    return pl.pallas_call(
        take_attention_kernel,
        grid_spec=pltpu.PrefetchScalarGridSpec(
            num_scalar_prefetch=1,
            grid=(1,),
            in_specs=[block] * 3 + [pl.BlockSpec((count, depth), lambda n, at: (at[0], 0))],
            out_specs=pl.BlockSpec((depth, 4 * count), lambda n, at: (0, 0)),
        ),
        out_shape=jax.ShapeDtypeStruct((depth, 4 * count), query.dtype),
        compiler_params=pltpu.CompilerParams(vmem_limit_bytes=VMEM_LIMIT),
    )(me, query, key, value, out)


def take_hidden_kernel(at, gate, up, down, both, rows):
    count = gate.shape[1]
    both[:, :count] = gate[...]
    both[:, count:] = up[...]
    rows[...] = down[...]


def take_hidden(me, gate, up, down, count):
    depth = gate.shape[0]
    block = pl.BlockSpec((depth, count), lambda n, at: (0, at[0]))
    return pl.pallas_call(
        take_hidden_kernel,
        grid_spec=pltpu.PrefetchScalarGridSpec(
            num_scalar_prefetch=1,
            grid=(1,),
            in_specs=[block] * 2 + [pl.BlockSpec((count, depth), lambda n, at: (at[0], 0))],
            out_specs=[pl.BlockSpec((depth, 2 * count), lambda n, at: (0, 0)), pl.BlockSpec((count, depth), lambda n, at: (0, 0))],
        ),
        out_shape=[jax.ShapeDtypeStruct((depth, 2 * count), gate.dtype), jax.ShapeDtypeStruct((count, depth), down.dtype)],
        compiler_params=pltpu.CompilerParams(vmem_limit_bytes=VMEM_LIMIT),
    )(me, gate, up, down)


def first_swaps(block):
    pieces = [block]
    for mask in masks(lax.axis_size("ctx"))[:-1]:
        pieces = pieces + [swap(piece, "ctx", mask) for piece in pieces]
    return pieces


def last_swap(pieces):
    return pieces + [swap(piece, "ctx", 1) for piece in pieces]


def order_of_pieces():
    return lax.axis_index("ctx") ^ jnp.array(offsets(lax.axis_size("ctx")), jnp.int32)


CHUNKS = 2


def chunk_of(m):
    return lambda n, c, at: (jnp.where(n == m, c, jnp.where(n < m, 0, CHUNKS - 1)), 0)


def place_kernel(at, *refs):
    out = refs[-1]
    for n, piece in enumerate(refs[:-1]):

        @pl.when(pl.program_id(0) == n)
        def _():
            out[...] = wide(piece[...])


def place_pieces(pieces, axis):
    rows, cols = pieces[0].shape
    shape = [rows, cols]
    shape[axis] *= len(pieces)
    block = (rows // CHUNKS, cols)
    return pl.pallas_call(
        place_kernel,
        grid_spec=pltpu.PrefetchScalarGridSpec(
            num_scalar_prefetch=1,
            grid=(len(pieces), CHUNKS),
            in_specs=[pl.BlockSpec(block, chunk_of(m)) for m in range(len(pieces))],
            out_specs=pl.BlockSpec(block, lambda n, c, at: (at[n] * CHUNKS + c, 0) if axis == 0 else (c, at[n])),
        ),
        out_shape=jax.ShapeDtypeStruct(shape, jnp.float32),
        compiler_params=pltpu.CompilerParams(vmem_limit_bytes=VMEM_LIMIT),
        cost_estimate=pl.CostEstimate(flops=0, bytes_accessed=6 * math.prod(shape), transcendentals=0),
    )(order_of_pieces(), *pieces)


def place_attention_kernel(at, *refs):
    pieces, outs = refs[:-4], refs[-4:]
    count = outs[0].shape[1]
    pairs = count // PAIR
    for n, piece in enumerate(pieces):

        @pl.when(pl.program_id(0) == n)
        def _():
            for p in range(pairs):
                for m in range(3):
                    outs[m][:, p * PAIR : (p + 1) * PAIR] = wide(piece[:, (3 * p + m) * PAIR : (3 * p + m + 1) * PAIR])
            outs[3][...] = wide(piece[:, 3 * count :]).T


def place_attention(pieces):
    depth, count = pieces[0].shape[0], pieces[0].shape[1] // 4
    whole = len(pieces) * count
    rows = depth // CHUNKS
    side = pl.BlockSpec((rows, count), lambda n, c, at: (c, at[n]))
    return pl.pallas_call(
        place_attention_kernel,
        grid_spec=pltpu.PrefetchScalarGridSpec(
            num_scalar_prefetch=1,
            grid=(len(pieces), CHUNKS),
            in_specs=[pl.BlockSpec((rows, 4 * count), chunk_of(m)) for m in range(len(pieces))],
            out_specs=[side] * 3 + [pl.BlockSpec((count, rows), lambda n, c, at: (at[n], c))],
        ),
        out_shape=[jax.ShapeDtypeStruct((depth, whole), jnp.float32)] * 3 + [jax.ShapeDtypeStruct((whole, depth), jnp.float32)],
        compiler_params=pltpu.CompilerParams(vmem_limit_bytes=VMEM_LIMIT),
        cost_estimate=pl.CostEstimate(flops=0, bytes_accessed=24 * depth * whole, transcendentals=0),
    )(order_of_pieces(), *pieces)


def local(
    hidden_in,
    out_grad,
    segment_ids,
    attn_gain,
    w_query,
    w_key,
    w_value,
    w_out,
    mlp_gain,
    w_gate,
    w_up,
    w_down,
):
    group = lax.axis_size("ctx")
    me = lax.axis_index("ctx")
    local_rows = hidden_in.shape[1]
    tokens = local_rows * group
    head_cols = w_query.shape[1] // group
    pairs = head_cols // PAIR
    ff_cols = w_gate.shape[1] // group

    def gather(weight, axis):
        return lax.all_gather(weight, "fsdp", axis=axis, tiled=True)

    def settle(part, axis):
        return lax.psum_scatter(part, "fsdp", scatter_dimension=axis, tiled=True)

    at = me[None]
    w_attn = gather(take_attention(at, w_query, w_key, w_value, w_out, head_cols), 0)
    qkv_cols = 3 * head_cols
    w_qkv, w_out_t = w_attn[:, :qkv_cols], w_attn[:, qkv_cols:]
    own_gate_up, own_down = take_hidden(at, w_gate, w_up, w_down, ff_cols)
    full_gate_up = gather(own_gate_up, 0)
    full_down = gather(own_down, 1)

    kernels = fits_kernels()
    if kernels:
        attn_in, branch_cot, segments, gains = start_exchange(hidden_in[0], out_grad[0], segment_ids[0], attn_gain, mlp_gain)
        gain_one, gain_two = gains[0], gains[1]
    else:
        gains = wide(gather(jnp.stack([attn_gain, mlp_gain]), 1))
        gain_one, gain_two = gains[0], gains[1]
        rows_in = wide(hidden_in[0])
        r1 = lax.rsqrt(jnp.mean(rows_in * rows_in, axis=-1, keepdims=True) + EPS)
        attn_in = gather_rows(low(rows_in * r1 * gain_one), "ctx")
        segments = gather_rows(segment_ids[0], "ctx")
        branch_cot = gather_rows(out_grad[0], "ctx")

    firsts = jnp.stack([(me ^ at) * local_rows for at in offsets(group)])
    positions = (firsts[:, None] + jnp.arange(local_rows, dtype=jnp.int32)[None, :]).reshape(tokens)
    exponents = jnp.arange(0, HEAD_DIM, 2).astype(jnp.float32) / HEAD_DIM
    inverse = jnp.float32(ROPE_BASE) ** (-exponents)
    angles = positions.astype(jnp.float32)[:, None] * inverse[None, :]
    cos = jnp.tile(jnp.cos(angles), (1, 4))
    sin = jnp.tile(jnp.sin(angles), (1, 4))
    info = jnp.stack([positions[::BLOCK], segments[::BLOCK], segments[BLOCK - 1 :: BLOCK]])
    seg_col, seg_row = segments[:, None], segments[None, :]

    qkv = product(attn_in, w_qkv)
    rot, mixed, mixed_wide, lse = attention_forward(info, qkv, cos, sin, seg_col, seg_row)

    own_in = wide(own_part(hidden_in[0]))
    if kernels:
        mlp_in, resid = forward_mid(mixed, w_attn, hidden_in[0], gain_two)
    else:
        part = scatter_both(lambda lo, hi: contract_cols(mixed[lo:hi], w_out_t), tokens)
        resid = own_in + part
        r2 = lax.rsqrt(jnp.mean(resid * resid, axis=-1, keepdims=True) + EPS)
        mlp_in = gather_rows(join_tp(low(resid * r2 * gain_two)), "ctx")
    acts = product(mlp_in, full_gate_up)
    gate_act, up_act = acts[:, :ff_cols], acts[:, ff_cols:]
    sigmoid = jax.nn.sigmoid(gate_act)
    hidden = low(gate_act * sigmoid * up_act)
    gate_slope = low(up_act * sigmoid * (1.0 + gate_act * (1.0 - sigmoid)))
    up_slope = low(gate_act * sigmoid)
    hidden, gate_slope, up_slope = lax.optimization_barrier((hidden, gate_slope, up_slope))
    down_part = low(contract_rows(hidden, branch_cot))
    down_part, full_down, branch_cot = lax.optimization_barrier((down_part, full_down, branch_cot))
    down_own = settle(down_part, 1)

    hidden_cot = contract_cols(branch_cot, full_down)
    gate_cot = low(hidden_cot * gate_slope)
    up_cot = low(hidden_cot * up_slope)
    gate_part = low(contract_rows(mlp_in, gate_cot))
    up_part = low(contract_rows(mlp_in, up_cot))
    gate_own = settle(gate_part, 0)
    up_own = settle(up_part, 0)
    if kernels:
        gate_cot, up_cot, gate_part, up_part = lax.optimization_barrier((gate_cot, up_cot, gate_part, up_part))
        attn_cot, resid_cot, gain_two_part = backward_mid(gate_cot, up_cot, full_gate_up, resid, out_grad[0], gain_two)
    else:
        mlp_in_cot = scatter_both(
            lambda lo, hi: contract_cols(gate_cot[lo:hi], full_gate_up[:, :ff_cols])
            + contract_cols(up_cot[lo:hi], full_gate_up[:, ff_cols:]),
            tokens,
        )
        back, terms = norm_back(resid, r2, gain_two, mlp_in_cot)
        gain_two_part = jnp.sum(terms, axis=0, keepdims=True)
        resid_cot = wide(own_part(out_grad[0])) + back
        attn_cot = gather_rows(join_tp(low(resid_cot)), "ctx")
    mixed_cot = low(product(attn_cot, w_out_t))
    out_part = low(contract_rows(attn_cot, mixed))
    mixed_cot, out_part, down_own, gate_own = lax.optimization_barrier((mixed_cot, out_part, down_own, gate_own))
    down_pieces, gate_pieces = first_swaps(down_own), first_swaps(gate_own)
    cots = attention_backward(info, rot, cos, sin, seg_col, seg_row, mixed_cot, mixed_wide, lse)
    count = len(down_pieces)
    cots, *pieces = lax.optimization_barrier((cots, *down_pieces, *gate_pieces))
    down_pieces, gate_pieces = pieces[:count], pieces[count:]
    attn_part = jnp.concatenate([low(contract_rows(attn_in, cots)), out_part], axis=1)
    attn_own = settle(attn_part, 0)
    if kernels:
        cots, attn_part = lax.optimization_barrier((cots, attn_part))
        output, input_grad, gain_sums = finish_exchange(
            cots, w_attn, hidden, full_down, resid, resid_cot, hidden_in[0], gain_one, gain_two_part
        )
    else:
        out_sum = scatter_both(lambda lo, hi: product(hidden[lo:hi], full_down), tokens)
        output = join_tp(low(resid + out_sum))
        attn_in_cot = scatter_both(lambda lo, hi: contract_cols(cots[lo:hi], w_qkv), tokens)
        back, terms = norm_back(own_in, own_part(r1), gain_one, attn_in_cot)
        input_grad = join_tp(low(resid_cot + back))
        gain_sums = lax.psum(jnp.concatenate([jnp.sum(terms, axis=0, keepdims=True), gain_two_part]), ("fsdp", "ctx", "tp"))
    output, input_grad, up_own = lax.optimization_barrier((output, input_grad, up_own))
    up_pieces = first_swaps(up_own)
    down_grad = place_pieces(last_swap(down_pieces), 0)
    gate_grad = place_pieces(last_swap(gate_pieces), 1)
    attn_pieces = first_swaps(attn_own)
    down_grad, gate_grad, *pieces = lax.optimization_barrier((down_grad, gate_grad, *up_pieces, *attn_pieces))
    up_pieces, attn_pieces = pieces[:count], pieces[count:]
    attn_pieces = last_swap(attn_pieces)
    up_grad = place_pieces(last_swap(up_pieces), 1)
    query_grad, key_grad, value_grad, out_proj_grad = place_attention(attn_pieces)

    gain_sums = lax.dynamic_slice_in_dim(gain_sums, lax.axis_index("fsdp") * attn_gain.shape[0], attn_gain.shape[0], 1)
    return (
        output[None],
        input_grad[None],
        gain_sums[0],
        query_grad,
        key_grad,
        value_grad,
        out_proj_grad,
        gain_sums[1],
        gate_grad,
        up_grad,
        down_grad,
    )


def solution(mesh):
    weight, gain = P("fsdp", "tp"), P("fsdp")
    rows = P("fsdp", "ctx", None)
    in_specs = (rows, rows, P("fsdp", "ctx"), gain, weight, weight, weight, P("tp", "fsdp"), gain, weight, weight, P("tp", "fsdp"))
    out_specs = (rows, rows, gain, weight, weight, weight, P("tp", "fsdp"), gain, weight, weight, P("tp", "fsdp"))
    return jax.shard_map(local, mesh=mesh, in_specs=in_specs, out_specs=out_specs, check_vma=False)
```

```python
import math

import jax
import jax.numpy as jnp
from jax import lax
from jax.experimental import pallas as pl
from jax.experimental.pallas import tpu as pltpu
from jax.sharding import PartitionSpec as P

HEAD_DIM = 64
EPS = 1e-05
ROPE_BASE = 130000.0
MASKED = -1e30
PAIR = 2 * HEAD_DIM
BLOCK = 512
VMEM_LIMIT = 60 * 1024 * 1024


def low(values):
    return values.astype(jnp.bfloat16)


def wide(values):
    return values.astype(jnp.float32)


def product(a, b):
    return jnp.dot(a, b, preferred_element_type=jnp.float32)


def contract_rows(a, b):
    return lax.dot_general(a, b, (((0,), (0,)), ((), ())), preferred_element_type=jnp.float32)


def contract_cols(a, b):
    return lax.dot_general(a, b, (((1,), (1,)), ((), ())), preferred_element_type=jnp.float32)


def aligned(start, count):
    return pl.ds(pl.multiple_of(start, count), count)


def first_head():
    return lax.broadcasted_iota(jnp.int32, (1, PAIR), 1) < HEAD_DIM


def split_heads(rows):
    zero = jnp.zeros_like(rows)
    mask = first_head()
    return jnp.where(mask, rows, zero), jnp.where(mask, zero, rows)


def turn(rows, sign):
    half = HEAD_DIM // 2
    lanes = lax.broadcasted_iota(jnp.int32, (1, PAIR), 1)
    up = pltpu.roll(rows, PAIR - half, 1)
    down = pltpu.roll(rows, half, 1)
    return jnp.where(lanes % HEAD_DIM < half, -sign * up, sign * down)


def forward_kernel(info, qkv_ref, cos_ref, sin_ref, seg_col, seg_row, rot_ref, out_ref, wide_ref, lse_ref, best, total, acc):
    blocks = qkv_ref.shape[0] // BLOCK

    def prepare(n, _):
        rows = pl.ds(pl.multiple_of(n * BLOCK, BLOCK), BLOCK)
        cos, sin = cos_ref[rows, :], sin_ref[rows, :]
        q = qkv_ref[rows, :PAIR]
        k = qkv_ref[rows, PAIR : 2 * PAIR]
        rot_ref[rows, :PAIR] = low(low(q * cos + turn(q, 1.0) * sin) * jnp.bfloat16(HEAD_DIM**-0.5))
        rot_ref[rows, PAIR : 2 * PAIR] = low(k * cos + turn(k, 1.0) * sin)
        rot_ref[rows, 2 * PAIR :] = low(qkv_ref[rows, 2 * PAIR :])
        return 0

    lax.fori_loop(0, blocks, prepare, 0)

    def visit(i, j, diagonal):
        rows = pl.ds(pl.multiple_of(i * BLOCK, BLOCK), BLOCK)
        cols = pl.ds(pl.multiple_of(j * BLOCK, BLOCK), BLOCK)
        allowed = seg_col[rows, :1] == seg_row[:1, cols]
        if diagonal:
            at = lax.broadcasted_iota(jnp.int32, (BLOCK, BLOCK), 0)
            allowed = allowed & (at >= lax.broadcasted_iota(jnp.int32, (BLOCK, BLOCK), 1))
        keys = rot_ref[cols, PAIR : 2 * PAIR]
        values = rot_ref[cols, 2 * PAIR :]
        for h, q in enumerate(split_heads(rot_ref[rows, :PAIR])):
            scores = jnp.where(allowed, contract_cols(q, keys), MASKED)
            top = jnp.max(scores, axis=1, keepdims=True)
            if diagonal:
                p = jnp.exp(scores - top)
                best[h] = jnp.broadcast_to(top, (BLOCK, PAIR))
                total[h] = jnp.broadcast_to(jnp.sum(p, axis=1, keepdims=True), (BLOCK, PAIR))
                acc[h] = product(low(p), values)
            else:
                old = best[h][:, :1]
                new = jnp.maximum(old, top)
                fade = jnp.exp(old - new)
                p = jnp.exp(scores - new)
                best[h] = jnp.broadcast_to(new, (BLOCK, PAIR))
                total[h] = total[h] * fade + jnp.sum(p, axis=1, keepdims=True)
                acc[h] = acc[h] * fade + product(low(p), values)

    def one_row(i, _):
        rows = pl.ds(pl.multiple_of(i * BLOCK, BLOCK), BLOCK)
        visit(i, i, True)

        def one_col(j, _):
            @pl.when((info[0, j] < info[0, i]) & (info[2, j] >= info[1, i]))
            def _():
                visit(i, j, False)

            return 0

        lax.fori_loop(0, blocks, one_col, 0)
        mixed = jnp.where(first_head(), acc[0] / total[0], acc[1] / total[1])
        out_ref[rows, :] = low(mixed)
        wide_ref[rows, :] = mixed
        for h in range(2):
            lse_ref[0, h : h + 1, rows] = (best[h] + jnp.log(total[h])).T[:1, :]
        return 0

    lax.fori_loop(0, blocks, one_row, 0)


class Backward:
    def __init__(self, pair, rot, cos, sin, seg_col, seg_row, cot, mixed, lse, out, delta, dq, follows):
        self.pair, self.follows = pair, follows
        self.rot, self.cos, self.sin, self.seg_col, self.seg_row = rot, cos, sin, seg_col, seg_row
        self.cot, self.mixed, self.lse, self.out, self.delta, self.dq = cot, mixed, lse, out, delta, dq
        self.blocks = rot.shape[0] // BLOCK

    def part(self, n):
        return aligned((3 * self.pair + n) * PAIR, PAIR)

    def own(self):
        return aligned(self.pair * PAIR, PAIR)

    def prepare(self):
        def some(n, _):
            rows = aligned(n * BLOCK, BLOCK)
            terms = (wide(self.cot[rows, self.own()]) * self.mixed[rows, self.own()]).T
            self.delta[0:1, rows] = jnp.sum(terms[:HEAD_DIM], axis=0, keepdims=True)
            self.delta[1:2, rows] = jnp.sum(terms[HEAD_DIM:], axis=0, keepdims=True)
            self.dq[rows, :] = jnp.zeros((BLOCK, PAIR), jnp.float32)
            return 0

        lax.fori_loop(0, self.blocks, some, 0)

    def visit(self, row, rows_count, col, cols_count, diagonal, dk, dv):
        rows, cols = aligned(row, rows_count), aligned(col, cols_count)
        allowed = self.seg_col[cols, :1] == self.seg_row[:1, rows]
        if diagonal:
            at = lax.broadcasted_iota(jnp.int32, (cols_count, rows_count), 0)
            allowed = allowed & (at <= lax.broadcasted_iota(jnp.int32, (cols_count, rows_count), 1))
        queries, cots = self.rot[rows, self.part(0)], self.cot[rows, self.own()]
        query_heads, cot_heads = split_heads(queries), split_heads(cots)
        key_heads = split_heads(self.rot[cols, self.part(1)])
        value_heads = split_heads(self.rot[cols, self.part(2)])
        total = self.dq[rows, :]
        for h in range(2):
            scores = contract_cols(key_heads[h], queries)
            probs = jnp.where(allowed, jnp.exp(scores - self.lse[self.pair, h : h + 1, rows]), 0.0)
            dv = dv + product(low(probs), cot_heads[h])
            prob_cot = contract_cols(value_heads[h], cots)
            score_cot = low(probs * (prob_cot - self.delta[h : h + 1, rows]))
            dk = dk + product(score_cot, query_heads[h])
            total = total + contract_rows(score_cot, key_heads[h])
        self.dq[rows, :] = total
        return dk, dv

    def unturn(self, grad, rows):
        return low(grad * self.cos[rows, :] + turn(grad * self.sin[rows, :], -1.0))

    def column(self, j):
        start, half = j * BLOCK, BLOCK // 2
        zero = jnp.zeros((half, PAIR), jnp.float32)
        halves = [
            self.visit(start, BLOCK, start, half, True, zero, zero),
            self.visit(start + half, half, start + half, half, True, zero, zero),
        ]
        state = tuple(jnp.concatenate(pair, axis=0) for pair in zip(*halves))

        def one_row(i, state):
            return lax.cond(
                self.follows(i, j),
                lambda state: self.visit(i * BLOCK, BLOCK, start, BLOCK, False, *state),
                lambda state: state,
                state,
            )

        dk, dv = lax.fori_loop(0, self.blocks, one_row, state)
        cols = aligned(start, BLOCK)
        self.out[cols, self.part(1)] = self.unturn(dk, cols)
        self.out[cols, self.part(2)] = low(dv)

    def finish(self):
        def some(n, _):
            rows = aligned(n * BLOCK, BLOCK)
            self.out[rows, self.part(0)] = self.unturn(self.dq[rows, :] * HEAD_DIM**-0.5, rows)
            return 0

        lax.fori_loop(0, self.blocks, some, 0)


def backward_kernel(info, *refs):
    def follows(i, j):
        return (info[0, j] < info[0, i]) & (info[2, j] >= info[1, i])

    back = Backward(0, *refs, follows)
    back.prepare()

    def one_col(j, _):
        back.column(j)
        return 0

    lax.fori_loop(0, back.blocks, one_col, 0)
    back.finish()


def attention_forward(info, qkv, cos, sin, seg_col, seg_row):
    tokens, width = qkv.shape
    pairs = width // (3 * PAIR)
    whole = lambda p, info: (0, 0)
    return pl.pallas_call(
        forward_kernel,
        grid_spec=pltpu.PrefetchScalarGridSpec(
            num_scalar_prefetch=1,
            grid=(pairs,),
            in_specs=[
                pl.BlockSpec((tokens, 3 * PAIR), lambda p, info: (0, p)),
                pl.BlockSpec((tokens, PAIR), whole),
                pl.BlockSpec((tokens, PAIR), whole),
                pl.BlockSpec((tokens, 1), whole),
                pl.BlockSpec((1, tokens), whole),
            ],
            out_specs=[
                pl.BlockSpec((tokens, 3 * PAIR), lambda p, info: (0, p)),
                pl.BlockSpec((tokens, PAIR), lambda p, info: (0, p)),
                pl.BlockSpec((tokens, PAIR), lambda p, info: (0, p)),
                pl.BlockSpec((1, 2, tokens), lambda p, info: (p, 0, 0)),
            ],
            scratch_shapes=[
                pltpu.VMEM((2, BLOCK, PAIR), jnp.float32),
                pltpu.VMEM((2, BLOCK, PAIR), jnp.float32),
                pltpu.VMEM((2, BLOCK, PAIR), jnp.float32),
            ],
        ),
        out_shape=[
            jax.ShapeDtypeStruct((tokens, width), jnp.bfloat16),
            jax.ShapeDtypeStruct((tokens, pairs * PAIR), jnp.bfloat16),
            jax.ShapeDtypeStruct((tokens, pairs * PAIR), jnp.float32),
            jax.ShapeDtypeStruct((pairs, 2, tokens), jnp.float32),
        ],
        compiler_params=pltpu.CompilerParams(vmem_limit_bytes=VMEM_LIMIT),
        cost_estimate=pl.CostEstimate(flops=tokens * tokens * width, bytes_accessed=10 * tokens * width, transcendentals=tokens * tokens * 2 * pairs),
    )(info, qkv, cos, sin, seg_col, seg_row)


def attention_backward(info, rot, cos, sin, seg_col, seg_row, cot, mixed, lse):
    tokens, width = rot.shape
    pairs = width // (3 * PAIR)
    whole = lambda p, info: (0, 0)
    return pl.pallas_call(
        backward_kernel,
        grid_spec=pltpu.PrefetchScalarGridSpec(
            num_scalar_prefetch=1,
            grid=(pairs,),
            in_specs=[
                pl.BlockSpec((tokens, 3 * PAIR), lambda p, info: (0, p)),
                pl.BlockSpec((tokens, PAIR), whole),
                pl.BlockSpec((tokens, PAIR), whole),
                pl.BlockSpec((tokens, 1), whole),
                pl.BlockSpec((1, tokens), whole),
                pl.BlockSpec((tokens, PAIR), lambda p, info: (0, p)),
                pl.BlockSpec((tokens, PAIR), lambda p, info: (0, p)),
                pl.BlockSpec((1, 2, tokens), lambda p, info: (p, 0, 0)),
            ],
            out_specs=pl.BlockSpec((tokens, 3 * PAIR), lambda p, info: (0, p)),
            scratch_shapes=[
                pltpu.VMEM((2, tokens), jnp.float32),
                pltpu.VMEM((tokens, PAIR), jnp.float32),
            ],
        ),
        out_shape=jax.ShapeDtypeStruct((tokens, width), jnp.bfloat16),
        compiler_params=pltpu.CompilerParams(vmem_limit_bytes=VMEM_LIMIT),
        cost_estimate=pl.CostEstimate(flops=3 * tokens * tokens * width, bytes_accessed=10 * tokens * width, transcendentals=tokens * tokens * 2 * pairs),
    )(info, rot, cos, sin, seg_col, seg_row, cot, mixed, lse)


def swap(values, axis, mask):
    size = lax.axis_size(axis)
    return lax.ppermute(values, axis, [(i, i ^ mask) for i in range(size)])


def masks(size):
    return [1 << n for n in reversed(range(size.bit_length() - 1))]


def offsets(size):
    held = [0]
    for mask in masks(size):
        held = held + [at ^ mask for at in held]
    return held


def gather_rows(rows, axis):
    for mask in masks(lax.axis_size(axis)):
        rows = jnp.concatenate([rows, swap(rows, axis, mask)], axis=0)
    return rows


def scatter_rows(make, count, axis):
    todo = list(reversed(masks(lax.axis_size(axis))))
    half = count // 2
    there = swap(low(make(half, count)), axis, todo[0])
    rows = make(0, half) + wide(there)
    for mask in todo[1:]:
        half = rows.shape[0] // 2
        rows = rows[:half] + wide(swap(low(rows[half:]), axis, mask))
    return rows


def scatter_both(make, count):
    rows = scatter_rows(make, count, "ctx")
    size = lax.axis_size("tp")
    me = lax.axis_index("tp")
    for mask in masks(size):
        half = rows.shape[0] // 2
        upper = (me & mask) != 0
        mine = jnp.where(upper, rows[half:], rows[:half])
        other = jnp.where(upper, rows[:half], rows[half:])
        rows = mine + wide(swap(low(other), "tp", mask))
    return rows


def join_tp(rows):
    size = lax.axis_size("tp")
    me = lax.axis_index("tp")
    for mask in reversed(masks(size)):
        upper = (me & mask) != 0
        other = swap(rows, "tp", mask)
        rows = jnp.where(upper, jnp.concatenate([other, rows], 0), jnp.concatenate([rows, other], 0))
    return rows


def own_part(rows):
    size = lax.axis_size("tp")
    count = rows.shape[0] // size
    return lax.dynamic_slice_in_dim(rows, lax.axis_index("tp") * count, count, 0)


MESH = pl.DeviceIdType.MESH
TILE = 512


def fits_kernels():
    return lax.axis_size("ctx") == 4 and lax.axis_size("tp") == 2


class Place:
    def __init__(self):
        me = lax.axis_index("ctx")
        x, core = me // 2, me % 2
        self.tp = lax.axis_index("tp")
        self.x = {"ctx": (1 - x) * 2 + core}
        self.core = {"ctx": x * 2 + 1 - core}
        self.cross = {"ctx": (1 - x) * 2 + 1 - core}
        self.y = {"tp": 1 - self.tp}

    def others(self, axis):
        size, me = lax.axis_size(axis), lax.axis_index(axis)
        return [{axis: (me + n) % size} for n in range(1, size)]


def meet(devices):
    barrier = pltpu.get_barrier_semaphore()
    for device in devices:
        pl.semaphore_signal(barrier, inc=1, device_id=device, device_id_type=MESH)
    pl.semaphore_wait(barrier, len(devices))


class Links:
    def __init__(self, send, recv):
        self.send, self.recv, self.count, self.sent = send, recv, 0, []

    def copy(self, src, dst, device, at=None):
        n = self.count
        self.count += 1
        made = pltpu.make_async_remote_copy(src, dst, self.send.at[n], self.recv.at[n], device_id=device, device_id_type=MESH)
        self.sent.append(made)
        return made

    def drain(self):
        for made in self.sent:
            made.wait_send()


def start_kernel(hidden, grads, segs, gains, attn_in, cot, segs_out, gains_out, hbuf, nbuf, gbuf, gain_row, send, recv, local_sem):
    place, links = Place(), Links(send, recv)
    rows = hidden.shape[0]
    half, quarter = rows // 2, rows // 4
    z = lax.axis_index("fsdp")
    near = [place.x, place.core, place.cross, place.y]
    far = place.others("fsdp")
    meet(near + far)

    def span(block, part, chunk=None):
        if chunk is None:
            return aligned(block * rows + part * half, half)
        return aligned(block * rows + part * half + chunk * quarter, quarter)

    mine, other = place.tp, 1 - place.tp
    tiny = [links.copy(gains, gains_out.at[z], device) for device in far]
    tiny_segs = [links.copy(segs, segs_out.at[n + 1], device) for n, device in enumerate(near[:3])]
    for made in tiny + tiny_segs:
        made.start()
    over_x = {}
    for name, src, dst in (("h", hidden, hbuf), ("g", grads, gbuf)):
        for q in range(2):
            over_x[name, q] = links.copy(src.at[span(0, mine, q)], dst.at[span(1, mine, q)], place.x)
    over_core = {name: links.copy(src, dst.at[aligned(2 * rows, rows)], place.core) for name, src, dst in (("h", hidden, hbuf), ("g", grads, gbuf))}
    for key in (("h", 0), ("h", 1)):
        over_x[key].start()
    over_core["h"].start()
    for key in (("g", 0), ("g", 1)):
        over_x[key].start()
    over_core["g"].start()
    kept = []

    def keep(src, dst):
        made = pltpu.make_async_copy(src, dst, local_sem.at[len(kept)])
        made.start()
        kept.append(made)

    keep(grads, cot.at[aligned(0, rows)])
    gains_out[z] = gains[...]
    segs_out[0] = segs[...]
    for made in tiny:
        made.wait_recv()
    lanes = 128
    groups = gains.shape[0] // 2
    for device in range(gains_out.shape[0]):
        for row in range(groups):
            gain_row[:, pl.ds((device * groups + row) * lanes, lanes)] = gains_out[device, row : row + 1, :]

    def normalize(src, at, block, count):
        def some(n, _):
            there = aligned(at + n * 64, 64)
            values = wide(src[there, :])
            scale = lax.rsqrt(jnp.mean(values * values, axis=1, keepdims=True) + EPS)
            nbuf[aligned(block + n * 64, 64), :] = low(values * scale * gain_row[...])
            return 0

        lax.fori_loop(0, count // 64, some, 0)
        keep(nbuf.at[pl.ds(block, count)], attn_in.at[pl.ds(block, count)])

    normalize(hidden, 0, 0, rows)
    over_y, across, last = {}, {}, {}

    def pass_on(name, buf):
        for q in range(2):
            over_x[name, q].wait_recv()
            over_y[name, q] = links.copy(buf.at[span(1, mine, q)], buf.at[span(1, mine, q)], place.y)
            across[name, q] = links.copy(buf.at[span(1, mine, q)], buf.at[span(3, mine, q)], place.core)
            over_y[name, q].start()
            across[name, q].start()

    def finish(name, buf):
        for q in range(2):
            over_y[name, q].wait_recv()
            last[name, q] = links.copy(buf.at[span(1, other, q)], buf.at[span(3, other, q)], place.core)
            last[name, q].start()

    pass_on("h", hbuf)
    over_core["h"].wait_recv()
    normalize(hbuf, 2 * rows, 2 * rows, rows)
    finish("h", hbuf)
    normalize(hbuf, rows, rows, rows)
    pass_on("g", gbuf)
    for q in range(2):
        across["h", q].wait_recv()
        last["h", q].wait_recv()
    normalize(hbuf, 3 * rows, 3 * rows, rows)
    over_core["g"].wait_recv()
    keep(gbuf.at[aligned(2 * rows, rows)], cot.at[aligned(2 * rows, rows)])
    finish("g", gbuf)
    keep(gbuf.at[aligned(rows, rows)], cot.at[aligned(rows, rows)])
    for q in range(2):
        across["g", q].wait_recv()
        last["g", q].wait_recv()
    keep(gbuf.at[aligned(3 * rows, rows)], cot.at[aligned(3 * rows, rows)])
    for made in tiny_segs:
        made.wait_recv()
    links.drain()
    for made in kept:
        made.wait()


def start_exchange(hidden, grads, segments, attn_gain, mlp_gain):
    rows, width = hidden.shape
    fsdp = lax.axis_size("fsdp")
    segs = jnp.concatenate([segments.reshape(-1, 128), jnp.zeros((8 - rows // 128, 128), jnp.int32)], axis=0)
    gains = wide(jnp.concatenate([attn_gain, mlp_gain])).reshape(-1, 128)
    vmem = pl.BlockSpec(memory_space=pltpu.VMEM)
    hbm = pl.BlockSpec(memory_space=pl.ANY)
    tokens = 4 * rows
    attn_in, cot, segs, gains = pl.pallas_call(
        start_kernel,
        in_specs=[vmem] * 4,
        out_specs=[hbm, hbm, vmem, vmem],
        out_shape=[
            jax.ShapeDtypeStruct((tokens, width), jnp.bfloat16),
            jax.ShapeDtypeStruct((tokens, width), jnp.bfloat16),
            jax.ShapeDtypeStruct((4, 8, 128), jnp.int32),
            jax.ShapeDtypeStruct((fsdp,) + gains.shape, jnp.float32),
        ],
        scratch_shapes=[
            pltpu.VMEM((tokens, width), jnp.bfloat16),
            pltpu.VMEM((tokens, width), jnp.bfloat16),
            pltpu.VMEM((tokens, width), jnp.bfloat16),
            pltpu.VMEM((1, width), jnp.float32),
            pltpu.SemaphoreType.DMA((fsdp + 32,)),
            pltpu.SemaphoreType.DMA((fsdp + 32,)),
            pltpu.SemaphoreType.DMA((8,)),
        ],
        compiler_params=pltpu.CompilerParams(collective_id=0, has_side_effects=True, vmem_limit_bytes=VMEM_LIMIT),
        cost_estimate=pl.CostEstimate(flops=0, bytes_accessed=200_000_000, transcendentals=0),
    )(hidden, grads, segs, gains)
    segs = segs[:, : rows // 128].reshape(tokens)
    gains = jnp.transpose(gains.reshape(fsdp, 2, -1), (1, 0, 2)).reshape(2, width)
    return attn_in, cot, segs, gains


def scatter_scratch(rows, width):
    part, half = rows // 8, width // 2
    return [
        pltpu.VMEM((4, part, width), jnp.bfloat16),
        pltpu.VMEM((4, part, width), jnp.bfloat16),
        pltpu.VMEM((6, part, half), jnp.bfloat16),
        pltpu.VMEM((6, part, half), jnp.bfloat16),
        pltpu.VMEM((2, part, half), jnp.float32),
        pltpu.VMEM((part, width), jnp.float32),
        pltpu.SemaphoreType.DMA((14,)),
        pltpu.SemaphoreType.DMA((14,)),
    ]


class Scatter:
    def __init__(self, place, make, count, refs, first=("x", "y")):
        self.place, self.make = place, make
        self.hi, self.core_in, self.out, self.come, self.wait, self.total, send, recv = refs
        self.part = count // 8
        self.half = self.total.shape[1] // 2
        self.links = Links(send, recv)
        self.core = {}
        for side in range(2):
            cols = pl.ds(side * self.half, self.half)
            for n in range(4):
                self.core[n, side] = self.links.copy(self.hi.at[n, :, cols], self.core_in.at[n, :, cols], place.core)
        self.send, self.away, self.stays = [], {}, {}
        for side, link in enumerate(first):
            to, then = (place.x, place.y) if link == "x" else (place.y, place.x)
            for n, device in enumerate((to, to, then)):
                at = 3 * side + n
                self.send.append(self.links.copy(self.out.at[at], self.come.at[at], device))
            second, stay = (1, 2) if link == "x" else (2, 1)
            self.away[0, side], self.away[second, side] = 3 * side, 3 * side + 1
            self.stays[side] = stay

    def rows(self, n):
        tp = self.place.tp
        part = (1 - tp) + (n % 2) * (2 * tp - 1)
        return ((1 - n // 2) * 2 + part) * self.part

    def columns(self, side, each):
        tiles = self.half // TILE

        def one(n, _):
            each(aligned(side * self.half + n * TILE, TILE), aligned(n * TILE, TILE))
            return 0

        lax.fori_loop(0, tiles, one, 0)

    def to_core(self, n, side):
        rows = aligned(4 * self.part + self.rows(n), self.part)

        def each(cols, _):
            self.hi[n, :, cols] = low(self.make(rows, cols))

        self.columns(side, each)
        self.core[n, side].start()

    def to_links(self, n, side):
        rows = aligned(self.rows(n), self.part)
        self.core[n, side].wait_recv()

        def each(cols, at):
            value = self.make(rows, cols) + wide(self.core_in[n, :, cols])
            if (n, side) in self.away:
                self.out[self.away[n, side], :, at] = low(value)
            elif n == 3:
                self.total[:, cols] = value
            else:
                self.wait[side, :, at] = value

        self.columns(side, each)
        if (n, side) in self.away:
            self.send[self.away[n, side]].start()

    def units(self):
        return (
            [(0, side) for side in range(2)]
            + [(n, side) for n in (1, 2) for side in range(2) if (n, side) in self.away]
            + [(self.stays[side], side) for side in range(2)]
            + [(3, side) for side in range(2)]
        )

    def start(self):
        units = self.units()
        ahead = 2
        for unit in units[:ahead]:
            self.to_core(*unit)
        for at, unit in enumerate(units):
            self.to_links(*unit)
            if at + ahead < len(units):
                self.to_core(*units[at + ahead])

    def turn(self):
        for side in range(2):
            came, goes = 3 * side, 3 * side + 2
            self.send[came].wait_recv()

            def each(_, at):
                self.out[goes, :, at] = low(self.wait[side, :, at] + wide(self.come[came, :, at]))

            self.columns(side, each)
            self.send[goes].start()

    def finish(self):
        for side in range(2):
            for n in (1, 2):
                self.send[3 * side + n].wait_recv()
            cols = pl.ds(side * self.half, self.half)
            self.total[:, cols] = self.total[:, cols] + wide(self.come[3 * side + 1]) + wide(self.come[3 * side + 2])
        self.links.drain()


def gather_plane(place, links, mine, full, part):
    half = mine.shape[1] // 2
    left, right = pl.ds(0, half), pl.ds(half, half)
    own, other = place.tp, 1 - place.tp

    def rows(block, tp):
        return aligned((block * 2 + tp) * part, part)

    y_left = links.copy(mine.at[:, left], full.at[rows(0, own), left], place.y)
    x_right = links.copy(mine.at[:, right], full.at[rows(1, own), right], place.x)
    y_right = links.copy(mine.at[:, right], full.at[rows(0, own), right], place.y)
    x_left = links.copy(mine.at[:, left], full.at[rows(1, own), left], place.x)
    core = [links.copy(mine, full.at[rows(2, own)], place.core)]
    for made in (y_left, x_right, y_right, x_left, core[0]):
        made.start()
    waits = []

    def relay(come, block, tp, cols, onward=None):
        come.wait_recv()
        here = full.at[rows(block, tp), cols]
        if onward == "x":
            made = links.copy(here, full.at[rows(1, tp), cols], place.x)
        elif onward == "y":
            made = links.copy(here, full.at[rows(block, tp), cols], place.y)
        if onward:
            made.start()
        over = links.copy(here, full.at[rows(block + 2, tp), cols], place.core)
        over.start()
        core.append(over)
        return made if onward else None

    far_left = relay(y_left, 0, other, left, "x")
    far_right = relay(x_right, 1, own, right, "y")
    relay(y_right, 0, other, right)
    relay(x_left, 1, own, left)
    relay(far_left, 1, other, left)
    relay(far_right, 1, other, right)
    for made in core:
        made.wait_recv()


def own_rows_of(ref, place, part):
    return ref[aligned(place.tp * part, part), :]


def forward_mid_kernel(mixed, weight, hidden, gain, full, resid_out, mine, *refs):
    place = Place()
    scatter_refs, (send, recv, local_sem) = refs[:-3], refs[-3:]
    count = mixed.shape[0]
    part = count // 8
    meet([place.x, place.core, place.y])
    scatter = Scatter(place, lambda rows, cols: contract_cols(mixed[rows, :], weight[cols, weight.shape[1] - mixed.shape[1] :]), count, scatter_refs)
    scatter.start()
    scatter.turn()
    scatter.finish()
    step = 64

    def some(n, _):
        rows = aligned(n * step, step)
        values = wide(hidden[aligned(place.tp * part + n * step, step), :]) + scatter.total[rows, :]
        resid_out[rows, :] = values
        scale = lax.rsqrt(jnp.mean(values * values, axis=1, keepdims=True) + EPS)
        mine[rows, :] = low(values * scale * gain[...])
        return 0

    lax.fori_loop(0, part // step, some, 0)
    stay = pltpu.make_async_copy(mine, full.at[aligned(place.tp * part, part)], local_sem)
    stay.start()
    links = Links(send, recv)
    gather_plane(place, links, mine, full, part)
    links.drain()
    stay.wait()


def mid_scratch(count, width):
    return [pltpu.VMEM((count // 8, width), jnp.bfloat16)] + scatter_scratch(count, width) + [
        pltpu.SemaphoreType.DMA((16,)),
        pltpu.SemaphoreType.DMA((16,)),
        pltpu.SemaphoreType.DMA,
    ]


def forward_mid(mixed, weight, hidden, gain):
    count, width = mixed.shape[0], weight.shape[0]
    vmem = pl.BlockSpec(memory_space=pltpu.VMEM)
    return pl.pallas_call(
        forward_mid_kernel,
        in_specs=[vmem] * 4,
        out_specs=[pl.BlockSpec(memory_space=pl.ANY), vmem],
        out_shape=[jax.ShapeDtypeStruct((count, width), jnp.bfloat16), jax.ShapeDtypeStruct((count // 8, width), jnp.float32)],
        scratch_shapes=mid_scratch(count, width),
        compiler_params=pltpu.CompilerParams(collective_id=1, has_side_effects=True, vmem_limit_bytes=VMEM_LIMIT),
        cost_estimate=pl.CostEstimate(flops=0, bytes_accessed=300_000_000, transcendentals=0),
    )(mixed, weight, hidden, gain[None, :])


def norm_back(values, scale, gain, cot):
    scaled = cot * gain
    lean = jnp.mean(values * scaled, axis=1, keepdims=True)
    return scale * scaled - values * (scale * scale * scale) * lean, cot * (values * scale)


def backward_mid_kernel(gate_cot, up_cot, weights, resid, grads, gain, full, cot_out, gain_out, mine, *refs):
    place = Place()
    scatter_refs, (send, recv, local_sem) = refs[:-3], refs[-3:]
    count, hidden_cols = gate_cot.shape
    part = count // 8
    meet([place.x, place.core, place.y])

    def make(rows, cols):
        return contract_cols(gate_cot[rows, :], weights[cols, :hidden_cols]) + contract_cols(up_cot[rows, :], weights[cols, hidden_cols:])

    scatter = Scatter(place, make, count, scatter_refs)
    scatter.start()
    scatter.turn()
    scatter.finish()
    step = 32

    def some(n, sums):
        rows = aligned(n * step, step)
        values = resid[rows, :]
        scale = lax.rsqrt(jnp.mean(values * values, axis=1, keepdims=True) + EPS)
        back, terms = norm_back(values, scale, gain[...], scatter.total[rows, :])
        cot = wide(grads[aligned(place.tp * part + n * step, step), :]) + back
        cot_out[rows, :] = cot
        mine[rows, :] = low(cot)
        return sums + jnp.sum(terms, axis=0, keepdims=True)

    gain_out[...] = lax.fori_loop(0, part // step, some, jnp.zeros(gain.shape, jnp.float32))
    stay = pltpu.make_async_copy(mine, full.at[aligned(place.tp * part, part)], local_sem)
    stay.start()
    links = Links(send, recv)
    gather_plane(place, links, mine, full, part)
    links.drain()
    stay.wait()


def backward_mid(gate_cot, up_cot, weights, resid, grads, gain):
    count, width = gate_cot.shape[0], weights.shape[0]
    vmem = pl.BlockSpec(memory_space=pltpu.VMEM)
    return pl.pallas_call(
        backward_mid_kernel,
        in_specs=[vmem] * 6,
        out_specs=[pl.BlockSpec(memory_space=pl.ANY), vmem, vmem],
        out_shape=[
            jax.ShapeDtypeStruct((count, width), jnp.bfloat16),
            jax.ShapeDtypeStruct((count // 8, width), jnp.float32),
            jax.ShapeDtypeStruct((1, width), jnp.float32),
        ],
        scratch_shapes=mid_scratch(count, width),
        compiler_params=pltpu.CompilerParams(collective_id=2, has_side_effects=True, vmem_limit_bytes=VMEM_LIMIT),
        cost_estimate=pl.CostEstimate(flops=0, bytes_accessed=300_000_000, transcendentals=0),
    )(gate_cot, up_cot, weights, resid, grads, gain[None, :])


def input_kernel(cots, weights, resid_cot, hidden, gain, gain_two, grad_out, gains_out, sums, come, *refs):
    place = Place()
    (send, recv), refs = refs[-2:], refs[:-2]
    count = cots.shape[0]
    part = count // 8
    meet([place.x, place.core, place.y] + place.others("fsdp"))
    scatter = Scatter(place, lambda rows, cols: contract_cols(cots[rows, :], weights[cols, : cots.shape[1]]), count, refs, ("y", "y"))
    links = Links(send, recv)
    scatter.start()
    scatter.turn()
    scatter.finish()
    step = 32

    def some(n, total):
        rows = aligned(n * step, step)
        values = wide(hidden[aligned(place.tp * part + n * step, step), :])
        scale = lax.rsqrt(jnp.mean(values * values, axis=1, keepdims=True) + EPS)
        back, terms = norm_back(values, scale, gain[...], scatter.total[rows, :])
        grad_out[rows, :] = low(resid_cot[rows, :] + back)
        return total + jnp.sum(terms, axis=0, keepdims=True)

    sums[0, 0:1, :] = lax.fori_loop(0, part // step, some, jnp.zeros(gain.shape, jnp.float32))
    sums[0, 1:2, :] = gain_two[...]
    near = [place.x, place.core, place.y]
    for n, device in enumerate(near):
        made = links.copy(sums.at[n], come.at[n], device)
        made.start()
        made.wait_recv()
        sums[n + 1] = sums[n] + come[n]
    at = len(near)
    far = [links.copy(sums.at[at], come.at[at + n], device) for n, device in enumerate(place.others("fsdp"))]
    for made in far:
        made.start()
    total = sums[at]
    for n, made in enumerate(far):
        made.wait_recv()
        total = total + come[at + n]
    gains_out[...] = total
    links.drain()


def input_exchange(cots, weights, resid_cot, hidden, gain, gain_two):
    count, width = cots.shape[0], weights.shape[0]
    fsdp = lax.axis_size("fsdp")
    vmem = pl.BlockSpec(memory_space=pltpu.VMEM)
    return pl.pallas_call(
        input_kernel,
        in_specs=[vmem] * 6,
        out_specs=[vmem, vmem],
        out_shape=[jax.ShapeDtypeStruct((count // 8, width), jnp.bfloat16), jax.ShapeDtypeStruct((2, width), jnp.float32)],
        scratch_shapes=[
            pltpu.VMEM((4, 2, width), jnp.float32),
            pltpu.VMEM((2 + fsdp, 2, width), jnp.float32),
        ]
        + scatter_scratch(count, width)
        + [pltpu.SemaphoreType.DMA((4 + fsdp,)), pltpu.SemaphoreType.DMA((4 + fsdp,))],
        compiler_params=pltpu.CompilerParams(collective_id=3, has_side_effects=True, vmem_limit_bytes=VMEM_LIMIT),
        cost_estimate=pl.CostEstimate(flops=0, bytes_accessed=180_000_000, transcendentals=0),
    )(cots, weights, resid_cot, hidden, gain[None, :], gain_two)


def attention_output_kernel(
    rot, cos, sin, seg_col, seg_row, cot, mixed, lse, hidden_act, down, resid, cots, out, delta, dq, *refs
):
    place = Place()
    count = hidden_act.shape[0]
    me = lax.axis_index("ctx")
    blocks = count // BLOCK
    per = count // 4 // BLOCK

    def at(block):
        n = block // per
        return (((me // 2 + n % 2) % 2) * 2 + (me % 2 + n // 2) % 2) * per + block % per

    def follows(i, j):
        return (at(j) < at(i)) & (at(i) - at(j) <= blocks // 2)

    meet([place.x, place.core, place.y])
    scatter = Scatter(place, lambda rows, cols: product(hidden_act[rows, :], down[:, cols]), count, refs, ("y", "y"))
    scatter.start()
    pairs = rot.shape[1] // (3 * PAIR)
    steps = pairs * blocks

    def step(n, _):
        back = Backward(n // blocks, rot, cos, sin, seg_col, seg_row, cot, mixed, lse, cots, delta, dq, follows)

        @pl.when(n % blocks == 0)
        def _():
            back.prepare()

        back.column(n % blocks)

        @pl.when(n % blocks == blocks - 1)
        def _():
            back.finish()

        @pl.when(n == steps // 4 - 1)
        def _():
            scatter.turn()

        return 0

    lax.fori_loop(0, steps, step, 0)
    scatter.finish()
    out[...] = low(resid[...] + scatter.total[...])


def attention_output(rot, cos, sin, seg_col, seg_row, cot, mixed, lse, hidden_act, down, resid):
    count, width = hidden_act.shape[0], down.shape[1]
    vmem = pl.BlockSpec(memory_space=pltpu.VMEM)
    return pl.pallas_call(
        attention_output_kernel,
        in_specs=[vmem] * 11,
        out_specs=[vmem, vmem],
        out_shape=[
            jax.ShapeDtypeStruct(rot.shape, jnp.bfloat16),
            jax.ShapeDtypeStruct((count // 8, width), jnp.bfloat16),
        ],
        scratch_shapes=[
            pltpu.VMEM((2, count), jnp.float32),
            pltpu.VMEM((count, PAIR), jnp.float32),
        ]
        + scatter_scratch(count, width),
        compiler_params=pltpu.CompilerParams(collective_id=4, has_side_effects=True, vmem_limit_bytes=VMEM_LIMIT),
        cost_estimate=pl.CostEstimate(flops=0, bytes_accessed=220_000_000, transcendentals=0),
    )(rot, cos, sin, seg_col, seg_row, cot, mixed, lse, hidden_act, down, resid)


def take_attention_kernel(at, query, key, value, out, taken):
    pairs = query.shape[1] // PAIR
    for p in range(pairs):
        for n, part in enumerate((query, key, value)):
            taken[:, (3 * p + n) * PAIR : (3 * p + n + 1) * PAIR] = part[:, p * PAIR : (p + 1) * PAIR]
    taken[:, 3 * pairs * PAIR :] = out[...].T


def take_attention(me, query, key, value, out, count):
    depth = query.shape[0]
    block = pl.BlockSpec((depth, count), lambda n, at: (0, at[0]))
    return pl.pallas_call(
        take_attention_kernel,
        grid_spec=pltpu.PrefetchScalarGridSpec(
            num_scalar_prefetch=1,
            grid=(1,),
            in_specs=[block] * 3 + [pl.BlockSpec((count, depth), lambda n, at: (at[0], 0))],
            out_specs=pl.BlockSpec((depth, 4 * count), lambda n, at: (0, 0)),
        ),
        out_shape=jax.ShapeDtypeStruct((depth, 4 * count), query.dtype),
        compiler_params=pltpu.CompilerParams(vmem_limit_bytes=VMEM_LIMIT),
    )(me, query, key, value, out)


def take_hidden_kernel(at, gate, up, down, both, rows):
    count = gate.shape[1]
    both[:, :count] = gate[...]
    both[:, count:] = up[...]
    rows[...] = down[...]


def take_hidden(me, gate, up, down, count):
    depth = gate.shape[0]
    block = pl.BlockSpec((depth, count), lambda n, at: (0, at[0]))
    return pl.pallas_call(
        take_hidden_kernel,
        grid_spec=pltpu.PrefetchScalarGridSpec(
            num_scalar_prefetch=1,
            grid=(1,),
            in_specs=[block] * 2 + [pl.BlockSpec((count, depth), lambda n, at: (at[0], 0))],
            out_specs=[pl.BlockSpec((depth, 2 * count), lambda n, at: (0, 0)), pl.BlockSpec((count, depth), lambda n, at: (0, 0))],
        ),
        out_shape=[jax.ShapeDtypeStruct((depth, 2 * count), gate.dtype), jax.ShapeDtypeStruct((count, depth), down.dtype)],
        compiler_params=pltpu.CompilerParams(vmem_limit_bytes=VMEM_LIMIT),
    )(me, gate, up, down)


def first_swaps(block):
    pieces = [block]
    for mask in masks(lax.axis_size("ctx"))[:-1]:
        pieces = pieces + [swap(piece, "ctx", mask) for piece in pieces]
    return pieces


def last_swap(pieces):
    return pieces + [swap(piece, "ctx", 1) for piece in pieces]


def order_of_pieces():
    return lax.axis_index("ctx") ^ jnp.array(offsets(lax.axis_size("ctx")), jnp.int32)


def place_kernel(at, *refs):
    out = refs[-1]
    for n, piece in enumerate(refs[:-1]):

        @pl.when(pl.program_id(0) == n)
        def _():
            out[...] = wide(piece[...])


def place_pieces(pieces, axis):
    block = pieces[0].shape
    shape = list(block)
    shape[axis] *= len(pieces)
    return pl.pallas_call(
        place_kernel,
        grid_spec=pltpu.PrefetchScalarGridSpec(
            num_scalar_prefetch=1,
            grid=(len(pieces),),
            in_specs=[pl.BlockSpec(block, lambda n, at: (0, 0))] * len(pieces),
            out_specs=pl.BlockSpec(block, lambda n, at: (at[n], 0) if axis == 0 else (0, at[n])),
        ),
        out_shape=jax.ShapeDtypeStruct(shape, jnp.float32),
        compiler_params=pltpu.CompilerParams(vmem_limit_bytes=VMEM_LIMIT),
        cost_estimate=pl.CostEstimate(flops=0, bytes_accessed=6 * math.prod(shape), transcendentals=0),
    )(order_of_pieces(), *pieces)


def place_attention_kernel(at, *refs):
    pieces, outs = refs[:-4], refs[-4:]
    count = outs[0].shape[1]
    pairs = count // PAIR
    for n, piece in enumerate(pieces):

        @pl.when(pl.program_id(0) == n)
        def _():
            for p in range(pairs):
                for m in range(3):
                    outs[m][:, p * PAIR : (p + 1) * PAIR] = wide(piece[:, (3 * p + m) * PAIR : (3 * p + m + 1) * PAIR])
            outs[3][...] = wide(piece[:, 3 * count :]).T


def place_attention(pieces):
    depth, count = pieces[0].shape[0], pieces[0].shape[1] // 4
    whole = len(pieces) * count
    side = pl.BlockSpec((depth, count), lambda n, at: (0, at[n]))
    return pl.pallas_call(
        place_attention_kernel,
        grid_spec=pltpu.PrefetchScalarGridSpec(
            num_scalar_prefetch=1,
            grid=(len(pieces),),
            in_specs=[pl.BlockSpec(pieces[0].shape, lambda n, at: (0, 0))] * len(pieces),
            out_specs=[side] * 3 + [pl.BlockSpec((count, depth), lambda n, at: (at[n], 0))],
        ),
        out_shape=[jax.ShapeDtypeStruct((depth, whole), jnp.float32)] * 3 + [jax.ShapeDtypeStruct((whole, depth), jnp.float32)],
        compiler_params=pltpu.CompilerParams(vmem_limit_bytes=VMEM_LIMIT),
        cost_estimate=pl.CostEstimate(flops=0, bytes_accessed=24 * depth * whole, transcendentals=0),
    )(order_of_pieces(), *pieces)


def local(
    hidden_in,
    out_grad,
    segment_ids,
    attn_gain,
    w_query,
    w_key,
    w_value,
    w_out,
    mlp_gain,
    w_gate,
    w_up,
    w_down,
):
    group = lax.axis_size("ctx")
    me = lax.axis_index("ctx")
    local_rows = hidden_in.shape[1]
    tokens = local_rows * group
    head_cols = w_query.shape[1] // group
    pairs = head_cols // PAIR
    ff_cols = w_gate.shape[1] // group

    def gather(weight, axis):
        return lax.all_gather(weight, "fsdp", axis=axis, tiled=True)

    def settle(part, axis):
        return lax.psum_scatter(part, "fsdp", scatter_dimension=axis, tiled=True)

    at = me[None]
    w_attn = gather(take_attention(at, w_query, w_key, w_value, w_out, head_cols), 0)
    qkv_cols = 3 * head_cols
    w_qkv, w_out_t = w_attn[:, :qkv_cols], w_attn[:, qkv_cols:]
    own_gate_up, own_down = take_hidden(at, w_gate, w_up, w_down, ff_cols)
    full_gate_up = gather(own_gate_up, 0)
    full_down = gather(own_down, 1)

    kernels = fits_kernels()
    if kernels:
        attn_in, branch_cot, segments, gains = start_exchange(hidden_in[0], out_grad[0], segment_ids[0], attn_gain, mlp_gain)
        gain_one, gain_two = gains[0], gains[1]
    else:
        gains = wide(gather(jnp.stack([attn_gain, mlp_gain]), 1))
        gain_one, gain_two = gains[0], gains[1]
        rows_in = wide(hidden_in[0])
        r1 = lax.rsqrt(jnp.mean(rows_in * rows_in, axis=-1, keepdims=True) + EPS)
        attn_in = gather_rows(low(rows_in * r1 * gain_one), "ctx")
        segments = gather_rows(segment_ids[0], "ctx")
        branch_cot = gather_rows(out_grad[0], "ctx")

    firsts = jnp.stack([(me ^ at) * local_rows for at in offsets(group)])
    positions = (firsts[:, None] + jnp.arange(local_rows, dtype=jnp.int32)[None, :]).reshape(tokens)
    exponents = jnp.arange(0, HEAD_DIM, 2).astype(jnp.float32) / HEAD_DIM
    inverse = jnp.float32(ROPE_BASE) ** (-exponents)
    angles = positions.astype(jnp.float32)[:, None] * inverse[None, :]
    cos = jnp.tile(jnp.cos(angles), (1, 4))
    sin = jnp.tile(jnp.sin(angles), (1, 4))
    info = jnp.stack([positions[::BLOCK], segments[::BLOCK], segments[BLOCK - 1 :: BLOCK]])
    seg_col, seg_row = segments[:, None], segments[None, :]

    qkv = product(attn_in, w_qkv)
    rot, mixed, mixed_wide, lse = attention_forward(info, qkv, cos, sin, seg_col, seg_row)

    own_in = wide(own_part(hidden_in[0]))
    if kernels:
        mlp_in, resid = forward_mid(mixed, w_attn, hidden_in[0], gain_two)
    else:
        part = scatter_both(lambda lo, hi: contract_cols(mixed[lo:hi], w_out_t), tokens)
        resid = own_in + part
        r2 = lax.rsqrt(jnp.mean(resid * resid, axis=-1, keepdims=True) + EPS)
        mlp_in = gather_rows(join_tp(low(resid * r2 * gain_two)), "ctx")
    acts = product(mlp_in, full_gate_up)
    gate_act, up_act = acts[:, :ff_cols], acts[:, ff_cols:]
    sigmoid = jax.nn.sigmoid(gate_act)
    hidden = low(gate_act * sigmoid * up_act)
    gate_slope = low(up_act * sigmoid * (1.0 + gate_act * (1.0 - sigmoid)))
    up_slope = low(gate_act * sigmoid)
    hidden, gate_slope, up_slope = lax.optimization_barrier((hidden, gate_slope, up_slope))
    down_part = low(contract_rows(hidden, branch_cot))
    down_part, full_down, branch_cot = lax.optimization_barrier((down_part, full_down, branch_cot))
    down_own = settle(down_part, 1)

    hidden_cot = contract_cols(branch_cot, full_down)
    gate_cot = low(hidden_cot * gate_slope)
    up_cot = low(hidden_cot * up_slope)
    gate_part = low(contract_rows(mlp_in, gate_cot))
    up_part = low(contract_rows(mlp_in, up_cot))
    gate_own = settle(gate_part, 0)
    up_own = settle(up_part, 0)
    if kernels:
        gate_cot, up_cot, gate_part, up_part = lax.optimization_barrier((gate_cot, up_cot, gate_part, up_part))
        attn_cot, resid_cot, gain_two_part = backward_mid(gate_cot, up_cot, full_gate_up, resid, out_grad[0], gain_two)
    else:
        mlp_in_cot = scatter_both(
            lambda lo, hi: contract_cols(gate_cot[lo:hi], full_gate_up[:, :ff_cols])
            + contract_cols(up_cot[lo:hi], full_gate_up[:, ff_cols:]),
            tokens,
        )
        back, terms = norm_back(resid, r2, gain_two, mlp_in_cot)
        gain_two_part = jnp.sum(terms, axis=0, keepdims=True)
        resid_cot = wide(own_part(out_grad[0])) + back
        attn_cot = gather_rows(join_tp(low(resid_cot)), "ctx")
    mixed_cot = low(product(attn_cot, w_out_t))
    out_part = low(contract_rows(attn_cot, mixed))
    mixed_cot, down_own = lax.optimization_barrier((mixed_cot, down_own))
    mixed_cot, out_part, gate_own = lax.optimization_barrier((mixed_cot, out_part, gate_own))
    down_pieces, gate_pieces = first_swaps(down_own), first_swaps(gate_own)
    count = len(down_pieces)
    if kernels:
        cots, output = attention_output(rot, cos, sin, seg_col, seg_row, mixed_cot, mixed_wide, lse, hidden, full_down, resid)
    else:
        cots = attention_backward(info, rot, cos, sin, seg_col, seg_row, mixed_cot, mixed_wide, lse)
    cots, *pieces = lax.optimization_barrier((cots, *down_pieces, *gate_pieces))
    down_pieces, gate_pieces = pieces[:count], pieces[count:]
    attn_part = jnp.concatenate([low(contract_rows(attn_in, cots)), out_part], axis=1)
    attn_own = settle(attn_part, 0)
    if kernels:
        cots, attn_part, up_own = lax.optimization_barrier((cots, attn_part, up_own))
        up_pieces = first_swaps(up_own)
        input_grad, gain_sums = input_exchange(cots, w_attn, resid_cot, hidden_in[0], gain_one, gain_two_part)
        input_grad, output, *up_pieces = lax.optimization_barrier((input_grad, output, *up_pieces))
        output, input_grad = join_tp(output), join_tp(input_grad)
    else:
        up_pieces = first_swaps(up_own)
        out_sum = scatter_both(lambda lo, hi: product(hidden[lo:hi], full_down), tokens)
        output = join_tp(low(resid + out_sum))
        attn_in_cot = scatter_both(lambda lo, hi: contract_cols(cots[lo:hi], w_qkv), tokens)
        back, terms = norm_back(own_in, own_part(r1), gain_one, attn_in_cot)
        input_grad = join_tp(low(resid_cot + back))
        gain_sums = lax.psum(jnp.concatenate([jnp.sum(terms, axis=0, keepdims=True), gain_two_part]), ("fsdp", "ctx", "tp"))
    attn_pieces = first_swaps(attn_own)
    down_grad = place_pieces(last_swap(down_pieces), 0)
    gate_grad = place_pieces(last_swap(gate_pieces), 1)
    up_grad = place_pieces(last_swap(up_pieces), 1)
    down_grad, gate_grad, up_grad, output, input_grad, *attn_pieces = lax.optimization_barrier(
        (down_grad, gate_grad, up_grad, output, input_grad, *attn_pieces)
    )
    query_grad, key_grad, value_grad, out_proj_grad = place_attention(last_swap(attn_pieces))

    gain_sums = lax.dynamic_slice_in_dim(gain_sums, lax.axis_index("fsdp") * attn_gain.shape[0], attn_gain.shape[0], 1)
    return (
        output[None],
        input_grad[None],
        gain_sums[0],
        query_grad,
        key_grad,
        value_grad,
        out_proj_grad,
        gain_sums[1],
        gate_grad,
        up_grad,
        down_grad,
    )


def solution(mesh):
    weight, gain = P("fsdp", "tp"), P("fsdp")
    rows = P("fsdp", "ctx", None)
    in_specs = (rows, rows, P("fsdp", "ctx"), gain, weight, weight, weight, P("tp", "fsdp"), gain, weight, weight, P("tp", "fsdp"))
    out_specs = (rows, rows, gain, weight, weight, weight, P("tp", "fsdp"), gain, weight, weight, P("tp", "fsdp"))
    return jax.shard_map(local, mesh=mesh, in_specs=in_specs, out_specs=out_specs, check_vma=False)
```

```python
import math

import jax
import jax.numpy as jnp
from jax import lax
from jax.experimental import pallas as pl
from jax.experimental.pallas import tpu as pltpu
from jax.sharding import PartitionSpec as P


HEAD_DIM = 64
EPS = 1e-05
ROPE_BASE = 130000.0
MASKED = -1e30
PAIR = 2 * HEAD_DIM
BLOCK = 512
VMEM_LIMIT = 60 * 1024 * 1024


def low(values):
    return values.astype(jnp.bfloat16)


def wide(values):
    return values.astype(jnp.float32)


def product(a, b):
    return jnp.dot(a, b, preferred_element_type=jnp.float32)


def contract_rows(a, b):
    return lax.dot_general(a, b, (((0,), (0,)), ((), ())), preferred_element_type=jnp.float32)


def contract_cols(a, b):
    return lax.dot_general(a, b, (((1,), (1,)), ((), ())), preferred_element_type=jnp.float32)


def aligned(start, count):
    return pl.ds(pl.multiple_of(start, count), count)


def first_head():
    return lax.broadcasted_iota(jnp.int32, (1, PAIR), 1) < HEAD_DIM


def split_heads(rows):
    zero = jnp.zeros_like(rows)
    mask = first_head()
    return jnp.where(mask, rows, zero), jnp.where(mask, zero, rows)


def turn(rows, sign):
    half = HEAD_DIM // 2
    lanes = lax.broadcasted_iota(jnp.int32, (1, PAIR), 1)
    up = pltpu.roll(rows, PAIR - half, 1)
    down = pltpu.roll(rows, half, 1)
    return jnp.where(lanes % HEAD_DIM < half, -sign * up, sign * down)


def forward_kernel(info, qkv_ref, cos_ref, sin_ref, seg_col, seg_row, rot_ref, out_ref, wide_ref, lse_ref, best, total, acc):
    blocks = qkv_ref.shape[0] // BLOCK

    def prepare(n, _):
        rows = pl.ds(pl.multiple_of(n * BLOCK, BLOCK), BLOCK)
        cos, sin = cos_ref[rows, :], sin_ref[rows, :]
        q = qkv_ref[rows, :PAIR]
        k = qkv_ref[rows, PAIR : 2 * PAIR]
        rot_ref[rows, :PAIR] = low(low(q * cos + turn(q, 1.0) * sin) * jnp.bfloat16(HEAD_DIM**-0.5))
        rot_ref[rows, PAIR : 2 * PAIR] = low(k * cos + turn(k, 1.0) * sin)
        rot_ref[rows, 2 * PAIR :] = low(qkv_ref[rows, 2 * PAIR :])
        return 0

    lax.fori_loop(0, blocks, prepare, 0)

    def visit(i, j, diagonal):
        rows = pl.ds(pl.multiple_of(i * BLOCK, BLOCK), BLOCK)
        cols = pl.ds(pl.multiple_of(j * BLOCK, BLOCK), BLOCK)
        allowed = seg_col[rows, :1] == seg_row[:1, cols]
        if diagonal:
            at = lax.broadcasted_iota(jnp.int32, (BLOCK, BLOCK), 0)
            allowed = allowed & (at >= lax.broadcasted_iota(jnp.int32, (BLOCK, BLOCK), 1))
        keys = rot_ref[cols, PAIR : 2 * PAIR]
        values = rot_ref[cols, 2 * PAIR :]
        for h, q in enumerate(split_heads(rot_ref[rows, :PAIR])):
            scores = jnp.where(allowed, contract_cols(q, keys), MASKED)
            top = jnp.max(scores, axis=1, keepdims=True)
            if diagonal:
                p = jnp.exp(scores - top)
                best[h] = jnp.broadcast_to(top, (BLOCK, PAIR))
                total[h] = jnp.broadcast_to(jnp.sum(p, axis=1, keepdims=True), (BLOCK, PAIR))
                acc[h] = product(low(p), values)
            else:
                old = best[h][:, :1]
                new = jnp.maximum(old, top)
                fade = jnp.exp(old - new)
                p = jnp.exp(scores - new)
                best[h] = jnp.broadcast_to(new, (BLOCK, PAIR))
                total[h] = total[h] * fade + jnp.sum(p, axis=1, keepdims=True)
                acc[h] = acc[h] * fade + product(low(p), values)

    def one_row(i, _):
        rows = pl.ds(pl.multiple_of(i * BLOCK, BLOCK), BLOCK)
        visit(i, i, True)

        def one_col(j, _):
            @pl.when((info[0, j] < info[0, i]) & (info[2, j] >= info[1, i]))
            def _():
                visit(i, j, False)

            return 0

        lax.fori_loop(0, blocks, one_col, 0)
        mixed = jnp.where(first_head(), acc[0] / total[0], acc[1] / total[1])
        out_ref[rows, :] = low(mixed)
        wide_ref[rows, :] = mixed
        for h in range(2):
            lse_ref[0, h : h + 1, rows] = (best[h] + jnp.log(total[h])).T[:1, :]
        return 0

    lax.fori_loop(0, blocks, one_row, 0)


class Backward:
    def __init__(self, pair, rot, cos, sin, seg_col, seg_row, cot, mixed, lse, out, delta, dq, follows):
        self.pair, self.follows = pair, follows
        self.rot, self.cos, self.sin, self.seg_col, self.seg_row = rot, cos, sin, seg_col, seg_row
        self.cot, self.mixed, self.lse, self.out, self.delta, self.dq = cot, mixed, lse, out, delta, dq
        self.blocks = rot.shape[0] // BLOCK

    def part(self, n):
        return aligned((3 * self.pair + n) * PAIR, PAIR)

    def own(self):
        return aligned(self.pair * PAIR, PAIR)

    def prepare(self):
        def some(n, _):
            rows = aligned(n * BLOCK, BLOCK)
            terms = (wide(self.cot[rows, self.own()]) * self.mixed[rows, self.own()]).T
            self.delta[0:1, rows] = jnp.sum(terms[:HEAD_DIM], axis=0, keepdims=True)
            self.delta[1:2, rows] = jnp.sum(terms[HEAD_DIM:], axis=0, keepdims=True)
            self.dq[rows, :] = jnp.zeros((BLOCK, PAIR), jnp.float32)
            return 0

        lax.fori_loop(0, self.blocks, some, 0)

    def visit(self, row, rows_count, col, cols_count, diagonal, dk, dv):
        rows, cols = aligned(row, rows_count), aligned(col, cols_count)
        allowed = self.seg_col[cols, :1] == self.seg_row[:1, rows]
        if diagonal:
            at = lax.broadcasted_iota(jnp.int32, (cols_count, rows_count), 0)
            allowed = allowed & (at <= lax.broadcasted_iota(jnp.int32, (cols_count, rows_count), 1))
        queries, cots = self.rot[rows, self.part(0)], self.cot[rows, self.own()]
        query_heads, cot_heads = split_heads(queries), split_heads(cots)
        key_heads = split_heads(self.rot[cols, self.part(1)])
        value_heads = split_heads(self.rot[cols, self.part(2)])
        total = self.dq[rows, :]
        for h in range(2):
            scores = contract_cols(key_heads[h], queries)
            probs = jnp.where(allowed, jnp.exp(scores - self.lse[self.pair, h : h + 1, rows]), 0.0)
            dv = dv + product(low(probs), cot_heads[h])
            prob_cot = contract_cols(value_heads[h], cots)
            score_cot = low(probs * (prob_cot - self.delta[h : h + 1, rows]))
            dk = dk + product(score_cot, query_heads[h])
            total = total + contract_rows(score_cot, key_heads[h])
        self.dq[rows, :] = total
        return dk, dv

    def unturn(self, grad, rows):
        return low(grad * self.cos[rows, :] + turn(grad * self.sin[rows, :], -1.0))

    def column(self, j):
        start, half = j * BLOCK, BLOCK // 2
        zero = jnp.zeros((half, PAIR), jnp.float32)
        halves = [
            self.visit(start, BLOCK, start, half, True, zero, zero),
            self.visit(start + half, half, start + half, half, True, zero, zero),
        ]
        state = tuple(jnp.concatenate(pair, axis=0) for pair in zip(*halves))

        def one_row(i, state):
            return lax.cond(
                self.follows(i, j),
                lambda state: self.visit(i * BLOCK, BLOCK, start, BLOCK, False, *state),
                lambda state: state,
                state,
            )

        dk, dv = lax.fori_loop(0, self.blocks, one_row, state)
        cols = aligned(start, BLOCK)
        self.out[cols, self.part(1)] = self.unturn(dk, cols)
        self.out[cols, self.part(2)] = low(dv)

    def finish(self):
        def some(n, _):
            rows = aligned(n * BLOCK, BLOCK)
            self.out[rows, self.part(0)] = self.unturn(self.dq[rows, :] * HEAD_DIM**-0.5, rows)
            return 0

        lax.fori_loop(0, self.blocks, some, 0)


def backward_kernel(info, *refs):
    def follows(i, j):
        return (info[0, j] < info[0, i]) & (info[2, j] >= info[1, i])

    back = Backward(0, *refs, follows)
    back.prepare()

    def one_col(j, _):
        back.column(j)
        return 0

    lax.fori_loop(0, back.blocks, one_col, 0)
    back.finish()


def attention_forward(info, qkv, cos, sin, seg_col, seg_row):
    tokens, width = qkv.shape
    pairs = width // (3 * PAIR)
    whole = lambda p, info: (0, 0)
    return pl.pallas_call(
        forward_kernel,
        grid_spec=pltpu.PrefetchScalarGridSpec(
            num_scalar_prefetch=1,
            grid=(pairs,),
            in_specs=[
                pl.BlockSpec((tokens, 3 * PAIR), lambda p, info: (0, p)),
                pl.BlockSpec((tokens, PAIR), whole),
                pl.BlockSpec((tokens, PAIR), whole),
                pl.BlockSpec((tokens, 1), whole),
                pl.BlockSpec((1, tokens), whole),
            ],
            out_specs=[
                pl.BlockSpec((tokens, 3 * PAIR), lambda p, info: (0, p)),
                pl.BlockSpec((tokens, PAIR), lambda p, info: (0, p)),
                pl.BlockSpec((tokens, PAIR), lambda p, info: (0, p)),
                pl.BlockSpec((1, 2, tokens), lambda p, info: (p, 0, 0)),
            ],
            scratch_shapes=[
                pltpu.VMEM((2, BLOCK, PAIR), jnp.float32),
                pltpu.VMEM((2, BLOCK, PAIR), jnp.float32),
                pltpu.VMEM((2, BLOCK, PAIR), jnp.float32),
            ],
        ),
        out_shape=[
            jax.ShapeDtypeStruct((tokens, width), jnp.bfloat16),
            jax.ShapeDtypeStruct((tokens, pairs * PAIR), jnp.bfloat16),
            jax.ShapeDtypeStruct((tokens, pairs * PAIR), jnp.float32),
            jax.ShapeDtypeStruct((pairs, 2, tokens), jnp.float32),
        ],
        compiler_params=pltpu.CompilerParams(vmem_limit_bytes=VMEM_LIMIT),
        cost_estimate=pl.CostEstimate(flops=tokens * tokens * width, bytes_accessed=10 * tokens * width, transcendentals=tokens * tokens * 2 * pairs),
    )(info, qkv, cos, sin, seg_col, seg_row)


def attention_backward(info, rot, cos, sin, seg_col, seg_row, cot, mixed, lse):
    tokens, width = rot.shape
    pairs = width // (3 * PAIR)
    whole = lambda p, info: (0, 0)
    return pl.pallas_call(
        backward_kernel,
        grid_spec=pltpu.PrefetchScalarGridSpec(
            num_scalar_prefetch=1,
            grid=(pairs,),
            in_specs=[
                pl.BlockSpec((tokens, 3 * PAIR), lambda p, info: (0, p)),
                pl.BlockSpec((tokens, PAIR), whole),
                pl.BlockSpec((tokens, PAIR), whole),
                pl.BlockSpec((tokens, 1), whole),
                pl.BlockSpec((1, tokens), whole),
                pl.BlockSpec((tokens, PAIR), lambda p, info: (0, p)),
                pl.BlockSpec((tokens, PAIR), lambda p, info: (0, p)),
                pl.BlockSpec((1, 2, tokens), lambda p, info: (p, 0, 0)),
            ],
            out_specs=pl.BlockSpec((tokens, 3 * PAIR), lambda p, info: (0, p)),
            scratch_shapes=[
                pltpu.VMEM((2, tokens), jnp.float32),
                pltpu.VMEM((tokens, PAIR), jnp.float32),
            ],
        ),
        out_shape=jax.ShapeDtypeStruct((tokens, width), jnp.bfloat16),
        compiler_params=pltpu.CompilerParams(vmem_limit_bytes=VMEM_LIMIT),
        cost_estimate=pl.CostEstimate(flops=3 * tokens * tokens * width, bytes_accessed=10 * tokens * width, transcendentals=tokens * tokens * 2 * pairs),
    )(info, rot, cos, sin, seg_col, seg_row, cot, mixed, lse)


def swap(values, axis, mask):
    size = lax.axis_size(axis)
    return lax.ppermute(values, axis, [(i, i ^ mask) for i in range(size)])


def masks(size):
    return [1 << n for n in reversed(range(size.bit_length() - 1))]


def offsets(size):
    held = [0]
    for mask in masks(size):
        held = held + [at ^ mask for at in held]
    return held


def gather_rows(rows, axis):
    for mask in masks(lax.axis_size(axis)):
        rows = jnp.concatenate([rows, swap(rows, axis, mask)], axis=0)
    return rows


def scatter_rows(make, count, axis):
    todo = list(reversed(masks(lax.axis_size(axis))))
    half = count // 2
    there = swap(low(make(half, count)), axis, todo[0])
    rows = make(0, half) + wide(there)
    for mask in todo[1:]:
        half = rows.shape[0] // 2
        rows = rows[:half] + wide(swap(low(rows[half:]), axis, mask))
    return rows


def scatter_both(make, count):
    rows = scatter_rows(make, count, "ctx")
    size = lax.axis_size("tp")
    me = lax.axis_index("tp")
    for mask in masks(size):
        half = rows.shape[0] // 2
        upper = (me & mask) != 0
        mine = jnp.where(upper, rows[half:], rows[:half])
        other = jnp.where(upper, rows[:half], rows[half:])
        rows = mine + wide(swap(low(other), "tp", mask))
    return rows


def join_tp(rows):
    size = lax.axis_size("tp")
    me = lax.axis_index("tp")
    for mask in reversed(masks(size)):
        upper = (me & mask) != 0
        other = swap(rows, "tp", mask)
        rows = jnp.where(upper, jnp.concatenate([other, rows], 0), jnp.concatenate([rows, other], 0))
    return rows


def own_part(rows):
    size = lax.axis_size("tp")
    count = rows.shape[0] // size
    return lax.dynamic_slice_in_dim(rows, lax.axis_index("tp") * count, count, 0)


MESH = pl.DeviceIdType.MESH
TILE = 512


def fits_kernels():
    return lax.axis_size("ctx") == 4 and lax.axis_size("tp") == 2


class Place:
    def __init__(self):
        me = lax.axis_index("ctx")
        x, core = me // 2, me % 2
        self.tp = lax.axis_index("tp")
        self.x = {"ctx": (1 - x) * 2 + core}
        self.core = {"ctx": x * 2 + 1 - core}
        self.cross = {"ctx": (1 - x) * 2 + 1 - core}
        self.y = {"tp": 1 - self.tp}

    def others(self, axis):
        size, me = lax.axis_size(axis), lax.axis_index(axis)
        return [{axis: (me + n) % size} for n in range(1, size)]


def meet(devices):
    barrier = pltpu.get_barrier_semaphore()
    for device in devices:
        pl.semaphore_signal(barrier, inc=1, device_id=device, device_id_type=MESH)
    pl.semaphore_wait(barrier, len(devices))


class Links:
    def __init__(self, send, recv):
        self.send, self.recv, self.count, self.sent = send, recv, 0, []

    def copy(self, src, dst, device, at=None):
        n = self.count
        self.count += 1
        made = pltpu.make_async_remote_copy(src, dst, self.send.at[n], self.recv.at[n], device_id=device, device_id_type=MESH)
        self.sent.append(made)
        return made

    def drain(self):
        for made in self.sent:
            made.wait_send()


def start_kernel(hidden, grads, segs, gains, attn_in, cot, segs_out, gains_out, hbuf, nbuf, gbuf, gain_row, send, recv, local_sem):
    place, links = Place(), Links(send, recv)
    rows = hidden.shape[0]
    half, quarter = rows // 2, rows // 4
    z = lax.axis_index("fsdp")
    near = [place.x, place.core, place.cross, place.y]
    far = place.others("fsdp")
    meet(near + far)

    def span(block, part, chunk=None):
        if chunk is None:
            return aligned(block * rows + part * half, half)
        return aligned(block * rows + part * half + chunk * quarter, quarter)

    mine, other = place.tp, 1 - place.tp
    tiny = [links.copy(gains, gains_out.at[z], device) for device in far]
    tiny_segs = [links.copy(segs, segs_out.at[n + 1], device) for n, device in enumerate(near[:3])]
    for made in tiny + tiny_segs:
        made.start()
    over_x = {}
    for name, src, dst in (("h", hidden, hbuf), ("g", grads, gbuf)):
        for q in range(2):
            over_x[name, q] = links.copy(src.at[span(0, mine, q)], dst.at[span(1, mine, q)], place.x)
    over_core = {name: links.copy(src, dst.at[aligned(2 * rows, rows)], place.core) for name, src, dst in (("h", hidden, hbuf), ("g", grads, gbuf))}
    for key in (("h", 0), ("h", 1)):
        over_x[key].start()
    over_core["h"].start()
    for key in (("g", 0), ("g", 1)):
        over_x[key].start()
    over_core["g"].start()
    kept = []

    def keep(src, dst):
        made = pltpu.make_async_copy(src, dst, local_sem.at[len(kept)])
        made.start()
        kept.append(made)

    keep(grads, cot.at[aligned(0, rows)])
    gains_out[z] = gains[...]
    segs_out[0] = segs[...]
    for made in tiny:
        made.wait_recv()
    lanes = 128
    groups = gains.shape[0] // 2
    for device in range(gains_out.shape[0]):
        for row in range(groups):
            gain_row[:, pl.ds((device * groups + row) * lanes, lanes)] = gains_out[device, row : row + 1, :]

    def normalize(src, at, block, count):
        def some(n, _):
            there = aligned(at + n * 64, 64)
            values = wide(src[there, :])
            scale = lax.rsqrt(jnp.mean(values * values, axis=1, keepdims=True) + EPS)
            nbuf[aligned(block + n * 64, 64), :] = low(values * scale * gain_row[...])
            return 0

        lax.fori_loop(0, count // 64, some, 0)
        keep(nbuf.at[pl.ds(block, count)], attn_in.at[pl.ds(block, count)])

    normalize(hidden, 0, 0, rows)
    over_y, across, last = {}, {}, {}

    def pass_on(name, buf):
        for q in range(2):
            over_x[name, q].wait_recv()
            over_y[name, q] = links.copy(buf.at[span(1, mine, q)], buf.at[span(1, mine, q)], place.y)
            across[name, q] = links.copy(buf.at[span(1, mine, q)], buf.at[span(3, mine, q)], place.core)
            over_y[name, q].start()
            across[name, q].start()

    def finish(name, buf):
        for q in range(2):
            over_y[name, q].wait_recv()
            last[name, q] = links.copy(buf.at[span(1, other, q)], buf.at[span(3, other, q)], place.core)
            last[name, q].start()

    pass_on("h", hbuf)
    over_core["h"].wait_recv()
    normalize(hbuf, 2 * rows, 2 * rows, rows)
    finish("h", hbuf)
    normalize(hbuf, rows, rows, rows)
    pass_on("g", gbuf)
    for q in range(2):
        across["h", q].wait_recv()
        last["h", q].wait_recv()
    normalize(hbuf, 3 * rows, 3 * rows, rows)
    over_core["g"].wait_recv()
    keep(gbuf.at[aligned(2 * rows, rows)], cot.at[aligned(2 * rows, rows)])
    finish("g", gbuf)
    keep(gbuf.at[aligned(rows, rows)], cot.at[aligned(rows, rows)])
    for q in range(2):
        across["g", q].wait_recv()
        last["g", q].wait_recv()
    keep(gbuf.at[aligned(3 * rows, rows)], cot.at[aligned(3 * rows, rows)])
    for made in tiny_segs:
        made.wait_recv()
    links.drain()
    for made in kept:
        made.wait()


def start_exchange(hidden, grads, segments, attn_gain, mlp_gain):
    rows, width = hidden.shape
    fsdp = lax.axis_size("fsdp")
    segs = jnp.concatenate([segments.reshape(-1, 128), jnp.zeros((8 - rows // 128, 128), jnp.int32)], axis=0)
    gains = wide(jnp.concatenate([attn_gain, mlp_gain])).reshape(-1, 128)
    vmem = pl.BlockSpec(memory_space=pltpu.VMEM)
    hbm = pl.BlockSpec(memory_space=pl.ANY)
    tokens = 4 * rows
    attn_in, cot, segs, gains = pl.pallas_call(
        start_kernel,
        in_specs=[vmem] * 4,
        out_specs=[hbm, hbm, vmem, vmem],
        out_shape=[
            jax.ShapeDtypeStruct((tokens, width), jnp.bfloat16),
            jax.ShapeDtypeStruct((tokens, width), jnp.bfloat16),
            jax.ShapeDtypeStruct((4, 8, 128), jnp.int32),
            jax.ShapeDtypeStruct((fsdp,) + gains.shape, jnp.float32),
        ],
        scratch_shapes=[
            pltpu.VMEM((tokens, width), jnp.bfloat16),
            pltpu.VMEM((tokens, width), jnp.bfloat16),
            pltpu.VMEM((tokens, width), jnp.bfloat16),
            pltpu.VMEM((1, width), jnp.float32),
            pltpu.SemaphoreType.DMA((fsdp + 32,)),
            pltpu.SemaphoreType.DMA((fsdp + 32,)),
            pltpu.SemaphoreType.DMA((8,)),
        ],
        compiler_params=pltpu.CompilerParams(collective_id=0, has_side_effects=True, vmem_limit_bytes=VMEM_LIMIT),
        cost_estimate=pl.CostEstimate(flops=0, bytes_accessed=200_000_000, transcendentals=0),
    )(hidden, grads, segs, gains)
    segs = segs[:, : rows // 128].reshape(tokens)
    gains = jnp.transpose(gains.reshape(fsdp, 2, -1), (1, 0, 2)).reshape(2, width)
    return attn_in, cot, segs, gains


def scatter_scratch(rows, width):
    part, half = rows // 8, width // 2
    return [
        pltpu.VMEM((4, part, width), jnp.bfloat16),
        pltpu.VMEM((4, part, width), jnp.bfloat16),
        pltpu.VMEM((6, part, half), jnp.bfloat16),
        pltpu.VMEM((6, part, half), jnp.bfloat16),
        pltpu.VMEM((2, part, half), jnp.float32),
        pltpu.VMEM((part, width), jnp.float32),
        pltpu.SemaphoreType.DMA((14,)),
        pltpu.SemaphoreType.DMA((14,)),
    ]


class Scatter:
    def __init__(self, place, make, count, refs, first=("x", "y")):
        self.place, self.make = place, make
        self.hi, self.core_in, self.out, self.come, self.wait, self.total, send, recv = refs
        self.part = count // 8
        self.half = self.total.shape[1] // 2
        self.links = Links(send, recv)
        self.core = {}
        for side in range(2):
            cols = pl.ds(side * self.half, self.half)
            for n in range(4):
                self.core[n, side] = self.links.copy(self.hi.at[n, :, cols], self.core_in.at[n, :, cols], place.core)
        self.send, self.away, self.stays = [], {}, {}
        for side, link in enumerate(first):
            to, then = (place.x, place.y) if link == "x" else (place.y, place.x)
            for n, device in enumerate((to, to, then)):
                at = 3 * side + n
                self.send.append(self.links.copy(self.out.at[at], self.come.at[at], device))
            second, stay = (1, 2) if link == "x" else (2, 1)
            self.away[0, side], self.away[second, side] = 3 * side, 3 * side + 1
            self.stays[side] = stay

    def rows(self, n):
        tp = self.place.tp
        part = (1 - tp) + (n % 2) * (2 * tp - 1)
        return ((1 - n // 2) * 2 + part) * self.part

    def columns(self, side, each):
        tiles = self.half // TILE

        def one(n, _):
            each(aligned(side * self.half + n * TILE, TILE), aligned(n * TILE, TILE))
            return 0

        lax.fori_loop(0, tiles, one, 0)

    def to_core(self, n, side):
        rows = aligned(4 * self.part + self.rows(n), self.part)

        def each(cols, _):
            self.hi[n, :, cols] = low(self.make(rows, cols))

        self.columns(side, each)
        self.core[n, side].start()

    def to_links(self, n, side):
        rows = aligned(self.rows(n), self.part)
        self.core[n, side].wait_recv()

        def each(cols, at):
            value = self.make(rows, cols) + wide(self.core_in[n, :, cols])
            if (n, side) in self.away:
                self.out[self.away[n, side], :, at] = low(value)
            elif n == 3:
                self.total[:, cols] = value
            else:
                self.wait[side, :, at] = value

        self.columns(side, each)
        if (n, side) in self.away:
            self.send[self.away[n, side]].start()

    def units(self):
        return (
            [(0, side) for side in range(2)]
            + [(n, side) for n in (1, 2) for side in range(2) if (n, side) in self.away]
            + [(self.stays[side], side) for side in range(2)]
            + [(3, side) for side in range(2)]
        )

    def start(self, waits=()):
        units = self.units()
        ahead = 2
        waits = list(waits) + [()] * 3
        for at, unit in enumerate(units[:ahead]):
            for made in waits[at]:
                made.wait()
            self.to_core(*unit)
        for made in waits[2]:
            made.wait()
        for at, unit in enumerate(units):
            self.to_links(*unit)
            if at + ahead < len(units):
                self.to_core(*units[at + ahead])

    def turn(self):
        for side in range(2):
            came, goes = 3 * side, 3 * side + 2
            self.send[came].wait_recv()

            def each(_, at):
                self.out[goes, :, at] = low(self.wait[side, :, at] + wide(self.come[came, :, at]))

            self.columns(side, each)
            self.send[goes].start()

    def finish(self):
        for side in range(2):
            for n in (1, 2):
                self.send[3 * side + n].wait_recv()
            cols = pl.ds(side * self.half, self.half)
            self.total[:, cols] = self.total[:, cols] + wide(self.come[3 * side + 1]) + wide(self.come[3 * side + 2])
        self.links.drain()


def gather_plane(place, links, mine, full, part):
    half = mine.shape[1] // 2
    left, right = pl.ds(0, half), pl.ds(half, half)
    own, other = place.tp, 1 - place.tp

    def rows(block, tp):
        return aligned((block * 2 + tp) * part, part)

    y_left = links.copy(mine.at[:, left], full.at[rows(0, own), left], place.y)
    x_right = links.copy(mine.at[:, right], full.at[rows(1, own), right], place.x)
    y_right = links.copy(mine.at[:, right], full.at[rows(0, own), right], place.y)
    x_left = links.copy(mine.at[:, left], full.at[rows(1, own), left], place.x)
    core = [links.copy(mine, full.at[rows(2, own)], place.core)]
    for made in (y_left, x_right, y_right, x_left, core[0]):
        made.start()

    def relay(come, block, tp, cols, onward=None):
        come.wait_recv()
        here = full.at[rows(block, tp), cols]
        if onward == "x":
            made = links.copy(here, full.at[rows(1, tp), cols], place.x)
        elif onward == "y":
            made = links.copy(here, full.at[rows(block, tp), cols], place.y)
        if onward:
            made.start()
        over = links.copy(here, full.at[rows(block + 2, tp), cols], place.core)
        over.start()
        core.append(over)
        return made if onward else None

    far_left = relay(y_left, 0, other, left, "x")
    far_right = relay(x_right, 1, own, right, "y")
    relay(y_right, 0, other, right)
    relay(x_left, 1, own, left)
    relay(far_left, 1, other, left)
    relay(far_right, 1, other, right)
    for made in core:
        made.wait_recv()


def load(sems, pairs):
    made = [pltpu.make_async_copy(src, dst, sems.at[n]) for n, (src, dst) in enumerate(pairs)]
    for copy in made:
        copy.start()
    return made


def forward_mid_kernel(mixed, weight, hidden, gain, full, resid_out, mine, *refs):
    place = Place()
    scatter_refs, (send, recv, local_sem) = refs[:-3], refs[-3:]
    count = mixed.shape[0]
    part = count // 8
    meet([place.x, place.core, place.y])
    scatter = Scatter(place, lambda rows, cols: contract_cols(mixed[rows, :], weight[cols, weight.shape[1] - mixed.shape[1] :]), count, scatter_refs)
    scatter.start()
    scatter.turn()
    scatter.finish()
    step = 64

    def some(n, _):
        rows = aligned(n * step, step)
        values = wide(hidden[aligned(place.tp * part + n * step, step), :]) + scatter.total[rows, :]
        resid_out[rows, :] = values
        scale = lax.rsqrt(jnp.mean(values * values, axis=1, keepdims=True) + EPS)
        mine[rows, :] = low(values * scale * gain[...])
        return 0

    lax.fori_loop(0, part // step, some, 0)
    stay = pltpu.make_async_copy(mine, full.at[aligned(place.tp * part, part)], local_sem)
    stay.start()
    links = Links(send, recv)
    gather_plane(place, links, mine, full, part)
    links.drain()
    stay.wait()


def mid_scratch(count, width):
    return [pltpu.VMEM((count // 8, width), jnp.bfloat16)] + scatter_scratch(count, width) + [
        pltpu.SemaphoreType.DMA((16,)),
        pltpu.SemaphoreType.DMA((16,)),
        pltpu.SemaphoreType.DMA,
    ]


def forward_mid(mixed, weight, hidden, gain):
    count, width = mixed.shape[0], weight.shape[0]
    vmem = pl.BlockSpec(memory_space=pltpu.VMEM)
    return pl.pallas_call(
        forward_mid_kernel,
        in_specs=[vmem] * 4,
        out_specs=[pl.BlockSpec(memory_space=pl.ANY), vmem],
        out_shape=[jax.ShapeDtypeStruct((count, width), jnp.bfloat16), jax.ShapeDtypeStruct((count // 8, width), jnp.float32)],
        scratch_shapes=mid_scratch(count, width),
        compiler_params=pltpu.CompilerParams(collective_id=1, has_side_effects=True, vmem_limit_bytes=VMEM_LIMIT),
        cost_estimate=pl.CostEstimate(flops=0, bytes_accessed=300_000_000, transcendentals=0),
    )(mixed, weight, hidden, gain[None, :])


def norm_back(values, scale, gain, cot):
    scaled = cot * gain
    lean = jnp.mean(values * scaled, axis=1, keepdims=True)
    return scale * scaled - values * (scale * scale * scale) * lean, cot * (values * scale)


def backward_mid_kernel(
    gate_hbm, up_hbm, weights_hbm, resid_hbm, grads_hbm, gain, full, cot_out, gain_out,
    gate_cot, up_cot, weights, resid, grads, sems, mine, *refs
):
    place = Place()
    scatter_refs, (send, recv, local_sem) = refs[:-3], refs[-3:]
    count, hidden_cols = gate_cot.shape
    part = count // 8
    width = weights.shape[0]
    lower, upper = pl.ds(0, count // 2), pl.ds(count // 2, count // 2)
    left, right = pl.ds(0, width // 2), pl.ds(width // 2, width // 2)
    loads = load(
        sems,
        [
            (weights_hbm.at[left], weights.at[left]),
            (gate_hbm.at[upper], gate_cot.at[upper]),
            (up_hbm.at[upper], up_cot.at[upper]),
            (weights_hbm.at[right], weights.at[right]),
            (gate_hbm.at[lower], gate_cot.at[lower]),
            (up_hbm.at[lower], up_cot.at[lower]),
            (resid_hbm, resid),
            (grads_hbm.at[aligned(place.tp * part, part)], grads),
        ],
    )
    meet([place.x, place.core, place.y])

    def make(rows, cols):
        return contract_cols(gate_cot[rows, :], weights[cols, :hidden_cols]) + contract_cols(up_cot[rows, :], weights[cols, hidden_cols:])

    scatter = Scatter(place, make, count, scatter_refs)
    scatter.start((loads[:3], loads[3:4], loads[4:6]))
    scatter.turn()
    scatter.finish()
    for made in loads[6:]:
        made.wait()
    step = 32

    def some(n, sums):
        rows = aligned(n * step, step)
        values = resid[rows, :]
        scale = lax.rsqrt(jnp.mean(values * values, axis=1, keepdims=True) + EPS)
        back, terms = norm_back(values, scale, gain[...], scatter.total[rows, :])
        cot = wide(grads[rows, :]) + back
        cot_out[rows, :] = cot
        mine[rows, :] = low(cot)
        return sums + jnp.sum(terms, axis=0, keepdims=True)

    gain_out[...] = lax.fori_loop(0, part // step, some, jnp.zeros(gain.shape, jnp.float32))
    stay = pltpu.make_async_copy(mine, full.at[aligned(place.tp * part, part)], local_sem)
    stay.start()
    links = Links(send, recv)
    gather_plane(place, links, mine, full, part)
    links.drain()
    stay.wait()


def backward_mid(gate_cot, up_cot, weights, resid, grads, gain):
    count, width = gate_cot.shape[0], weights.shape[0]
    vmem = pl.BlockSpec(memory_space=pltpu.VMEM)
    hbm = pl.BlockSpec(memory_space=pl.ANY)
    return pl.pallas_call(
        backward_mid_kernel,
        in_specs=[hbm] * 5 + [vmem],
        out_specs=[pl.BlockSpec(memory_space=pl.ANY), vmem, vmem],
        out_shape=[
            jax.ShapeDtypeStruct((count, width), jnp.bfloat16),
            jax.ShapeDtypeStruct((count // 8, width), jnp.float32),
            jax.ShapeDtypeStruct((1, width), jnp.float32),
        ],
        scratch_shapes=[
            pltpu.VMEM(gate_cot.shape, jnp.bfloat16),
            pltpu.VMEM(up_cot.shape, jnp.bfloat16),
            pltpu.VMEM(weights.shape, jnp.bfloat16),
            pltpu.VMEM(resid.shape, jnp.float32),
            pltpu.VMEM(resid.shape, jnp.bfloat16),
            pltpu.SemaphoreType.DMA((8,)),
        ]
        + mid_scratch(count, width),
        compiler_params=pltpu.CompilerParams(collective_id=2, has_side_effects=True, vmem_limit_bytes=VMEM_LIMIT),
        cost_estimate=pl.CostEstimate(flops=0, bytes_accessed=300_000_000, transcendentals=0),
    )(gate_cot, up_cot, weights, resid, grads, gain[None, :])


def input_kernel(cots, weights, cot_hbm, hidden_hbm, gain, gain_two, grad_out, gains_out, resid_cot, hidden, sems, sums, come, *refs):
    place = Place()
    (send, recv), refs = refs[-2:], refs[:-2]
    count = cots.shape[0]
    part = count // 8
    loads = load(sems, [(cot_hbm, resid_cot), (hidden_hbm.at[aligned(place.tp * part, part)], hidden)])
    meet([place.x, place.core, place.y] + place.others("fsdp"))
    scatter = Scatter(place, lambda rows, cols: contract_cols(cots[rows, :], weights[cols, : cots.shape[1]]), count, refs, ("y", "y"))
    links = Links(send, recv)
    scatter.start()
    scatter.turn()
    scatter.finish()
    for made in loads:
        made.wait()
    step = 32

    def some(n, total):
        rows = aligned(n * step, step)
        values = wide(hidden[rows, :])
        scale = lax.rsqrt(jnp.mean(values * values, axis=1, keepdims=True) + EPS)
        back, terms = norm_back(values, scale, gain[...], scatter.total[rows, :])
        grad_out[rows, :] = low(resid_cot[rows, :] + back)
        return total + jnp.sum(terms, axis=0, keepdims=True)

    sums[0, 0:1, :] = lax.fori_loop(0, part // step, some, jnp.zeros(gain.shape, jnp.float32))
    sums[0, 1:2, :] = gain_two[...]
    near = [place.x, place.core, place.y]
    for n, device in enumerate(near):
        made = links.copy(sums.at[n], come.at[n], device)
        made.start()
        made.wait_recv()
        sums[n + 1] = sums[n] + come[n]
    at = len(near)
    far = [links.copy(sums.at[at], come.at[at + n], device) for n, device in enumerate(place.others("fsdp"))]
    for made in far:
        made.start()
    total = sums[at]
    for n, made in enumerate(far):
        made.wait_recv()
        total = total + come[at + n]
    gains_out[...] = total
    links.drain()


def input_exchange(cots, weights, resid_cot, hidden, gain, gain_two):
    count, width = cots.shape[0], weights.shape[0]
    fsdp = lax.axis_size("fsdp")
    vmem = pl.BlockSpec(memory_space=pltpu.VMEM)
    return pl.pallas_call(
        input_kernel,
        in_specs=[vmem] * 2 + [pl.BlockSpec(memory_space=pl.ANY)] * 2 + [vmem] * 2,
        out_specs=[vmem, vmem],
        out_shape=[jax.ShapeDtypeStruct((count // 8, width), jnp.bfloat16), jax.ShapeDtypeStruct((2, width), jnp.float32)],
        scratch_shapes=[
            pltpu.VMEM(resid_cot.shape, jnp.float32),
            pltpu.VMEM(resid_cot.shape, jnp.bfloat16),
            pltpu.SemaphoreType.DMA((2,)),
            pltpu.VMEM((4, 2, width), jnp.float32),
            pltpu.VMEM((2 + fsdp, 2, width), jnp.float32),
        ]
        + scatter_scratch(count, width)
        + [pltpu.SemaphoreType.DMA((4 + fsdp,)), pltpu.SemaphoreType.DMA((4 + fsdp,))],
        compiler_params=pltpu.CompilerParams(collective_id=3, has_side_effects=True, vmem_limit_bytes=VMEM_LIMIT),
        cost_estimate=pl.CostEstimate(flops=0, bytes_accessed=180_000_000, transcendentals=0),
    )(cots, weights, resid_cot, hidden, gain[None, :], gain_two)


def attention_output_kernel(
    rot_hbm, cos_hbm, sin_hbm, seg_col, seg_row, cot_hbm, mixed_hbm, lse, hidden_act, down, resid_hbm, cots, out,
    rot, cos, sin, cot, mixed, resid, sems, delta, dq, *refs
):
    place = Place()
    count = hidden_act.shape[0]
    me = lax.axis_index("ctx")
    blocks = count // BLOCK
    per = count // 4 // BLOCK

    def at(block):
        n = block // per
        return (((me // 2 + n % 2) % 2) * 2 + (me % 2 + n // 2) % 2) * per + block % per

    def follows(i, j):
        return (at(j) < at(i)) & (at(i) - at(j) <= blocks // 2)

    loads = load(
        sems, [(rot_hbm, rot), (cos_hbm, cos), (sin_hbm, sin), (cot_hbm, cot), (mixed_hbm, mixed), (resid_hbm, resid)]
    )
    meet([place.x, place.core, place.y])
    scatter = Scatter(place, lambda rows, cols: product(hidden_act[rows, :], down[:, cols]), count, refs, ("y", "y"))
    scatter.start()
    for made in loads:
        made.wait()
    pairs = rot.shape[1] // (3 * PAIR)
    steps = pairs * blocks

    def step(n, _):
        back = Backward(n // blocks, rot, cos, sin, seg_col, seg_row, cot, mixed, lse, cots, delta, dq, follows)

        @pl.when(n % blocks == 0)
        def _():
            back.prepare()

        back.column(n % blocks)

        @pl.when(n % blocks == blocks - 1)
        def _():
            back.finish()

        @pl.when(n == steps // 4 - 1)
        def _():
            scatter.turn()

        return 0

    lax.fori_loop(0, steps, step, 0)
    scatter.finish()
    out[...] = low(resid[...] + scatter.total[...])


def attention_output(rot, cos, sin, seg_col, seg_row, cot, mixed, lse, hidden_act, down, resid):
    count, width = hidden_act.shape[0], down.shape[1]
    vmem = pl.BlockSpec(memory_space=pltpu.VMEM)
    hbm = pl.BlockSpec(memory_space=pl.ANY)
    return pl.pallas_call(
        attention_output_kernel,
        in_specs=[hbm] * 3 + [vmem] * 2 + [hbm] * 2 + [vmem] * 3 + [hbm],
        out_specs=[vmem, vmem],
        out_shape=[
            jax.ShapeDtypeStruct(rot.shape, jnp.bfloat16),
            jax.ShapeDtypeStruct((count // 8, width), jnp.bfloat16),
        ],
        scratch_shapes=[pltpu.VMEM(array.shape, array.dtype) for array in (rot, cos, sin, cot, mixed, resid)]
        + [
            pltpu.SemaphoreType.DMA((6,)),
            pltpu.VMEM((2, count), jnp.float32),
            pltpu.VMEM((count, PAIR), jnp.float32),
        ]
        + scatter_scratch(count, width),
        compiler_params=pltpu.CompilerParams(collective_id=4, has_side_effects=True, vmem_limit_bytes=VMEM_LIMIT),
        cost_estimate=pl.CostEstimate(flops=0, bytes_accessed=220_000_000, transcendentals=0),
    )(rot, cos, sin, seg_col, seg_row, cot, mixed, lse, hidden_act, down, resid)


def take_attention_kernel(at, query, key, value, out, taken):
    pairs = query.shape[1] // PAIR
    for p in range(pairs):
        for n, part in enumerate((query, key, value)):
            taken[:, (3 * p + n) * PAIR : (3 * p + n + 1) * PAIR] = part[:, p * PAIR : (p + 1) * PAIR]
    taken[:, 3 * pairs * PAIR :] = out[...].T


def take_attention(me, query, key, value, out, count):
    depth = query.shape[0]
    block = pl.BlockSpec((depth, count), lambda n, at: (0, at[0]))
    return pl.pallas_call(
        take_attention_kernel,
        grid_spec=pltpu.PrefetchScalarGridSpec(
            num_scalar_prefetch=1,
            grid=(1,),
            in_specs=[block] * 3 + [pl.BlockSpec((count, depth), lambda n, at: (at[0], 0))],
            out_specs=pl.BlockSpec((depth, 4 * count), lambda n, at: (0, 0)),
        ),
        out_shape=jax.ShapeDtypeStruct((depth, 4 * count), query.dtype),
        compiler_params=pltpu.CompilerParams(vmem_limit_bytes=VMEM_LIMIT),
    )(me, query, key, value, out)


def take_hidden_kernel(at, gate, up, down, both, rows):
    count = gate.shape[1]
    both[:, :count] = gate[...]
    both[:, count:] = up[...]
    rows[...] = down[...]


def take_hidden(me, gate, up, down, count):
    depth = gate.shape[0]
    block = pl.BlockSpec((depth, count), lambda n, at: (0, at[0]))
    return pl.pallas_call(
        take_hidden_kernel,
        grid_spec=pltpu.PrefetchScalarGridSpec(
            num_scalar_prefetch=1,
            grid=(1,),
            in_specs=[block] * 2 + [pl.BlockSpec((count, depth), lambda n, at: (at[0], 0))],
            out_specs=[pl.BlockSpec((depth, 2 * count), lambda n, at: (0, 0)), pl.BlockSpec((count, depth), lambda n, at: (0, 0))],
        ),
        out_shape=[jax.ShapeDtypeStruct((depth, 2 * count), gate.dtype), jax.ShapeDtypeStruct((count, depth), down.dtype)],
        compiler_params=pltpu.CompilerParams(vmem_limit_bytes=VMEM_LIMIT),
    )(me, gate, up, down)


def first_swaps(block):
    pieces = [block]
    for mask in masks(lax.axis_size("ctx"))[:-1]:
        pieces = pieces + [swap(piece, "ctx", mask) for piece in pieces]
    return pieces


def last_swap(pieces):
    return pieces + [swap(piece, "ctx", 1) for piece in pieces]


def order_of_pieces():
    return lax.axis_index("ctx") ^ jnp.array(offsets(lax.axis_size("ctx")), jnp.int32)


def place_kernel(at, *refs):
    out = refs[-1]
    for n, piece in enumerate(refs[:-1]):

        @pl.when(pl.program_id(0) == n)
        def _():
            out[...] = wide(piece[...])


def place_pieces(pieces, axis):
    block = pieces[0].shape
    shape = list(block)
    shape[axis] *= len(pieces)
    return pl.pallas_call(
        place_kernel,
        grid_spec=pltpu.PrefetchScalarGridSpec(
            num_scalar_prefetch=1,
            grid=(len(pieces),),
            in_specs=[pl.BlockSpec(block, lambda n, at: (0, 0))] * len(pieces),
            out_specs=pl.BlockSpec(block, lambda n, at: (at[n], 0) if axis == 0 else (0, at[n])),
        ),
        out_shape=jax.ShapeDtypeStruct(shape, jnp.float32),
        compiler_params=pltpu.CompilerParams(vmem_limit_bytes=VMEM_LIMIT),
        cost_estimate=pl.CostEstimate(flops=0, bytes_accessed=6 * math.prod(shape), transcendentals=0),
    )(order_of_pieces(), *pieces)


def place_gate_up_kernel(at, *refs):
    pieces, (gate, up) = refs[:-2], refs[-2:]
    count = gate.shape[1]
    for n, piece in enumerate(pieces):

        @pl.when(pl.program_id(0) == n)
        def _():
            gate[...] = wide(piece[:, :count])
            up[...] = wide(piece[:, count:])


def place_gate_up(pieces):
    rows, cols = pieces[0].shape
    count, whole = cols // 2, cols // 2 * len(pieces)
    side = pl.BlockSpec((rows, count), lambda n, at: (0, at[n]))
    return pl.pallas_call(
        place_gate_up_kernel,
        grid_spec=pltpu.PrefetchScalarGridSpec(
            num_scalar_prefetch=1,
            grid=(len(pieces),),
            in_specs=[pl.BlockSpec((rows, cols), lambda n, at: (0, 0))] * len(pieces),
            out_specs=[side] * 2,
        ),
        out_shape=[jax.ShapeDtypeStruct((rows, whole), jnp.float32)] * 2,
        compiler_params=pltpu.CompilerParams(vmem_limit_bytes=VMEM_LIMIT),
        cost_estimate=pl.CostEstimate(flops=0, bytes_accessed=12 * rows * whole, transcendentals=0),
    )(order_of_pieces(), *pieces)


def place_attention_kernel(at, *refs):
    pieces, outs = refs[:-4], refs[-4:]
    count = outs[0].shape[1]
    pairs = count // PAIR
    for n, piece in enumerate(pieces):

        @pl.when(pl.program_id(0) == n)
        def _():
            for p in range(pairs):
                for m in range(3):
                    outs[m][:, p * PAIR : (p + 1) * PAIR] = wide(piece[:, (3 * p + m) * PAIR : (3 * p + m + 1) * PAIR])
            outs[3][...] = wide(piece[:, 3 * count :]).T


def place_attention(pieces):
    depth, count = pieces[0].shape[0], pieces[0].shape[1] // 4
    whole = len(pieces) * count
    side = pl.BlockSpec((depth, count), lambda n, at: (0, at[n]))
    return pl.pallas_call(
        place_attention_kernel,
        grid_spec=pltpu.PrefetchScalarGridSpec(
            num_scalar_prefetch=1,
            grid=(len(pieces),),
            in_specs=[pl.BlockSpec(pieces[0].shape, lambda n, at: (0, 0))] * len(pieces),
            out_specs=[side] * 3 + [pl.BlockSpec((count, depth), lambda n, at: (at[n], 0))],
        ),
        out_shape=[jax.ShapeDtypeStruct((depth, whole), jnp.float32)] * 3 + [jax.ShapeDtypeStruct((whole, depth), jnp.float32)],
        compiler_params=pltpu.CompilerParams(vmem_limit_bytes=VMEM_LIMIT),
        cost_estimate=pl.CostEstimate(flops=0, bytes_accessed=24 * depth * whole, transcendentals=0),
    )(order_of_pieces(), *pieces)


def local(
    hidden_in,
    out_grad,
    segment_ids,
    attn_gain,
    w_query,
    w_key,
    w_value,
    w_out,
    mlp_gain,
    w_gate,
    w_up,
    w_down,
):
    group = lax.axis_size("ctx")
    me = lax.axis_index("ctx")
    local_rows = hidden_in.shape[1]
    tokens = local_rows * group
    head_cols = w_query.shape[1] // group
    ff_cols = w_gate.shape[1] // group

    def gather(weight, axis):
        return lax.all_gather(weight, "fsdp", axis=axis, tiled=True)

    def settle(part, axis):
        return lax.psum_scatter(part, "fsdp", scatter_dimension=axis, tiled=True)

    at = me[None]
    w_attn = gather(take_attention(at, w_query, w_key, w_value, w_out, head_cols), 0)
    qkv_cols = 3 * head_cols
    w_qkv, w_out_t = w_attn[:, :qkv_cols], w_attn[:, qkv_cols:]
    own_gate_up, own_down = take_hidden(at, w_gate, w_up, w_down, ff_cols)
    full_gate_up = gather(own_gate_up, 0)
    full_down = gather(own_down, 1)

    kernels = fits_kernels()
    if kernels:
        attn_in, branch_cot, segments, gains = start_exchange(hidden_in[0], out_grad[0], segment_ids[0], attn_gain, mlp_gain)
        gain_one, gain_two = gains[0], gains[1]
    else:
        gains = wide(gather(jnp.stack([attn_gain, mlp_gain]), 1))
        gain_one, gain_two = gains[0], gains[1]
        rows_in = wide(hidden_in[0])
        r1 = lax.rsqrt(jnp.mean(rows_in * rows_in, axis=-1, keepdims=True) + EPS)
        attn_in = gather_rows(low(rows_in * r1 * gain_one), "ctx")
        segments = gather_rows(segment_ids[0], "ctx")
        branch_cot = gather_rows(out_grad[0], "ctx")

    firsts = jnp.stack([(me ^ at) * local_rows for at in offsets(group)])
    positions = (firsts[:, None] + jnp.arange(local_rows, dtype=jnp.int32)[None, :]).reshape(tokens)
    exponents = jnp.arange(0, HEAD_DIM, 2).astype(jnp.float32) / HEAD_DIM
    inverse = jnp.float32(ROPE_BASE) ** (-exponents)
    angles = positions.astype(jnp.float32)[:, None] * inverse[None, :]
    cos = jnp.tile(jnp.cos(angles), (1, 4))
    sin = jnp.tile(jnp.sin(angles), (1, 4))
    info = jnp.stack([positions[::BLOCK], segments[::BLOCK], segments[BLOCK - 1 :: BLOCK]])
    seg_col, seg_row = segments[:, None], segments[None, :]

    qkv = product(attn_in, w_qkv)
    rot, mixed, mixed_wide, lse = attention_forward(info, qkv, cos, sin, seg_col, seg_row)

    own_in = wide(own_part(hidden_in[0]))
    if kernels:
        mlp_in, resid = forward_mid(mixed, w_attn, hidden_in[0], gain_two)
    else:
        part = scatter_both(lambda lo, hi: contract_cols(mixed[lo:hi], w_out_t), tokens)
        resid = own_in + part
        r2 = lax.rsqrt(jnp.mean(resid * resid, axis=-1, keepdims=True) + EPS)
        mlp_in = gather_rows(join_tp(low(resid * r2 * gain_two)), "ctx")
    acts = product(mlp_in, full_gate_up)
    gate_act, up_act = acts[:, :ff_cols], acts[:, ff_cols:]
    sigmoid = jax.nn.sigmoid(gate_act)
    hidden = low(gate_act * sigmoid * up_act)
    gate_slope = low(up_act * sigmoid * (1.0 + gate_act * (1.0 - sigmoid)))
    up_slope = low(gate_act * sigmoid)
    hidden, gate_slope, up_slope = lax.optimization_barrier((hidden, gate_slope, up_slope))
    down_part = low(contract_rows(hidden, branch_cot))
    down_part, full_down, branch_cot = lax.optimization_barrier((down_part, full_down, branch_cot))
    down_own = settle(down_part, 1)

    hidden_cot = contract_cols(branch_cot, full_down)
    gate_cot = low(hidden_cot * gate_slope)
    up_cot = low(hidden_cot * up_slope)
    gate_up_part = jnp.concatenate([low(contract_rows(mlp_in, gate_cot)), low(contract_rows(mlp_in, up_cot))], axis=1)
    gate_up_own = settle(gate_up_part, 0)
    if kernels:
        gate_cot, up_cot, gate_up_part = lax.optimization_barrier((gate_cot, up_cot, gate_up_part))
        attn_cot, resid_cot, gain_two_part = backward_mid(gate_cot, up_cot, full_gate_up, resid, out_grad[0], gain_two)
    else:
        mlp_in_cot = scatter_both(
            lambda lo, hi: contract_cols(gate_cot[lo:hi], full_gate_up[:, :ff_cols])
            + contract_cols(up_cot[lo:hi], full_gate_up[:, ff_cols:]),
            tokens,
        )
        back, terms = norm_back(resid, r2, gain_two, mlp_in_cot)
        gain_two_part = jnp.sum(terms, axis=0, keepdims=True)
        resid_cot = wide(own_part(out_grad[0])) + back
        attn_cot = gather_rows(join_tp(low(resid_cot)), "ctx")
    mixed_cot = low(product(attn_cot, w_out_t))
    out_part = low(contract_rows(attn_cot, mixed))
    mixed_cot, out_part, down_own = lax.optimization_barrier((mixed_cot, out_part, down_own))
    down_pieces = first_swaps(down_own)
    if kernels:
        cots, output = attention_output(rot, cos, sin, seg_col, seg_row, mixed_cot, mixed_wide, lse, hidden, full_down, resid)
        output = join_tp(output)
    else:
        cots = attention_backward(info, rot, cos, sin, seg_col, seg_row, mixed_cot, mixed_wide, lse)
    cots, *down_pieces = lax.optimization_barrier((cots, *down_pieces))
    qkv_part = low(contract_rows(attn_in, cots))
    attn_part = jnp.concatenate([qkv_part, out_part], axis=1)
    attn_own = settle(attn_part, 0)
    if kernels:
        cots, attn_part, gate_up_own = lax.optimization_barrier((cots, attn_part, gate_up_own))
        gate_up_pieces = first_swaps(gate_up_own)
        input_grad, gain_sums = input_exchange(cots, w_attn, resid_cot, hidden_in[0], gain_one, gain_two_part)
        input_grad, *gate_up_pieces = lax.optimization_barrier((input_grad, *gate_up_pieces))
        input_grad = join_tp(input_grad)
    else:
        gate_up_pieces = first_swaps(gate_up_own)
        out_sum = scatter_both(lambda lo, hi: product(hidden[lo:hi], full_down), tokens)
        output = join_tp(low(resid + out_sum))
        attn_in_cot = scatter_both(lambda lo, hi: contract_cols(cots[lo:hi], w_qkv), tokens)
        back, terms = norm_back(own_in, own_part(r1), gain_one, attn_in_cot)
        input_grad = join_tp(low(resid_cot + back))
        gain_sums = lax.psum(jnp.concatenate([jnp.sum(terms, axis=0, keepdims=True), gain_two_part]), ("fsdp", "ctx", "tp"))
    attn_pieces = first_swaps(attn_own)
    down_grad = place_pieces(last_swap(down_pieces), 0)
    gate_grad, up_grad = place_gate_up(last_swap(gate_up_pieces))
    down_grad, gate_grad, up_grad, output, *attn_pieces = lax.optimization_barrier(
        (down_grad, gate_grad, up_grad, output, *attn_pieces)
    )
    query_grad, key_grad, value_grad, out_proj_grad = place_attention(last_swap(attn_pieces))

    gain_sums = lax.dynamic_slice_in_dim(gain_sums, lax.axis_index("fsdp") * attn_gain.shape[0], attn_gain.shape[0], 1)
    return (
        output[None],
        input_grad[None],
        gain_sums[0],
        query_grad,
        key_grad,
        value_grad,
        out_proj_grad,
        gain_sums[1],
        gate_grad,
        up_grad,
        down_grad,
    )


def solution(mesh):
    weight, gain = P("fsdp", "tp"), P("fsdp")
    rows = P("fsdp", "ctx", None)
    in_specs = (rows, rows, P("fsdp", "ctx"), gain, weight, weight, weight, P("tp", "fsdp"), gain, weight, weight, P("tp", "fsdp"))
    out_specs = (rows, rows, gain, weight, weight, weight, P("tp", "fsdp"), gain, weight, weight, P("tp", "fsdp"))
    return jax.shard_map(local, mesh=mesh, in_specs=in_specs, out_specs=out_specs, check_vma=False)
```

```python
import math

import jax
import jax.numpy as jnp
from jax import lax
from jax.experimental import pallas as pl
from jax.experimental.pallas import tpu as pltpu
from jax.sharding import PartitionSpec as P


HEAD_DIM = 64
EPS = 1e-05
ROPE_BASE = 130000.0
MASKED = -1e30
PAIR = 2 * HEAD_DIM
BLOCK = 512
VMEM_LIMIT = 60 * 1024 * 1024


def low(values):
    return values.astype(jnp.bfloat16)


def wide(values):
    return values.astype(jnp.float32)


def product(a, b):
    return jnp.dot(a, b, preferred_element_type=jnp.float32)


def contract_rows(a, b):
    return lax.dot_general(a, b, (((0,), (0,)), ((), ())), preferred_element_type=jnp.float32)


def contract_cols(a, b):
    return lax.dot_general(a, b, (((1,), (1,)), ((), ())), preferred_element_type=jnp.float32)


def aligned(start, count):
    return pl.ds(pl.multiple_of(start, count), count)


def first_head():
    return lax.broadcasted_iota(jnp.int32, (1, PAIR), 1) < HEAD_DIM


def split_heads(rows):
    zero = jnp.zeros_like(rows)
    mask = first_head()
    return jnp.where(mask, rows, zero), jnp.where(mask, zero, rows)


def turn(rows, sign):
    half = HEAD_DIM // 2
    lanes = lax.broadcasted_iota(jnp.int32, (1, PAIR), 1)
    up = pltpu.roll(rows, PAIR - half, 1)
    down = pltpu.roll(rows, half, 1)
    return jnp.where(lanes % HEAD_DIM < half, -sign * up, sign * down)


def forward_kernel(info, qkv_ref, cos_ref, sin_ref, seg_col, seg_row, rot_ref, out_ref, wide_ref, lse_ref, best, total, acc):
    blocks = qkv_ref.shape[0] // BLOCK

    def prepare(n, _):
        rows = pl.ds(pl.multiple_of(n * BLOCK, BLOCK), BLOCK)
        cos, sin = cos_ref[rows, :], sin_ref[rows, :]
        q = qkv_ref[rows, :PAIR]
        k = qkv_ref[rows, PAIR : 2 * PAIR]
        rot_ref[rows, :PAIR] = low(low(q * cos + turn(q, 1.0) * sin) * jnp.bfloat16(HEAD_DIM**-0.5))
        rot_ref[rows, PAIR : 2 * PAIR] = low(k * cos + turn(k, 1.0) * sin)
        rot_ref[rows, 2 * PAIR :] = low(qkv_ref[rows, 2 * PAIR :])
        return 0

    lax.fori_loop(0, blocks, prepare, 0)

    def visit(i, j, diagonal):
        rows = pl.ds(pl.multiple_of(i * BLOCK, BLOCK), BLOCK)
        cols = pl.ds(pl.multiple_of(j * BLOCK, BLOCK), BLOCK)
        allowed = seg_col[rows, :1] == seg_row[:1, cols]
        if diagonal:
            at = lax.broadcasted_iota(jnp.int32, (BLOCK, BLOCK), 0)
            allowed = allowed & (at >= lax.broadcasted_iota(jnp.int32, (BLOCK, BLOCK), 1))
        keys = rot_ref[cols, PAIR : 2 * PAIR]
        values = rot_ref[cols, 2 * PAIR :]
        for h, q in enumerate(split_heads(rot_ref[rows, :PAIR])):
            scores = jnp.where(allowed, contract_cols(q, keys), MASKED)
            top = jnp.max(scores, axis=1, keepdims=True)
            if diagonal:
                p = jnp.exp(scores - top)
                best[h] = jnp.broadcast_to(top, (BLOCK, PAIR))
                total[h] = jnp.broadcast_to(jnp.sum(p, axis=1, keepdims=True), (BLOCK, PAIR))
                acc[h] = product(low(p), values)
            else:
                old = best[h][:, :1]
                new = jnp.maximum(old, top)
                fade = jnp.exp(old - new)
                p = jnp.exp(scores - new)
                best[h] = jnp.broadcast_to(new, (BLOCK, PAIR))
                total[h] = total[h] * fade + jnp.sum(p, axis=1, keepdims=True)
                acc[h] = acc[h] * fade + product(low(p), values)

    def one_row(i, _):
        rows = pl.ds(pl.multiple_of(i * BLOCK, BLOCK), BLOCK)
        visit(i, i, True)

        def one_col(j, _):
            @pl.when((info[0, j] < info[0, i]) & (info[2, j] >= info[1, i]))
            def _():
                visit(i, j, False)

            return 0

        lax.fori_loop(0, blocks, one_col, 0)
        mixed = jnp.where(first_head(), acc[0] / total[0], acc[1] / total[1])
        out_ref[rows, :] = low(mixed)
        wide_ref[rows, :] = mixed
        for h in range(2):
            lse_ref[0, h : h + 1, rows] = (best[h] + jnp.log(total[h])).T[:1, :]
        return 0

    lax.fori_loop(0, blocks, one_row, 0)


class Backward:
    def __init__(self, pair, rot, cos, sin, seg_col, seg_row, cot, mixed, lse, out, delta, dq, follows):
        self.pair, self.follows = pair, follows
        self.rot, self.cos, self.sin, self.seg_col, self.seg_row = rot, cos, sin, seg_col, seg_row
        self.cot, self.mixed, self.lse, self.out, self.delta, self.dq = cot, mixed, lse, out, delta, dq
        self.blocks = rot.shape[0] // BLOCK

    def part(self, n):
        return aligned((3 * self.pair + n) * PAIR, PAIR)

    def own(self):
        return aligned(self.pair * PAIR, PAIR)

    def prepare(self):
        def some(n, _):
            rows = aligned(n * BLOCK, BLOCK)
            terms = (wide(self.cot[rows, self.own()]) * self.mixed[rows, self.own()]).T
            self.delta[0:1, rows] = jnp.sum(terms[:HEAD_DIM], axis=0, keepdims=True)
            self.delta[1:2, rows] = jnp.sum(terms[HEAD_DIM:], axis=0, keepdims=True)
            self.dq[rows, :] = jnp.zeros((BLOCK, PAIR), jnp.float32)
            return 0

        lax.fori_loop(0, self.blocks, some, 0)

    def visit(self, row, rows_count, col, cols_count, diagonal, dk, dv):
        rows, cols = aligned(row, rows_count), aligned(col, cols_count)
        allowed = self.seg_col[cols, :1] == self.seg_row[:1, rows]
        if diagonal:
            at = lax.broadcasted_iota(jnp.int32, (cols_count, rows_count), 0)
            allowed = allowed & (at <= lax.broadcasted_iota(jnp.int32, (cols_count, rows_count), 1))
        queries, cots = self.rot[rows, self.part(0)], self.cot[rows, self.own()]
        query_heads, cot_heads = split_heads(queries), split_heads(cots)
        key_heads = split_heads(self.rot[cols, self.part(1)])
        value_heads = split_heads(self.rot[cols, self.part(2)])
        total = self.dq[rows, :]
        for h in range(2):
            scores = contract_cols(key_heads[h], queries)
            probs = jnp.where(allowed, jnp.exp(scores - self.lse[self.pair, h : h + 1, rows]), 0.0)
            dv = dv + product(low(probs), cot_heads[h])
            prob_cot = contract_cols(value_heads[h], cots)
            score_cot = low(probs * (prob_cot - self.delta[h : h + 1, rows]))
            dk = dk + product(score_cot, query_heads[h])
            total = total + contract_rows(score_cot, key_heads[h])
        self.dq[rows, :] = total
        return dk, dv

    def unturn(self, grad, rows):
        return low(grad * self.cos[rows, :] + turn(grad * self.sin[rows, :], -1.0))

    def column(self, j):
        start, half = j * BLOCK, BLOCK // 2
        zero = jnp.zeros((half, PAIR), jnp.float32)
        halves = [
            self.visit(start, BLOCK, start, half, True, zero, zero),
            self.visit(start + half, half, start + half, half, True, zero, zero),
        ]
        state = tuple(jnp.concatenate(pair, axis=0) for pair in zip(*halves))

        def one_row(i, state):
            return lax.cond(
                self.follows(i, j),
                lambda state: self.visit(i * BLOCK, BLOCK, start, BLOCK, False, *state),
                lambda state: state,
                state,
            )

        dk, dv = lax.fori_loop(0, self.blocks, one_row, state)
        cols = aligned(start, BLOCK)
        self.out[cols, self.part(1)] = self.unturn(dk, cols)
        self.out[cols, self.part(2)] = low(dv)

    def finish(self):
        def some(n, _):
            rows = aligned(n * BLOCK, BLOCK)
            self.out[rows, self.part(0)] = self.unturn(self.dq[rows, :] * HEAD_DIM**-0.5, rows)
            return 0

        lax.fori_loop(0, self.blocks, some, 0)


def backward_kernel(info, *refs):
    def follows(i, j):
        return (info[0, j] < info[0, i]) & (info[2, j] >= info[1, i])

    back = Backward(0, *refs, follows)
    back.prepare()

    def one_col(j, _):
        back.column(j)
        return 0

    lax.fori_loop(0, back.blocks, one_col, 0)
    back.finish()


def attention_forward(info, qkv, cos, sin, seg_col, seg_row):
    tokens, width = qkv.shape
    pairs = width // (3 * PAIR)
    whole = lambda p, info: (0, 0)
    return pl.pallas_call(
        forward_kernel,
        grid_spec=pltpu.PrefetchScalarGridSpec(
            num_scalar_prefetch=1,
            grid=(pairs,),
            in_specs=[
                pl.BlockSpec((tokens, 3 * PAIR), lambda p, info: (0, p)),
                pl.BlockSpec((tokens, PAIR), whole),
                pl.BlockSpec((tokens, PAIR), whole),
                pl.BlockSpec((tokens, 1), whole),
                pl.BlockSpec((1, tokens), whole),
            ],
            out_specs=[
                pl.BlockSpec((tokens, 3 * PAIR), lambda p, info: (0, p)),
                pl.BlockSpec((tokens, PAIR), lambda p, info: (0, p)),
                pl.BlockSpec((tokens, PAIR), lambda p, info: (0, p)),
                pl.BlockSpec((1, 2, tokens), lambda p, info: (p, 0, 0)),
            ],
            scratch_shapes=[
                pltpu.VMEM((2, BLOCK, PAIR), jnp.float32),
                pltpu.VMEM((2, BLOCK, PAIR), jnp.float32),
                pltpu.VMEM((2, BLOCK, PAIR), jnp.float32),
            ],
        ),
        out_shape=[
            jax.ShapeDtypeStruct((tokens, width), jnp.bfloat16),
            jax.ShapeDtypeStruct((tokens, pairs * PAIR), jnp.bfloat16),
            jax.ShapeDtypeStruct((tokens, pairs * PAIR), jnp.float32),
            jax.ShapeDtypeStruct((pairs, 2, tokens), jnp.float32),
        ],
        compiler_params=pltpu.CompilerParams(vmem_limit_bytes=VMEM_LIMIT),
        cost_estimate=pl.CostEstimate(flops=tokens * tokens * width, bytes_accessed=10 * tokens * width, transcendentals=tokens * tokens * 2 * pairs),
    )(info, qkv, cos, sin, seg_col, seg_row)


def attention_backward(info, rot, cos, sin, seg_col, seg_row, cot, mixed, lse):
    tokens, width = rot.shape
    pairs = width // (3 * PAIR)
    whole = lambda p, info: (0, 0)
    return pl.pallas_call(
        backward_kernel,
        grid_spec=pltpu.PrefetchScalarGridSpec(
            num_scalar_prefetch=1,
            grid=(pairs,),
            in_specs=[
                pl.BlockSpec((tokens, 3 * PAIR), lambda p, info: (0, p)),
                pl.BlockSpec((tokens, PAIR), whole),
                pl.BlockSpec((tokens, PAIR), whole),
                pl.BlockSpec((tokens, 1), whole),
                pl.BlockSpec((1, tokens), whole),
                pl.BlockSpec((tokens, PAIR), lambda p, info: (0, p)),
                pl.BlockSpec((tokens, PAIR), lambda p, info: (0, p)),
                pl.BlockSpec((1, 2, tokens), lambda p, info: (p, 0, 0)),
            ],
            out_specs=pl.BlockSpec((tokens, 3 * PAIR), lambda p, info: (0, p)),
            scratch_shapes=[
                pltpu.VMEM((2, tokens), jnp.float32),
                pltpu.VMEM((tokens, PAIR), jnp.float32),
            ],
        ),
        out_shape=jax.ShapeDtypeStruct((tokens, width), jnp.bfloat16),
        compiler_params=pltpu.CompilerParams(vmem_limit_bytes=VMEM_LIMIT),
        cost_estimate=pl.CostEstimate(flops=3 * tokens * tokens * width, bytes_accessed=10 * tokens * width, transcendentals=tokens * tokens * 2 * pairs),
    )(info, rot, cos, sin, seg_col, seg_row, cot, mixed, lse)


def swap(values, axis, mask):
    size = lax.axis_size(axis)
    return lax.ppermute(values, axis, [(i, i ^ mask) for i in range(size)])


def masks(size):
    return [1 << n for n in reversed(range(size.bit_length() - 1))]


def offsets(size):
    held = [0]
    for mask in masks(size):
        held = held + [at ^ mask for at in held]
    return held


def gather_rows(rows, axis):
    for mask in masks(lax.axis_size(axis)):
        rows = jnp.concatenate([rows, swap(rows, axis, mask)], axis=0)
    return rows


def scatter_rows(make, count, axis):
    todo = list(reversed(masks(lax.axis_size(axis))))
    half = count // 2
    there = swap(low(make(half, count)), axis, todo[0])
    rows = make(0, half) + wide(there)
    for mask in todo[1:]:
        half = rows.shape[0] // 2
        rows = rows[:half] + wide(swap(low(rows[half:]), axis, mask))
    return rows


def scatter_both(make, count):
    rows = scatter_rows(make, count, "ctx")
    size = lax.axis_size("tp")
    me = lax.axis_index("tp")
    for mask in masks(size):
        half = rows.shape[0] // 2
        upper = (me & mask) != 0
        mine = jnp.where(upper, rows[half:], rows[:half])
        other = jnp.where(upper, rows[:half], rows[half:])
        rows = mine + wide(swap(low(other), "tp", mask))
    return rows


def join_tp(rows):
    size = lax.axis_size("tp")
    me = lax.axis_index("tp")
    for mask in reversed(masks(size)):
        upper = (me & mask) != 0
        other = swap(rows, "tp", mask)
        rows = jnp.where(upper, jnp.concatenate([other, rows], 0), jnp.concatenate([rows, other], 0))
    return rows


def own_part(rows):
    size = lax.axis_size("tp")
    count = rows.shape[0] // size
    return lax.dynamic_slice_in_dim(rows, lax.axis_index("tp") * count, count, 0)


MESH = pl.DeviceIdType.MESH
TILE = 512
STEP = 32


def fits_kernels():
    return lax.axis_size("ctx") == 4 and lax.axis_size("tp") == 2


class Place:
    def __init__(self):
        me = lax.axis_index("ctx")
        x, core = me // 2, me % 2
        self.tp = lax.axis_index("tp")
        self.x = {"ctx": (1 - x) * 2 + core}
        self.core = {"ctx": x * 2 + 1 - core}
        self.cross = {"ctx": (1 - x) * 2 + 1 - core}
        self.y = {"tp": 1 - self.tp}

    def plane(self):
        tp = self.y["tp"]
        return [self.x, self.core, self.cross, self.y] + [dict(device, tp=tp) for device in (self.x, self.core, self.cross)]

    def others(self, axis):
        size, me = lax.axis_size(axis), lax.axis_index(axis)
        return [{axis: (me + n) % size} for n in range(1, size)]


def meet(devices):
    barrier = pltpu.get_barrier_semaphore()
    for device in devices:
        pl.semaphore_signal(barrier, inc=1, device_id=device, device_id_type=MESH)
    pl.semaphore_wait(barrier, len(devices))


class Links:
    def __init__(self, send, recv):
        self.send, self.recv, self.count, self.sent = send, recv, 0, []

    def copy(self, src, dst, device, at=None):
        n = self.count
        self.count += 1
        made = pltpu.make_async_remote_copy(src, dst, self.send.at[n], self.recv.at[n], device_id=device, device_id_type=MESH)
        self.sent.append(made)
        return made

    def drain(self):
        for made in self.sent:
            made.wait_send()


def start_kernel(hidden, grads, segs, gains, attn_in, cot, segs_out, gains_out, hbuf, nbuf, gbuf, gain_row, send, recv, local_sem):
    place, links = Place(), Links(send, recv)
    rows = hidden.shape[0]
    half, quarter = rows // 2, rows // 4
    z = lax.axis_index("fsdp")
    near = [place.x, place.core, place.cross, place.y]
    far = place.others("fsdp")
    meet(near + far)

    def span(block, part, chunk=None):
        if chunk is None:
            return aligned(block * rows + part * half, half)
        return aligned(block * rows + part * half + chunk * quarter, quarter)

    mine, other = place.tp, 1 - place.tp
    tiny = [links.copy(gains, gains_out.at[z], device) for device in far]
    tiny_segs = [links.copy(segs, segs_out.at[n + 1], device) for n, device in enumerate(near[:3])]
    for made in tiny + tiny_segs:
        made.start()
    over_x = {}
    for name, src, dst in (("h", hidden, hbuf), ("g", grads, gbuf)):
        for q in range(2):
            over_x[name, q] = links.copy(src.at[span(0, mine, q)], dst.at[span(1, mine, q)], place.x)
    over_core = {name: links.copy(src, dst.at[aligned(2 * rows, rows)], place.core) for name, src, dst in (("h", hidden, hbuf), ("g", grads, gbuf))}
    for key in (("h", 0), ("h", 1)):
        over_x[key].start()
    over_core["h"].start()
    for key in (("g", 0), ("g", 1)):
        over_x[key].start()
    over_core["g"].start()
    kept = []

    def keep(src, dst):
        made = pltpu.make_async_copy(src, dst, local_sem.at[len(kept)])
        made.start()
        kept.append(made)

    keep(grads, cot.at[aligned(0, rows)])
    gains_out[z] = gains[...]
    segs_out[0] = segs[...]
    for made in tiny:
        made.wait_recv()
    lanes = 128
    groups = gains.shape[0] // 2
    for device in range(gains_out.shape[0]):
        for row in range(groups):
            gain_row[:, pl.ds((device * groups + row) * lanes, lanes)] = gains_out[device, row : row + 1, :]

    def normalize(src, at, block, count):
        def some(n, _):
            there = aligned(at + n * 64, 64)
            values = wide(src[there, :])
            scale = lax.rsqrt(jnp.mean(values * values, axis=1, keepdims=True) + EPS)
            nbuf[aligned(block + n * 64, 64), :] = low(values * scale * gain_row[...])
            return 0

        lax.fori_loop(0, count // 64, some, 0)
        keep(nbuf.at[pl.ds(block, count)], attn_in.at[pl.ds(block, count)])

    normalize(hidden, 0, 0, rows)
    over_y, across, last = {}, {}, {}

    def pass_on(name, buf):
        for q in range(2):
            over_x[name, q].wait_recv()
            over_y[name, q] = links.copy(buf.at[span(1, mine, q)], buf.at[span(1, mine, q)], place.y)
            across[name, q] = links.copy(buf.at[span(1, mine, q)], buf.at[span(3, mine, q)], place.core)
            over_y[name, q].start()
            across[name, q].start()

    def finish(name, buf):
        for q in range(2):
            over_y[name, q].wait_recv()
            last[name, q] = links.copy(buf.at[span(1, other, q)], buf.at[span(3, other, q)], place.core)
            last[name, q].start()

    pass_on("h", hbuf)
    over_core["h"].wait_recv()
    normalize(hbuf, 2 * rows, 2 * rows, rows)
    finish("h", hbuf)
    normalize(hbuf, rows, rows, rows)
    pass_on("g", gbuf)
    for q in range(2):
        across["h", q].wait_recv()
        last["h", q].wait_recv()
    normalize(hbuf, 3 * rows, 3 * rows, rows)
    over_core["g"].wait_recv()
    keep(gbuf.at[aligned(2 * rows, rows)], cot.at[aligned(2 * rows, rows)])
    finish("g", gbuf)
    keep(gbuf.at[aligned(rows, rows)], cot.at[aligned(rows, rows)])
    for q in range(2):
        across["g", q].wait_recv()
        last["g", q].wait_recv()
    keep(gbuf.at[aligned(3 * rows, rows)], cot.at[aligned(3 * rows, rows)])
    for made in tiny_segs:
        made.wait_recv()
    links.drain()
    for made in kept:
        made.wait()


def start_exchange(hidden, grads, segments, attn_gain, mlp_gain):
    rows, width = hidden.shape
    fsdp = lax.axis_size("fsdp")
    segs = jnp.concatenate([segments.reshape(-1, 128), jnp.zeros((8 - rows // 128, 128), jnp.int32)], axis=0)
    gains = wide(jnp.concatenate([attn_gain, mlp_gain])).reshape(-1, 128)
    vmem = pl.BlockSpec(memory_space=pltpu.VMEM)
    hbm = pl.BlockSpec(memory_space=pl.ANY)
    tokens = 4 * rows
    attn_in, cot, segs, gains = pl.pallas_call(
        start_kernel,
        in_specs=[vmem] * 4,
        out_specs=[hbm, hbm, vmem, vmem],
        out_shape=[
            jax.ShapeDtypeStruct((tokens, width), jnp.bfloat16),
            jax.ShapeDtypeStruct((tokens, width), jnp.bfloat16),
            jax.ShapeDtypeStruct((4, 8, 128), jnp.int32),
            jax.ShapeDtypeStruct((fsdp,) + gains.shape, jnp.float32),
        ],
        scratch_shapes=[
            pltpu.VMEM((tokens, width), jnp.bfloat16),
            pltpu.VMEM((tokens, width), jnp.bfloat16),
            pltpu.VMEM((tokens, width), jnp.bfloat16),
            pltpu.VMEM((1, width), jnp.float32),
            pltpu.SemaphoreType.DMA((fsdp + 32,)),
            pltpu.SemaphoreType.DMA((fsdp + 32,)),
            pltpu.SemaphoreType.DMA((8,)),
        ],
        compiler_params=pltpu.CompilerParams(collective_id=0, has_side_effects=True, vmem_limit_bytes=VMEM_LIMIT),
        cost_estimate=pl.CostEstimate(flops=0, bytes_accessed=200_000_000, transcendentals=0),
    )(hidden, grads, segs, gains)
    segs = segs[:, : rows // 128].reshape(tokens)
    gains = jnp.transpose(gains.reshape(fsdp, 2, -1), (1, 0, 2)).reshape(2, width)
    return attn_in, cot, segs, gains


def scatter_scratch(rows, width):
    part, half = rows // 8, width // 2
    return [
        pltpu.VMEM((4, part, width), jnp.bfloat16),
        pltpu.VMEM((4, part, width), jnp.bfloat16),
        pltpu.VMEM((6, part, half), jnp.bfloat16),
        pltpu.VMEM((6, part, half), jnp.bfloat16),
        pltpu.VMEM((2, part, half), jnp.float32),
        pltpu.VMEM((part, width), jnp.float32),
        pltpu.SemaphoreType.DMA((14,)),
        pltpu.SemaphoreType.DMA((14,)),
    ]


class Scatter:
    def __init__(self, place, make, count, refs, first=("x", "y")):
        self.place, self.make = place, make
        self.hi, self.core_in, self.out, self.come, self.wait, self.total, send, recv = refs
        self.part = count // 8
        self.half = self.total.shape[1] // 2
        self.links = Links(send, recv)
        self.core = {}
        for side in range(2):
            cols = pl.ds(side * self.half, self.half)
            for n in range(4):
                self.core[n, side] = self.links.copy(self.hi.at[n, :, cols], self.core_in.at[n, :, cols], place.core)
        self.send, self.away, self.stays = [], {}, {}
        for side, link in enumerate(first):
            to, then = (place.x, place.y) if link == "x" else (place.y, place.x)
            for n, device in enumerate((to, to, then)):
                at = 3 * side + n
                self.send.append(self.links.copy(self.out.at[at], self.come.at[at], device))
            second, stay = (1, 2) if link == "x" else (2, 1)
            self.away[0, side], self.away[second, side] = 3 * side, 3 * side + 1
            self.stays[side] = stay

    def rows(self, n):
        tp = self.place.tp
        part = (1 - tp) + (n % 2) * (2 * tp - 1)
        return ((1 - n // 2) * 2 + part) * self.part

    def columns(self, side, each):
        tiles = self.half // TILE

        def one(n, _):
            each(aligned(side * self.half + n * TILE, TILE), aligned(n * TILE, TILE))
            return 0

        lax.fori_loop(0, tiles, one, 0)

    def to_core(self, n, side):
        rows = aligned(4 * self.part + self.rows(n), self.part)

        def each(cols, _):
            self.hi[n, :, cols] = low(self.make(rows, cols))

        self.columns(side, each)
        self.core[n, side].start()

    def to_links(self, n, side):
        rows = aligned(self.rows(n), self.part)
        self.core[n, side].wait_recv()

        def each(cols, at):
            value = self.make(rows, cols) + wide(self.core_in[n, :, cols])
            if (n, side) in self.away:
                self.out[self.away[n, side], :, at] = low(value)
            elif n == 3:
                self.total[:, cols] = value
            else:
                self.wait[side, :, at] = value

        self.columns(side, each)
        if (n, side) in self.away:
            self.send[self.away[n, side]].start()

    def units(self):
        return (
            [(0, side) for side in range(2)]
            + [(n, side) for n in (1, 2) for side in range(2) if (n, side) in self.away]
            + [(self.stays[side], side) for side in range(2)]
            + [(3, side) for side in range(2)]
        )

    def start(self, waits=()):
        units = self.units()
        ahead = 2
        waits = list(waits) + [()] * 3
        for at, unit in enumerate(units[:ahead]):
            for made in waits[at]:
                made.wait()
            self.to_core(*unit)
        for made in waits[2]:
            made.wait()
        for at, unit in enumerate(units):
            self.to_links(*unit)
            if at + ahead < len(units):
                self.to_core(*units[at + ahead])

    def turn(self):
        for side in range(2):
            came, goes = 3 * side, 3 * side + 2
            self.send[came].wait_recv()

            def each(_, at):
                self.out[goes, :, at] = low(self.wait[side, :, at] + wide(self.come[came, :, at]))

            self.columns(side, each)
            self.send[goes].start()

    def finish(self):
        for side in range(2):
            for n in (1, 2):
                self.send[3 * side + n].wait_recv()
            cols = pl.ds(side * self.half, self.half)
            self.total[:, cols] = self.total[:, cols] + wide(self.come[3 * side + 1]) + wide(self.come[3 * side + 2])
        self.links.drain()


def gather_plane(place, links, mine, full, part):
    half = mine.shape[1] // 2
    left, right = pl.ds(0, half), pl.ds(half, half)
    own, other = place.tp, 1 - place.tp

    def rows(block, tp):
        return aligned((block * 2 + tp) * part, part)

    y_left = links.copy(mine.at[:, left], full.at[rows(0, own), left], place.y)
    x_right = links.copy(mine.at[:, right], full.at[rows(1, own), right], place.x)
    y_right = links.copy(mine.at[:, right], full.at[rows(0, own), right], place.y)
    x_left = links.copy(mine.at[:, left], full.at[rows(1, own), left], place.x)
    core = [links.copy(mine, full.at[rows(2, own)], place.core)]
    for made in (y_left, x_right, y_right, x_left, core[0]):
        made.start()

    def relay(come, block, tp, cols, onward=None):
        come.wait_recv()
        here = full.at[rows(block, tp), cols]
        if onward == "x":
            made = links.copy(here, full.at[rows(1, tp), cols], place.x)
        elif onward == "y":
            made = links.copy(here, full.at[rows(block, tp), cols], place.y)
        if onward:
            made.start()
        over = links.copy(here, full.at[rows(block + 2, tp), cols], place.core)
        over.start()
        core.append(over)
        return made if onward else None

    far_left = relay(y_left, 0, other, left, "x")
    far_right = relay(x_right, 1, own, right, "y")
    relay(y_right, 0, other, right)
    relay(x_left, 1, own, left)
    relay(far_left, 1, other, left)
    relay(far_right, 1, other, right)
    for made in core:
        made.wait_recv()


def load(sems, pairs):
    made = [pltpu.make_async_copy(src, dst, sems.at[n]) for n, (src, dst) in enumerate(pairs)]
    for copy in made:
        copy.start()
    return made


def forward_mid_kernel(mixed, weight, hidden, gain, full, resid_out, mine, *refs):
    place = Place()
    scatter_refs, (send, recv, local_sem) = refs[:-3], refs[-3:]
    count = mixed.shape[0]
    part = count // 8
    meet([place.x, place.core, place.y])
    scatter = Scatter(place, lambda rows, cols: contract_cols(mixed[rows, :], weight[cols, weight.shape[1] - mixed.shape[1] :]), count, scatter_refs)
    scatter.start()
    scatter.turn()
    scatter.finish()
    step = STEP

    def some(n, _):
        rows = aligned(n * step, step)
        values = wide(hidden[aligned(place.tp * part + n * step, step), :]) + scatter.total[rows, :]
        resid_out[rows, :] = values
        scale = lax.rsqrt(jnp.mean(values * values, axis=1, keepdims=True) + EPS)
        mine[rows, :] = low(values * scale * gain[...])
        return 0

    lax.fori_loop(0, part // step, some, 0)
    stay = pltpu.make_async_copy(mine, full.at[aligned(place.tp * part, part)], local_sem)
    stay.start()
    links = Links(send, recv)
    gather_plane(place, links, mine, full, part)
    links.drain()
    stay.wait()


def mid_scratch(count, width):
    return [pltpu.VMEM((count // 8, width), jnp.bfloat16)] + scatter_scratch(count, width) + [
        pltpu.SemaphoreType.DMA((16,)),
        pltpu.SemaphoreType.DMA((16,)),
        pltpu.SemaphoreType.DMA,
    ]


def forward_mid(mixed, weight, hidden, gain):
    count, width = mixed.shape[0], weight.shape[0]
    vmem = pl.BlockSpec(memory_space=pltpu.VMEM)
    return pl.pallas_call(
        forward_mid_kernel,
        in_specs=[vmem] * 4,
        out_specs=[pl.BlockSpec(memory_space=pl.ANY), vmem],
        out_shape=[jax.ShapeDtypeStruct((count, width), jnp.bfloat16), jax.ShapeDtypeStruct((count // 8, width), jnp.float32)],
        scratch_shapes=mid_scratch(count, width),
        compiler_params=pltpu.CompilerParams(collective_id=1, has_side_effects=True, vmem_limit_bytes=VMEM_LIMIT),
        cost_estimate=pl.CostEstimate(flops=0, bytes_accessed=300_000_000, transcendentals=0),
    )(mixed, weight, hidden, gain[None, :])


def norm_back(values, scale, gain, cot):
    scaled = cot * gain
    lean = jnp.mean(values * scaled, axis=1, keepdims=True)
    return scale * scaled - values * (scale * scale * scale) * lean, cot * (values * scale)


def backward_mid_kernel(
    hidden_hbm, weights_hbm, resid_hbm, grads_hbm, gain, full, cot_out, gain_out,
    hidden_cot, weights, resid, grads, sems, mine, *refs
):
    place = Place()
    scatter_refs, (send, recv, local_sem) = refs[:-3], refs[-3:]
    count = hidden_cot.shape[0]
    part = count // 8
    width = weights.shape[0]
    lower, upper = pl.ds(0, count // 2), pl.ds(count // 2, count // 2)
    left, right = pl.ds(0, width // 2), pl.ds(width // 2, width // 2)
    loads = load(
        sems,
        [
            (weights_hbm.at[left], weights.at[left]),
            (hidden_hbm.at[upper], hidden_cot.at[upper]),
            (weights_hbm.at[right], weights.at[right]),
            (hidden_hbm.at[lower], hidden_cot.at[lower]),
            (resid_hbm, resid),
            (grads_hbm.at[aligned(place.tp * part, part)], grads),
        ],
    )
    meet([place.x, place.core, place.y])

    def make(rows, cols):
        return contract_cols(hidden_cot[rows, :], weights[cols, :])

    scatter = Scatter(place, make, count, scatter_refs)
    scatter.start((loads[:2], loads[2:3], loads[3:4]))
    scatter.turn()
    scatter.finish()
    for made in loads[4:]:
        made.wait()
    step = STEP

    def some(n, sums):
        rows = aligned(n * step, step)
        values = resid[rows, :]
        scale = lax.rsqrt(jnp.mean(values * values, axis=1, keepdims=True) + EPS)
        back, terms = norm_back(values, scale, gain[...], scatter.total[rows, :])
        cot = wide(grads[rows, :]) + back
        cot_out[rows, :] = cot
        mine[rows, :] = low(cot)
        return sums + jnp.sum(terms, axis=0, keepdims=True)

    gain_out[...] = lax.fori_loop(0, part // step, some, jnp.zeros(gain.shape, jnp.float32))
    stay = pltpu.make_async_copy(mine, full.at[aligned(place.tp * part, part)], local_sem)
    stay.start()
    links = Links(send, recv)
    gather_plane(place, links, mine, full, part)
    links.drain()
    stay.wait()


def backward_mid(hidden_cot, weights, resid, grads, gain):
    count, width = hidden_cot.shape[0], weights.shape[0]
    vmem = pl.BlockSpec(memory_space=pltpu.VMEM)
    hbm = pl.BlockSpec(memory_space=pl.ANY)
    return pl.pallas_call(
        backward_mid_kernel,
        in_specs=[hbm] * 4 + [vmem],
        out_specs=[pl.BlockSpec(memory_space=pl.ANY), vmem, vmem],
        out_shape=[
            jax.ShapeDtypeStruct((count, width), jnp.bfloat16),
            jax.ShapeDtypeStruct((count // 8, width), jnp.float32),
            jax.ShapeDtypeStruct((1, width), jnp.float32),
        ],
        scratch_shapes=[
            pltpu.VMEM(hidden_cot.shape, jnp.bfloat16),
            pltpu.VMEM(weights.shape, jnp.bfloat16),
            pltpu.VMEM(resid.shape, jnp.float32),
            pltpu.VMEM(resid.shape, jnp.bfloat16),
            pltpu.SemaphoreType.DMA((6,)),
        ]
        + mid_scratch(count, width),
        compiler_params=pltpu.CompilerParams(collective_id=2, has_side_effects=True, vmem_limit_bytes=VMEM_LIMIT),
        cost_estimate=pl.CostEstimate(flops=0, bytes_accessed=300_000_000, transcendentals=0),
    )(hidden_cot, weights, resid, grads, gain[None, :])


def input_kernel(cots, weights, cot_hbm, hidden_hbm, gain, gain_two, grad_out, gains_out, resid_cot, hidden, sems, sums, come, *refs):
    place = Place()
    (send, recv), refs = refs[-2:], refs[:-2]
    count = cots.shape[0]
    part = count // 8
    loads = load(sems, [(cot_hbm, resid_cot), (hidden_hbm.at[aligned(place.tp * part, part)], hidden)])
    meet(place.plane() + place.others("fsdp"))
    scatter = Scatter(place, lambda rows, cols: contract_cols(cots[rows, :], weights[cols, : cots.shape[1]]), count, refs, ("y", "y"))
    links = Links(send, recv)
    scatter.start()
    scatter.turn()
    scatter.finish()
    for made in loads:
        made.wait()
    step = STEP

    def some(n, total):
        rows = aligned(n * step, step)
        values = wide(hidden[rows, :])
        scale = lax.rsqrt(jnp.mean(values * values, axis=1, keepdims=True) + EPS)
        back, terms = norm_back(values, scale, gain[...], scatter.total[rows, :])
        grad_out[rows, :] = low(resid_cot[rows, :] + back)
        return total + jnp.sum(terms, axis=0, keepdims=True)

    sums[0, 0:1, :] = lax.fori_loop(0, part // step, some, jnp.zeros(gain.shape, jnp.float32))
    sums[0, 1:2, :] = gain_two[...]
    total = sums[0]
    for stage, devices in enumerate((place.plane(), place.others("fsdp"))):
        at = stage * len(place.plane())
        made = [links.copy(sums.at[stage], come.at[at + n], device) for n, device in enumerate(devices)]
        for copy in made:
            copy.start()
        for n, copy in enumerate(made):
            copy.wait_recv()
            total = total + come[at + n]
        sums[stage + 1] = total
    gains_out[...] = total
    links.drain()


def input_exchange(cots, weights, resid_cot, hidden, gain, gain_two):
    count, width = cots.shape[0], weights.shape[0]
    fsdp = lax.axis_size("fsdp")
    vmem = pl.BlockSpec(memory_space=pltpu.VMEM)
    return pl.pallas_call(
        input_kernel,
        in_specs=[vmem] * 2 + [pl.BlockSpec(memory_space=pl.ANY)] * 2 + [vmem] * 2,
        out_specs=[vmem, vmem],
        out_shape=[jax.ShapeDtypeStruct((count // 8, width), jnp.bfloat16), jax.ShapeDtypeStruct((2, width), jnp.float32)],
        scratch_shapes=[
            pltpu.VMEM(resid_cot.shape, jnp.float32),
            pltpu.VMEM(resid_cot.shape, jnp.bfloat16),
            pltpu.SemaphoreType.DMA((2,)),
            pltpu.VMEM((3, 2, width), jnp.float32),
            pltpu.VMEM((6 + fsdp, 2, width), jnp.float32),
        ]
        + scatter_scratch(count, width)
        + [pltpu.SemaphoreType.DMA((6 + fsdp,)), pltpu.SemaphoreType.DMA((6 + fsdp,))],
        compiler_params=pltpu.CompilerParams(collective_id=3, has_side_effects=True, vmem_limit_bytes=VMEM_LIMIT),
        cost_estimate=pl.CostEstimate(flops=0, bytes_accessed=180_000_000, transcendentals=0),
    )(cots, weights, resid_cot, hidden, gain[None, :], gain_two)


def attention_output_kernel(
    rot_hbm, cos_hbm, sin_hbm, seg_col, seg_row, cot_hbm, mixed_hbm, lse, hidden_act, down, resid_hbm, cots, out,
    rot, cos, sin, cot, mixed, resid, sems, delta, dq, *refs
):
    place = Place()
    count = hidden_act.shape[0]
    me = lax.axis_index("ctx")
    blocks = count // BLOCK
    per = count // 4 // BLOCK

    def at(block):
        n = block // per
        return (((me // 2 + n % 2) % 2) * 2 + (me % 2 + n // 2) % 2) * per + block % per

    def follows(i, j):
        return (at(j) < at(i)) & (at(i) - at(j) <= blocks // 2)

    loads = load(
        sems, [(rot_hbm, rot), (cos_hbm, cos), (sin_hbm, sin), (cot_hbm, cot), (mixed_hbm, mixed), (resid_hbm, resid)]
    )
    meet([place.x, place.core, place.y])
    scatter = Scatter(place, lambda rows, cols: product(hidden_act[rows, :], down[:, cols]), count, refs, ("y", "y"))
    scatter.start()
    for made in loads:
        made.wait()
    pairs = rot.shape[1] // (3 * PAIR)
    steps = pairs * blocks

    def step(n, _):
        back = Backward(n // blocks, rot, cos, sin, seg_col, seg_row, cot, mixed, lse, cots, delta, dq, follows)

        @pl.when(n % blocks == 0)
        def _():
            back.prepare()

        back.column(n % blocks)

        @pl.when(n % blocks == blocks - 1)
        def _():
            back.finish()

        @pl.when(n == steps // 4 - 1)
        def _():
            scatter.turn()

        return 0

    lax.fori_loop(0, steps, step, 0)
    scatter.finish()
    out[...] = low(resid[...] + scatter.total[...])


def attention_output(rot, cos, sin, seg_col, seg_row, cot, mixed, lse, hidden_act, down, resid):
    count, width = hidden_act.shape[0], down.shape[1]
    vmem = pl.BlockSpec(memory_space=pltpu.VMEM)
    hbm = pl.BlockSpec(memory_space=pl.ANY)
    return pl.pallas_call(
        attention_output_kernel,
        in_specs=[hbm] * 3 + [vmem] * 2 + [hbm] * 2 + [vmem] * 3 + [hbm],
        out_specs=[vmem, vmem],
        out_shape=[
            jax.ShapeDtypeStruct(rot.shape, jnp.bfloat16),
            jax.ShapeDtypeStruct((count // 8, width), jnp.bfloat16),
        ],
        scratch_shapes=[pltpu.VMEM(array.shape, array.dtype) for array in (rot, cos, sin, cot, mixed, resid)]
        + [
            pltpu.SemaphoreType.DMA((6,)),
            pltpu.VMEM((2, count), jnp.float32),
            pltpu.VMEM((count, PAIR), jnp.float32),
        ]
        + scatter_scratch(count, width),
        compiler_params=pltpu.CompilerParams(collective_id=4, has_side_effects=True, vmem_limit_bytes=VMEM_LIMIT),
        cost_estimate=pl.CostEstimate(flops=0, bytes_accessed=220_000_000, transcendentals=0),
    )(rot, cos, sin, seg_col, seg_row, cot, mixed, lse, hidden_act, down, resid)


def hidden_cot_kernel(cot, down, gate_slope, up_slope, out):
    cols = down.shape[0]

    def some(n, _):
        at = aligned(n * TILE, TILE)
        back = contract_cols(cot[...], down[at, :])
        out[:, at] = low(back * gate_slope[:, at])
        out[:, aligned(cols + n * TILE, TILE)] = low(back * up_slope[:, at])
        return 0

    lax.fori_loop(0, cols // TILE, some, 0)


def hidden_cots(cot, down, gate_slope, up_slope):
    count, width = cot.shape
    cols = down.shape[0]
    rows = 512
    side = pl.BlockSpec((rows, cols), lambda n: (n, 0))
    return pl.pallas_call(
        hidden_cot_kernel,
        grid=(count // rows,),
        in_specs=[pl.BlockSpec((rows, width), lambda n: (n, 0)), pl.BlockSpec((cols, width), lambda n: (0, 0)), side, side],
        out_specs=pl.BlockSpec((rows, 2 * cols), lambda n: (n, 0)),
        out_shape=jax.ShapeDtypeStruct((count, 2 * cols), jnp.bfloat16),
        compiler_params=pltpu.CompilerParams(vmem_limit_bytes=VMEM_LIMIT),
        cost_estimate=pl.CostEstimate(flops=2 * count * width * cols, bytes_accessed=2 * count * (width + 4 * cols), transcendentals=0),
    )(cot, down, gate_slope, up_slope)


def take_attention_kernel(at, query, key, value, out, taken):
    pairs = query.shape[1] // PAIR
    for p in range(pairs):
        for n, part in enumerate((query, key, value)):
            taken[:, (3 * p + n) * PAIR : (3 * p + n + 1) * PAIR] = part[:, p * PAIR : (p + 1) * PAIR]
    taken[:, 3 * pairs * PAIR :] = out[...].T


def take_attention(me, query, key, value, out, count):
    depth = query.shape[0]
    block = pl.BlockSpec((depth, count), lambda n, at: (0, at[0]))
    return pl.pallas_call(
        take_attention_kernel,
        grid_spec=pltpu.PrefetchScalarGridSpec(
            num_scalar_prefetch=1,
            grid=(1,),
            in_specs=[block] * 3 + [pl.BlockSpec((count, depth), lambda n, at: (at[0], 0))],
            out_specs=pl.BlockSpec((depth, 4 * count), lambda n, at: (0, 0)),
        ),
        out_shape=jax.ShapeDtypeStruct((depth, 4 * count), query.dtype),
        compiler_params=pltpu.CompilerParams(vmem_limit_bytes=VMEM_LIMIT),
    )(me, query, key, value, out)


def take_hidden_kernel(at, gate, up, down, both, rows):
    count = gate.shape[1]
    both[:, :count] = gate[...]
    both[:, count:] = up[...]
    rows[...] = down[...]


def take_hidden(me, gate, up, down, count):
    depth = gate.shape[0]
    block = pl.BlockSpec((depth, count), lambda n, at: (0, at[0]))
    return pl.pallas_call(
        take_hidden_kernel,
        grid_spec=pltpu.PrefetchScalarGridSpec(
            num_scalar_prefetch=1,
            grid=(1,),
            in_specs=[block] * 2 + [pl.BlockSpec((count, depth), lambda n, at: (at[0], 0))],
            out_specs=[pl.BlockSpec((depth, 2 * count), lambda n, at: (0, 0)), pl.BlockSpec((count, depth), lambda n, at: (0, 0))],
        ),
        out_shape=[jax.ShapeDtypeStruct((depth, 2 * count), gate.dtype), jax.ShapeDtypeStruct((count, depth), down.dtype)],
        compiler_params=pltpu.CompilerParams(vmem_limit_bytes=VMEM_LIMIT),
    )(me, gate, up, down)


def first_swaps(block):
    pieces = [block]
    for mask in masks(lax.axis_size("ctx"))[:-1]:
        pieces = pieces + [swap(piece, "ctx", mask) for piece in pieces]
    return pieces


def last_swap(pieces):
    return pieces + [swap(piece, "ctx", 1) for piece in pieces]


def order_of_pieces():
    return lax.axis_index("ctx") ^ jnp.array(offsets(lax.axis_size("ctx")), jnp.int32)


def place_kernel(at, *refs):
    out = refs[-1]
    for n, piece in enumerate(refs[:-1]):

        @pl.when(pl.program_id(0) == n)
        def _():
            out[...] = wide(piece[...])


def place_pieces(pieces, axis):
    block = pieces[0].shape
    shape = list(block)
    shape[axis] *= len(pieces)
    return pl.pallas_call(
        place_kernel,
        grid_spec=pltpu.PrefetchScalarGridSpec(
            num_scalar_prefetch=1,
            grid=(len(pieces),),
            in_specs=[pl.BlockSpec(block, lambda n, at: (0, 0))] * len(pieces),
            out_specs=pl.BlockSpec(block, lambda n, at: (at[n], 0) if axis == 0 else (0, at[n])),
        ),
        out_shape=jax.ShapeDtypeStruct(shape, jnp.float32),
        compiler_params=pltpu.CompilerParams(vmem_limit_bytes=VMEM_LIMIT),
        cost_estimate=pl.CostEstimate(flops=0, bytes_accessed=6 * math.prod(shape), transcendentals=0),
    )(order_of_pieces(), *pieces)


def join_kernel(at, *refs):
    outs = refs[-2:]
    for n in range(2):

        @pl.when(pl.program_id(0) == n)
        def _():
            for m, out in enumerate(outs):
                out[...] = refs[2 * m + n][...]


def join_rows(first, second):
    rows, width = first[0].shape
    me = lax.axis_index("tp")
    whole = pl.BlockSpec((rows, width), lambda n, at: (0, 0))
    return pl.pallas_call(
        join_kernel,
        grid_spec=pltpu.PrefetchScalarGridSpec(
            num_scalar_prefetch=1,
            grid=(2,),
            in_specs=[whole] * 4,
            out_specs=[pl.BlockSpec((rows, width), lambda n, at: (at[n], 0))] * 2,
        ),
        out_shape=[jax.ShapeDtypeStruct((2 * rows, width), first[0].dtype)] * 2,
        compiler_params=pltpu.CompilerParams(vmem_limit_bytes=VMEM_LIMIT),
        cost_estimate=pl.CostEstimate(flops=0, bytes_accessed=16 * rows * width, transcendentals=0),
    )(jnp.stack([me, 1 - me]), *first, *second)


def place_gate_up_kernel(at, *refs):
    pieces, (gate, up) = refs[:-2], refs[-2:]
    count = gate.shape[1]
    for n, piece in enumerate(pieces):

        @pl.when(pl.program_id(0) == n)
        def _():
            gate[...] = wide(piece[:, :count])
            up[...] = wide(piece[:, count:])


def place_gate_up(pieces):
    rows, cols = pieces[0].shape
    count, whole = cols // 2, cols // 2 * len(pieces)
    side = pl.BlockSpec((rows, count), lambda n, at: (0, at[n]))
    return pl.pallas_call(
        place_gate_up_kernel,
        grid_spec=pltpu.PrefetchScalarGridSpec(
            num_scalar_prefetch=1,
            grid=(len(pieces),),
            in_specs=[pl.BlockSpec((rows, cols), lambda n, at: (0, 0))] * len(pieces),
            out_specs=[side] * 2,
        ),
        out_shape=[jax.ShapeDtypeStruct((rows, whole), jnp.float32)] * 2,
        compiler_params=pltpu.CompilerParams(vmem_limit_bytes=VMEM_LIMIT),
        cost_estimate=pl.CostEstimate(flops=0, bytes_accessed=12 * rows * whole, transcendentals=0),
    )(order_of_pieces(), *pieces)


def place_attention_kernel(at, *refs):
    pieces, outs = refs[:-4], refs[-4:]
    count = outs[0].shape[1]
    pairs = count // PAIR
    for n, piece in enumerate(pieces):

        @pl.when(pl.program_id(0) == n)
        def _():
            for p in range(pairs):
                for m in range(3):
                    outs[m][:, p * PAIR : (p + 1) * PAIR] = wide(piece[:, (3 * p + m) * PAIR : (3 * p + m + 1) * PAIR])
            outs[3][...] = wide(piece[:, 3 * count :]).T


def place_attention(pieces):
    depth, count = pieces[0].shape[0], pieces[0].shape[1] // 4
    whole = len(pieces) * count
    side = pl.BlockSpec((depth, count), lambda n, at: (0, at[n]))
    return pl.pallas_call(
        place_attention_kernel,
        grid_spec=pltpu.PrefetchScalarGridSpec(
            num_scalar_prefetch=1,
            grid=(len(pieces),),
            in_specs=[pl.BlockSpec(pieces[0].shape, lambda n, at: (0, 0))] * len(pieces),
            out_specs=[side] * 3 + [pl.BlockSpec((count, depth), lambda n, at: (at[n], 0))],
        ),
        out_shape=[jax.ShapeDtypeStruct((depth, whole), jnp.float32)] * 3 + [jax.ShapeDtypeStruct((whole, depth), jnp.float32)],
        compiler_params=pltpu.CompilerParams(vmem_limit_bytes=VMEM_LIMIT),
        cost_estimate=pl.CostEstimate(flops=0, bytes_accessed=24 * depth * whole, transcendentals=0),
    )(order_of_pieces(), *pieces)


def local(
    hidden_in,
    out_grad,
    segment_ids,
    attn_gain,
    w_query,
    w_key,
    w_value,
    w_out,
    mlp_gain,
    w_gate,
    w_up,
    w_down,
):
    group = lax.axis_size("ctx")
    me = lax.axis_index("ctx")
    local_rows = hidden_in.shape[1]
    tokens = local_rows * group
    head_cols = w_query.shape[1] // group
    ff_cols = w_gate.shape[1] // group

    def gather(weight, axis):
        return lax.all_gather(weight, "fsdp", axis=axis, tiled=True)

    def settle(part, axis):
        return lax.psum_scatter(part, "fsdp", scatter_dimension=axis, tiled=True)

    at = me[None]
    w_attn = gather(take_attention(at, w_query, w_key, w_value, w_out, head_cols), 0)
    qkv_cols = 3 * head_cols
    w_qkv, w_out_t = w_attn[:, :qkv_cols], w_attn[:, qkv_cols:]
    own_gate_up, own_down = take_hidden(at, w_gate, w_up, w_down, ff_cols)
    full_gate_up = gather(own_gate_up, 0)
    full_down = gather(own_down, 1)

    kernels = fits_kernels()
    if kernels:
        attn_in, branch_cot, segments, gains = start_exchange(hidden_in[0], out_grad[0], segment_ids[0], attn_gain, mlp_gain)
        gain_one, gain_two = gains[0], gains[1]
    else:
        gains = wide(gather(jnp.stack([attn_gain, mlp_gain]), 1))
        gain_one, gain_two = gains[0], gains[1]
        rows_in = wide(hidden_in[0])
        r1 = lax.rsqrt(jnp.mean(rows_in * rows_in, axis=-1, keepdims=True) + EPS)
        attn_in = gather_rows(low(rows_in * r1 * gain_one), "ctx")
        segments = gather_rows(segment_ids[0], "ctx")
        branch_cot = gather_rows(out_grad[0], "ctx")

    firsts = jnp.stack([(me ^ at) * local_rows for at in offsets(group)])
    positions = (firsts[:, None] + jnp.arange(local_rows, dtype=jnp.int32)[None, :]).reshape(tokens)
    exponents = jnp.arange(0, HEAD_DIM, 2).astype(jnp.float32) / HEAD_DIM
    inverse = jnp.float32(ROPE_BASE) ** (-exponents)
    angles = positions.astype(jnp.float32)[:, None] * inverse[None, :]
    cos = jnp.tile(jnp.cos(angles), (1, 4))
    sin = jnp.tile(jnp.sin(angles), (1, 4))
    info = jnp.stack([positions[::BLOCK], segments[::BLOCK], segments[BLOCK - 1 :: BLOCK]])
    seg_col, seg_row = segments[:, None], segments[None, :]

    qkv = product(attn_in, w_qkv)
    rot, mixed, mixed_wide, lse = attention_forward(info, qkv, cos, sin, seg_col, seg_row)

    own_in = wide(own_part(hidden_in[0]))
    if kernels:
        mlp_in, resid = forward_mid(mixed, w_attn, hidden_in[0], gain_two)
    else:
        part = scatter_both(lambda lo, hi: contract_cols(mixed[lo:hi], w_out_t), tokens)
        resid = own_in + part
        r2 = lax.rsqrt(jnp.mean(resid * resid, axis=-1, keepdims=True) + EPS)
        mlp_in = gather_rows(join_tp(low(resid * r2 * gain_two)), "ctx")
    acts = product(mlp_in, full_gate_up)
    gate_act, up_act = acts[:, :ff_cols], acts[:, ff_cols:]
    sigmoid = jax.nn.sigmoid(gate_act)
    hidden = low(gate_act * sigmoid * up_act)
    gate_slope = low(up_act * sigmoid * (1.0 + gate_act * (1.0 - sigmoid)))
    up_slope = low(gate_act * sigmoid)
    hidden, gate_slope, up_slope = lax.optimization_barrier((hidden, gate_slope, up_slope))
    down_part = low(contract_rows(hidden, branch_cot))
    down_part, full_down, branch_cot = lax.optimization_barrier((down_part, full_down, branch_cot))
    down_own = settle(down_part, 1)

    hidden_cot = hidden_cots(branch_cot, full_down, gate_slope, up_slope)
    gate_up_part = low(contract_rows(mlp_in, hidden_cot))
    gate_up_own = settle(gate_up_part, 0)
    if kernels:
        hidden_cot, gate_up_part = lax.optimization_barrier((hidden_cot, gate_up_part))
        attn_cot, resid_cot, gain_two_part = backward_mid(hidden_cot, full_gate_up, resid, out_grad[0], gain_two)
    else:
        mlp_in_cot = scatter_both(lambda lo, hi: contract_cols(hidden_cot[lo:hi], full_gate_up), tokens)
        back, terms = norm_back(resid, r2, gain_two, mlp_in_cot)
        gain_two_part = jnp.sum(terms, axis=0, keepdims=True)
        resid_cot = wide(own_part(out_grad[0])) + back
        attn_cot = gather_rows(join_tp(low(resid_cot)), "ctx")
    mixed_cot = low(product(attn_cot, w_out_t))
    out_part = low(contract_rows(attn_cot, mixed))
    mixed_cot, out_part, down_own = lax.optimization_barrier((mixed_cot, out_part, down_own))
    down_pieces = first_swaps(down_own)
    if kernels:
        cots, output = attention_output(rot, cos, sin, seg_col, seg_row, mixed_cot, mixed_wide, lse, hidden, full_down, resid)
        other_output = swap(output, "tp", 1)
    else:
        cots = attention_backward(info, rot, cos, sin, seg_col, seg_row, mixed_cot, mixed_wide, lse)
    cots, *down_pieces = lax.optimization_barrier((cots, *down_pieces))
    qkv_part = low(contract_rows(attn_in, cots))
    attn_part = jnp.concatenate([qkv_part, out_part], axis=1)
    attn_own = settle(attn_part, 0)
    if kernels:
        cots, attn_part, gate_up_own = lax.optimization_barrier((cots, attn_part, gate_up_own))
        gate_up_pieces = first_swaps(gate_up_own)
        input_grad, gain_sums = input_exchange(cots, w_attn, resid_cot, hidden_in[0], gain_one, gain_two_part)
        input_grad, *gate_up_pieces = lax.optimization_barrier((input_grad, *gate_up_pieces))
        other_input = swap(input_grad, "tp", 1)
        output, input_grad = join_rows((output, other_output), (input_grad, other_input))
    else:
        gate_up_pieces = first_swaps(gate_up_own)
        out_sum = scatter_both(lambda lo, hi: product(hidden[lo:hi], full_down), tokens)
        output = join_tp(low(resid + out_sum))
        attn_in_cot = scatter_both(lambda lo, hi: contract_cols(cots[lo:hi], w_qkv), tokens)
        back, terms = norm_back(own_in, own_part(r1), gain_one, attn_in_cot)
        input_grad = join_tp(low(resid_cot + back))
        gain_sums = lax.psum(jnp.concatenate([jnp.sum(terms, axis=0, keepdims=True), gain_two_part]), ("fsdp", "ctx", "tp"))
    attn_pieces = first_swaps(attn_own)
    down_pieces = last_swap(down_pieces)
    down_grad = place_pieces(down_pieces, 0)
    gate_up_pieces = last_swap(gate_up_pieces)
    gate_grad, up_grad = place_gate_up(gate_up_pieces)
    down_grad, gate_grad, up_grad, *attn_pieces = lax.optimization_barrier((down_grad, gate_grad, up_grad, *attn_pieces))
    query_grad, key_grad, value_grad, out_proj_grad = place_attention(last_swap(attn_pieces))

    gain_sums = lax.dynamic_slice_in_dim(gain_sums, lax.axis_index("fsdp") * attn_gain.shape[0], attn_gain.shape[0], 1)
    return (
        output[None],
        input_grad[None],
        gain_sums[0],
        query_grad,
        key_grad,
        value_grad,
        out_proj_grad,
        gain_sums[1],
        gate_grad,
        up_grad,
        down_grad,
    )


def solution(mesh):
    weight, gain = P("fsdp", "tp"), P("fsdp")
    rows = P("fsdp", "ctx", None)
    in_specs = (rows, rows, P("fsdp", "ctx"), gain, weight, weight, weight, P("tp", "fsdp"), gain, weight, weight, P("tp", "fsdp"))
    out_specs = (rows, rows, gain, weight, weight, weight, P("tp", "fsdp"), gain, weight, weight, P("tp", "fsdp"))
    return jax.shard_map(local, mesh=mesh, in_specs=in_specs, out_specs=out_specs, check_vma=False)
```

```python
import math

import jax
import jax.numpy as jnp
from jax import lax
from jax.experimental import pallas as pl
from jax.experimental.pallas import tpu as pltpu
from jax.sharding import PartitionSpec as P


HEAD_DIM = 64
EPS = 1e-05
ROPE_BASE = 130000.0
MASKED = -1e30
PAIR = 2 * HEAD_DIM
BLOCK = 512
VMEM_LIMIT = 60 * 1024 * 1024


def low(values):
    return values.astype(jnp.bfloat16)


def wide(values):
    return values.astype(jnp.float32)


def product(a, b):
    return jnp.dot(a, b, preferred_element_type=jnp.float32)


def contract_rows(a, b):
    return lax.dot_general(a, b, (((0,), (0,)), ((), ())), preferred_element_type=jnp.float32)


def contract_cols(a, b):
    return lax.dot_general(a, b, (((1,), (1,)), ((), ())), preferred_element_type=jnp.float32)


def aligned(start, count):
    return pl.ds(pl.multiple_of(start, count), count)


def first_head():
    return lax.broadcasted_iota(jnp.int32, (1, PAIR), 1) < HEAD_DIM


def split_heads(rows):
    zero = jnp.zeros_like(rows)
    mask = first_head()
    return jnp.where(mask, rows, zero), jnp.where(mask, zero, rows)


def turn(rows, sign):
    half = HEAD_DIM // 2
    lanes = lax.broadcasted_iota(jnp.int32, (1, PAIR), 1)
    up = pltpu.roll(rows, PAIR - half, 1)
    down = pltpu.roll(rows, half, 1)
    return jnp.where(lanes % HEAD_DIM < half, -sign * up, sign * down)


def forward_kernel(info, qkv_ref, cos_ref, sin_ref, seg_col, seg_row, rot_ref, out_ref, wide_ref, lse_ref, best, total, acc):
    blocks = qkv_ref.shape[0] // BLOCK

    def prepare(n, _):
        rows = pl.ds(pl.multiple_of(n * BLOCK, BLOCK), BLOCK)
        cos, sin = cos_ref[rows, :], sin_ref[rows, :]
        q = qkv_ref[rows, :PAIR]
        k = qkv_ref[rows, PAIR : 2 * PAIR]
        rot_ref[rows, :PAIR] = low(low(q * cos + turn(q, 1.0) * sin) * jnp.bfloat16(HEAD_DIM**-0.5))
        rot_ref[rows, PAIR : 2 * PAIR] = low(k * cos + turn(k, 1.0) * sin)
        rot_ref[rows, 2 * PAIR :] = low(qkv_ref[rows, 2 * PAIR :])
        return 0

    lax.fori_loop(0, blocks, prepare, 0)

    def visit(i, j, diagonal):
        rows = pl.ds(pl.multiple_of(i * BLOCK, BLOCK), BLOCK)
        cols = pl.ds(pl.multiple_of(j * BLOCK, BLOCK), BLOCK)
        allowed = seg_col[rows, :1] == seg_row[:1, cols]
        if diagonal:
            at = lax.broadcasted_iota(jnp.int32, (BLOCK, BLOCK), 0)
            allowed = allowed & (at >= lax.broadcasted_iota(jnp.int32, (BLOCK, BLOCK), 1))
        keys = rot_ref[cols, PAIR : 2 * PAIR]
        values = rot_ref[cols, 2 * PAIR :]
        for h, q in enumerate(split_heads(rot_ref[rows, :PAIR])):
            scores = jnp.where(allowed, contract_cols(q, keys), MASKED)
            top = jnp.max(scores, axis=1, keepdims=True)
            if diagonal:
                p = jnp.exp(scores - top)
                best[h] = jnp.broadcast_to(top, (BLOCK, PAIR))
                total[h] = jnp.broadcast_to(jnp.sum(p, axis=1, keepdims=True), (BLOCK, PAIR))
                acc[h] = product(low(p), values)
            else:
                old = best[h][:, :1]
                new = jnp.maximum(old, top)
                fade = jnp.exp(old - new)
                p = jnp.exp(scores - new)
                best[h] = jnp.broadcast_to(new, (BLOCK, PAIR))
                total[h] = total[h] * fade + jnp.sum(p, axis=1, keepdims=True)
                acc[h] = acc[h] * fade + product(low(p), values)

    def one_row(i, _):
        rows = pl.ds(pl.multiple_of(i * BLOCK, BLOCK), BLOCK)
        visit(i, i, True)

        def one_col(j, _):
            @pl.when((info[0, j] < info[0, i]) & (info[2, j] >= info[1, i]))
            def _():
                visit(i, j, False)

            return 0

        lax.fori_loop(0, blocks, one_col, 0)
        mixed = jnp.where(first_head(), acc[0] / total[0], acc[1] / total[1])
        out_ref[rows, :] = low(mixed)
        wide_ref[rows, :] = mixed
        for h in range(2):
            lse_ref[0, h : h + 1, rows] = (best[h] + jnp.log(total[h])).T[:1, :]
        return 0

    lax.fori_loop(0, blocks, one_row, 0)


class Backward:
    def __init__(self, pair, rot, cos, sin, seg_col, seg_row, cot, mixed, lse, out, delta, dq, follows):
        self.pair, self.follows = pair, follows
        self.rot, self.cos, self.sin, self.seg_col, self.seg_row = rot, cos, sin, seg_col, seg_row
        self.cot, self.mixed, self.lse, self.out, self.delta, self.dq = cot, mixed, lse, out, delta, dq
        self.blocks = rot.shape[0] // BLOCK

    def part(self, n):
        return aligned((3 * self.pair + n) * PAIR, PAIR)

    def own(self):
        return aligned(self.pair * PAIR, PAIR)

    def prepare(self):
        def some(n, _):
            rows = aligned(n * BLOCK, BLOCK)
            terms = (wide(self.cot[rows, self.own()]) * self.mixed[rows, self.own()]).T
            self.delta[0:1, rows] = jnp.sum(terms[:HEAD_DIM], axis=0, keepdims=True)
            self.delta[1:2, rows] = jnp.sum(terms[HEAD_DIM:], axis=0, keepdims=True)
            self.dq[rows, :] = jnp.zeros((BLOCK, PAIR), jnp.float32)
            return 0

        lax.fori_loop(0, self.blocks, some, 0)

    def visit(self, row, rows_count, col, cols_count, diagonal, dk, dv):
        rows, cols = aligned(row, rows_count), aligned(col, cols_count)
        allowed = self.seg_col[cols, :1] == self.seg_row[:1, rows]
        if diagonal:
            at = lax.broadcasted_iota(jnp.int32, (cols_count, rows_count), 0)
            allowed = allowed & (at <= lax.broadcasted_iota(jnp.int32, (cols_count, rows_count), 1))
        queries, cots = self.rot[rows, self.part(0)], self.cot[rows, self.own()]
        query_heads, cot_heads = split_heads(queries), split_heads(cots)
        key_heads = split_heads(self.rot[cols, self.part(1)])
        value_heads = split_heads(self.rot[cols, self.part(2)])
        total = self.dq[rows, :]
        for h in range(2):
            scores = contract_cols(key_heads[h], queries)
            probs = jnp.where(allowed, jnp.exp(scores - self.lse[self.pair, h : h + 1, rows]), 0.0)
            dv = dv + product(low(probs), cot_heads[h])
            prob_cot = contract_cols(value_heads[h], cots)
            score_cot = low(probs * (prob_cot - self.delta[h : h + 1, rows]))
            dk = dk + product(score_cot, query_heads[h])
            total = total + contract_rows(score_cot, key_heads[h])
        self.dq[rows, :] = total
        return dk, dv

    def unturn(self, grad, rows):
        return low(grad * self.cos[rows, :] + turn(grad * self.sin[rows, :], -1.0))

    def column(self, j):
        start, half = j * BLOCK, BLOCK // 2
        zero = jnp.zeros((half, PAIR), jnp.float32)
        halves = [
            self.visit(start, BLOCK, start, half, True, zero, zero),
            self.visit(start + half, half, start + half, half, True, zero, zero),
        ]
        state = tuple(jnp.concatenate(pair, axis=0) for pair in zip(*halves))

        def one_row(i, state):
            return lax.cond(
                self.follows(i, j),
                lambda state: self.visit(i * BLOCK, BLOCK, start, BLOCK, False, *state),
                lambda state: state,
                state,
            )

        dk, dv = lax.fori_loop(0, self.blocks, one_row, state)
        cols = aligned(start, BLOCK)
        self.out[cols, self.part(1)] = self.unturn(dk, cols)
        self.out[cols, self.part(2)] = low(dv)

    def finish(self):
        def some(n, _):
            rows = aligned(n * BLOCK, BLOCK)
            self.out[rows, self.part(0)] = self.unturn(self.dq[rows, :] * HEAD_DIM**-0.5, rows)
            return 0

        lax.fori_loop(0, self.blocks, some, 0)


def backward_kernel(info, *refs):
    def follows(i, j):
        return (info[0, j] < info[0, i]) & (info[2, j] >= info[1, i])

    back = Backward(0, *refs, follows)
    back.prepare()

    def one_col(j, _):
        back.column(j)
        return 0

    lax.fori_loop(0, back.blocks, one_col, 0)
    back.finish()


def attention_forward(info, qkv, cos, sin, seg_col, seg_row):
    tokens, width = qkv.shape
    pairs = width // (3 * PAIR)
    whole = lambda p, info: (0, 0)
    return pl.pallas_call(
        forward_kernel,
        grid_spec=pltpu.PrefetchScalarGridSpec(
            num_scalar_prefetch=1,
            grid=(pairs,),
            in_specs=[
                pl.BlockSpec((tokens, 3 * PAIR), lambda p, info: (0, p)),
                pl.BlockSpec((tokens, PAIR), whole),
                pl.BlockSpec((tokens, PAIR), whole),
                pl.BlockSpec((tokens, 1), whole),
                pl.BlockSpec((1, tokens), whole),
            ],
            out_specs=[
                pl.BlockSpec((tokens, 3 * PAIR), lambda p, info: (0, p)),
                pl.BlockSpec((tokens, PAIR), lambda p, info: (0, p)),
                pl.BlockSpec((tokens, PAIR), lambda p, info: (0, p)),
                pl.BlockSpec((1, 2, tokens), lambda p, info: (p, 0, 0)),
            ],
            scratch_shapes=[
                pltpu.VMEM((2, BLOCK, PAIR), jnp.float32),
                pltpu.VMEM((2, BLOCK, PAIR), jnp.float32),
                pltpu.VMEM((2, BLOCK, PAIR), jnp.float32),
            ],
        ),
        out_shape=[
            jax.ShapeDtypeStruct((tokens, width), jnp.bfloat16),
            jax.ShapeDtypeStruct((tokens, pairs * PAIR), jnp.bfloat16),
            jax.ShapeDtypeStruct((tokens, pairs * PAIR), jnp.float32),
            jax.ShapeDtypeStruct((pairs, 2, tokens), jnp.float32),
        ],
        compiler_params=pltpu.CompilerParams(vmem_limit_bytes=VMEM_LIMIT),
        cost_estimate=pl.CostEstimate(flops=tokens * tokens * width, bytes_accessed=10 * tokens * width, transcendentals=tokens * tokens * 2 * pairs),
    )(info, qkv, cos, sin, seg_col, seg_row)


def attention_backward(info, rot, cos, sin, seg_col, seg_row, cot, mixed, lse):
    tokens, width = rot.shape
    pairs = width // (3 * PAIR)
    whole = lambda p, info: (0, 0)
    return pl.pallas_call(
        backward_kernel,
        grid_spec=pltpu.PrefetchScalarGridSpec(
            num_scalar_prefetch=1,
            grid=(pairs,),
            in_specs=[
                pl.BlockSpec((tokens, 3 * PAIR), lambda p, info: (0, p)),
                pl.BlockSpec((tokens, PAIR), whole),
                pl.BlockSpec((tokens, PAIR), whole),
                pl.BlockSpec((tokens, 1), whole),
                pl.BlockSpec((1, tokens), whole),
                pl.BlockSpec((tokens, PAIR), lambda p, info: (0, p)),
                pl.BlockSpec((tokens, PAIR), lambda p, info: (0, p)),
                pl.BlockSpec((1, 2, tokens), lambda p, info: (p, 0, 0)),
            ],
            out_specs=pl.BlockSpec((tokens, 3 * PAIR), lambda p, info: (0, p)),
            scratch_shapes=[
                pltpu.VMEM((2, tokens), jnp.float32),
                pltpu.VMEM((tokens, PAIR), jnp.float32),
            ],
        ),
        out_shape=jax.ShapeDtypeStruct((tokens, width), jnp.bfloat16),
        compiler_params=pltpu.CompilerParams(vmem_limit_bytes=VMEM_LIMIT),
        cost_estimate=pl.CostEstimate(flops=3 * tokens * tokens * width, bytes_accessed=10 * tokens * width, transcendentals=tokens * tokens * 2 * pairs),
    )(info, rot, cos, sin, seg_col, seg_row, cot, mixed, lse)


def swap(values, axis, mask):
    size = lax.axis_size(axis)
    return lax.ppermute(values, axis, [(i, i ^ mask) for i in range(size)])


def masks(size):
    return [1 << n for n in reversed(range(size.bit_length() - 1))]


def offsets(size):
    held = [0]
    for mask in masks(size):
        held = held + [at ^ mask for at in held]
    return held


def gather_rows(rows, axis):
    for mask in masks(lax.axis_size(axis)):
        rows = jnp.concatenate([rows, swap(rows, axis, mask)], axis=0)
    return rows


def scatter_rows(make, count, axis):
    todo = list(reversed(masks(lax.axis_size(axis))))
    half = count // 2
    there = swap(low(make(half, count)), axis, todo[0])
    rows = make(0, half) + wide(there)
    for mask in todo[1:]:
        half = rows.shape[0] // 2
        rows = rows[:half] + wide(swap(low(rows[half:]), axis, mask))
    return rows


def scatter_both(make, count):
    rows = scatter_rows(make, count, "ctx")
    size = lax.axis_size("tp")
    me = lax.axis_index("tp")
    for mask in masks(size):
        half = rows.shape[0] // 2
        upper = (me & mask) != 0
        mine = jnp.where(upper, rows[half:], rows[:half])
        other = jnp.where(upper, rows[:half], rows[half:])
        rows = mine + wide(swap(low(other), "tp", mask))
    return rows


def join_tp(rows):
    size = lax.axis_size("tp")
    me = lax.axis_index("tp")
    for mask in reversed(masks(size)):
        upper = (me & mask) != 0
        other = swap(rows, "tp", mask)
        rows = jnp.where(upper, jnp.concatenate([other, rows], 0), jnp.concatenate([rows, other], 0))
    return rows


def own_part(rows):
    size = lax.axis_size("tp")
    count = rows.shape[0] // size
    return lax.dynamic_slice_in_dim(rows, lax.axis_index("tp") * count, count, 0)


MESH = pl.DeviceIdType.MESH
TILE = 512
STEP = 32


def fits_kernels():
    return lax.axis_size("ctx") == 4 and lax.axis_size("tp") == 2


class Place:
    def __init__(self):
        me = lax.axis_index("ctx")
        x, core = me // 2, me % 2
        self.tp = lax.axis_index("tp")
        self.x = {"ctx": (1 - x) * 2 + core}
        self.core = {"ctx": x * 2 + 1 - core}
        self.cross = {"ctx": (1 - x) * 2 + 1 - core}
        self.y = {"tp": 1 - self.tp}

    def plane(self):
        tp = self.y["tp"]
        return [self.x, self.core, self.cross, self.y] + [dict(device, tp=tp) for device in (self.x, self.core, self.cross)]

    def others(self, axis):
        size, me = lax.axis_size(axis), lax.axis_index(axis)
        return [{axis: (me + n) % size} for n in range(1, size)]


def meet(devices):
    barrier = pltpu.get_barrier_semaphore()
    for device in devices:
        pl.semaphore_signal(barrier, inc=1, device_id=device, device_id_type=MESH)
    pl.semaphore_wait(barrier, len(devices))


class Links:
    def __init__(self, send, recv):
        self.send, self.recv, self.count, self.sent = send, recv, 0, []

    def copy(self, src, dst, device, at=None):
        n = self.count
        self.count += 1
        made = pltpu.make_async_remote_copy(src, dst, self.send.at[n], self.recv.at[n], device_id=device, device_id_type=MESH)
        self.sent.append(made)
        return made

    def drain(self):
        for made in self.sent:
            made.wait_send()


def start_kernel(hidden, grads, segs, gains, attn_in, cot, segs_out, gains_out, hbuf, nbuf, gbuf, gain_row, send, recv, local_sem):
    place, links = Place(), Links(send, recv)
    rows = hidden.shape[0]
    half, quarter = rows // 2, rows // 4
    z = lax.axis_index("fsdp")
    near = [place.x, place.core, place.cross, place.y]
    far = place.others("fsdp")
    meet(near + far)

    def span(block, part, chunk=None):
        if chunk is None:
            return aligned(block * rows + part * half, half)
        return aligned(block * rows + part * half + chunk * quarter, quarter)

    mine, other = place.tp, 1 - place.tp
    tiny = [links.copy(gains, gains_out.at[z], device) for device in far]
    tiny_segs = [links.copy(segs, segs_out.at[n + 1], device) for n, device in enumerate(near[:3])]
    for made in tiny + tiny_segs:
        made.start()
    over_x = {}
    for name, src, dst in (("h", hidden, hbuf), ("g", grads, gbuf)):
        for q in range(2):
            over_x[name, q] = links.copy(src.at[span(0, mine, q)], dst.at[span(1, mine, q)], place.x)
    over_core = {name: links.copy(src, dst.at[aligned(2 * rows, rows)], place.core) for name, src, dst in (("h", hidden, hbuf), ("g", grads, gbuf))}
    for key in (("h", 0), ("h", 1)):
        over_x[key].start()
    over_core["h"].start()
    for key in (("g", 0), ("g", 1)):
        over_x[key].start()
    over_core["g"].start()
    kept = []

    def keep(src, dst):
        made = pltpu.make_async_copy(src, dst, local_sem.at[len(kept)])
        made.start()
        kept.append(made)

    keep(grads, cot.at[aligned(0, rows)])
    gains_out[z] = gains[...]
    segs_out[0] = segs[...]
    for made in tiny:
        made.wait_recv()
    lanes = 128
    groups = gains.shape[0] // 2
    for device in range(gains_out.shape[0]):
        for row in range(groups):
            gain_row[:, pl.ds((device * groups + row) * lanes, lanes)] = gains_out[device, row : row + 1, :]

    def normalize(src, at, block, count):
        def some(n, _):
            there = aligned(at + n * 64, 64)
            values = wide(src[there, :])
            scale = lax.rsqrt(jnp.mean(values * values, axis=1, keepdims=True) + EPS)
            nbuf[aligned(block + n * 64, 64), :] = low(values * scale * gain_row[...])
            return 0

        lax.fori_loop(0, count // 64, some, 0)
        keep(nbuf.at[pl.ds(block, count)], attn_in.at[pl.ds(block, count)])

    normalize(hidden, 0, 0, rows)
    over_y, across, last = {}, {}, {}

    def pass_on(name, buf):
        for q in range(2):
            over_x[name, q].wait_recv()
            over_y[name, q] = links.copy(buf.at[span(1, mine, q)], buf.at[span(1, mine, q)], place.y)
            across[name, q] = links.copy(buf.at[span(1, mine, q)], buf.at[span(3, mine, q)], place.core)
            over_y[name, q].start()
            across[name, q].start()

    def finish(name, buf):
        for q in range(2):
            over_y[name, q].wait_recv()
            last[name, q] = links.copy(buf.at[span(1, other, q)], buf.at[span(3, other, q)], place.core)
            last[name, q].start()

    pass_on("h", hbuf)
    over_core["h"].wait_recv()
    normalize(hbuf, 2 * rows, 2 * rows, rows)
    finish("h", hbuf)
    normalize(hbuf, rows, rows, rows)
    pass_on("g", gbuf)
    for q in range(2):
        across["h", q].wait_recv()
        last["h", q].wait_recv()
    normalize(hbuf, 3 * rows, 3 * rows, rows)
    over_core["g"].wait_recv()
    keep(gbuf.at[aligned(2 * rows, rows)], cot.at[aligned(2 * rows, rows)])
    finish("g", gbuf)
    keep(gbuf.at[aligned(rows, rows)], cot.at[aligned(rows, rows)])
    for q in range(2):
        across["g", q].wait_recv()
        last["g", q].wait_recv()
    keep(gbuf.at[aligned(3 * rows, rows)], cot.at[aligned(3 * rows, rows)])
    for made in tiny_segs:
        made.wait_recv()
    links.drain()
    for made in kept:
        made.wait()


def start_exchange(hidden, grads, segments, attn_gain, mlp_gain):
    rows, width = hidden.shape
    fsdp = lax.axis_size("fsdp")
    segs = jnp.concatenate([segments.reshape(-1, 128), jnp.zeros((8 - rows // 128, 128), jnp.int32)], axis=0)
    gains = wide(jnp.concatenate([attn_gain, mlp_gain])).reshape(-1, 128)
    vmem = pl.BlockSpec(memory_space=pltpu.VMEM)
    hbm = pl.BlockSpec(memory_space=pl.ANY)
    tokens = 4 * rows
    attn_in, cot, segs, gains = pl.pallas_call(
        start_kernel,
        in_specs=[vmem] * 4,
        out_specs=[hbm, hbm, vmem, vmem],
        out_shape=[
            jax.ShapeDtypeStruct((tokens, width), jnp.bfloat16),
            jax.ShapeDtypeStruct((tokens, width), jnp.bfloat16),
            jax.ShapeDtypeStruct((4, 8, 128), jnp.int32),
            jax.ShapeDtypeStruct((fsdp,) + gains.shape, jnp.float32),
        ],
        scratch_shapes=[
            pltpu.VMEM((tokens, width), jnp.bfloat16),
            pltpu.VMEM((tokens, width), jnp.bfloat16),
            pltpu.VMEM((tokens, width), jnp.bfloat16),
            pltpu.VMEM((1, width), jnp.float32),
            pltpu.SemaphoreType.DMA((fsdp + 32,)),
            pltpu.SemaphoreType.DMA((fsdp + 32,)),
            pltpu.SemaphoreType.DMA((8,)),
        ],
        compiler_params=pltpu.CompilerParams(collective_id=0, has_side_effects=True, vmem_limit_bytes=VMEM_LIMIT),
        cost_estimate=pl.CostEstimate(flops=0, bytes_accessed=200_000_000, transcendentals=0),
    )(hidden, grads, segs, gains)
    segs = segs[:, : rows // 128].reshape(tokens)
    gains = jnp.transpose(gains.reshape(fsdp, 2, -1), (1, 0, 2)).reshape(2, width)
    return attn_in, cot, segs, gains


def scatter_scratch(rows, width):
    part, half = rows // 8, width // 2
    return [
        pltpu.VMEM((4, part, width), jnp.bfloat16),
        pltpu.VMEM((4, part, width), jnp.bfloat16),
        pltpu.VMEM((6, part, half), jnp.bfloat16),
        pltpu.VMEM((6, part, half), jnp.bfloat16),
        pltpu.VMEM((2, part, half), jnp.float32),
        pltpu.VMEM((part, width), jnp.float32),
        pltpu.SemaphoreType.DMA((14,)),
        pltpu.SemaphoreType.DMA((14,)),
    ]


class Scatter:
    def __init__(self, place, make, count, refs, first=("x", "y")):
        self.place, self.make = place, make
        self.hi, self.core_in, self.out, self.come, self.wait, self.total, send, recv = refs
        self.part = count // 8
        self.half = self.total.shape[1] // 2
        self.links = Links(send, recv)
        self.core = {}
        for side in range(2):
            cols = pl.ds(side * self.half, self.half)
            for n in range(4):
                self.core[n, side] = self.links.copy(self.hi.at[n, :, cols], self.core_in.at[n, :, cols], place.core)
        self.send, self.away, self.stays = [], {}, {}
        for side, link in enumerate(first):
            to, then = (place.x, place.y) if link == "x" else (place.y, place.x)
            for n, device in enumerate((to, to, then)):
                at = 3 * side + n
                self.send.append(self.links.copy(self.out.at[at], self.come.at[at], device))
            second, stay = (1, 2) if link == "x" else (2, 1)
            self.away[0, side], self.away[second, side] = 3 * side, 3 * side + 1
            self.stays[side] = stay

    def rows(self, n):
        tp = self.place.tp
        part = (1 - tp) + (n % 2) * (2 * tp - 1)
        return ((1 - n // 2) * 2 + part) * self.part

    def columns(self, side, each):
        tiles = self.half // TILE

        def one(n, _):
            each(aligned(side * self.half + n * TILE, TILE), aligned(n * TILE, TILE))
            return 0

        lax.fori_loop(0, tiles, one, 0)

    def to_core(self, n, side):
        rows = aligned(4 * self.part + self.rows(n), self.part)

        def each(cols, _):
            self.hi[n, :, cols] = low(self.make(rows, cols))

        self.columns(side, each)
        self.core[n, side].start()

    def to_links(self, n, side):
        rows = aligned(self.rows(n), self.part)
        self.core[n, side].wait_recv()

        def each(cols, at):
            value = self.make(rows, cols) + wide(self.core_in[n, :, cols])
            if (n, side) in self.away:
                self.out[self.away[n, side], :, at] = low(value)
            elif n == 3:
                self.total[:, cols] = value
            else:
                self.wait[side, :, at] = value

        self.columns(side, each)
        if (n, side) in self.away:
            self.send[self.away[n, side]].start()

    def units(self):
        return (
            [(0, side) for side in range(2)]
            + [(n, side) for n in (1, 2) for side in range(2) if (n, side) in self.away]
            + [(self.stays[side], side) for side in range(2)]
            + [(3, side) for side in range(2)]
        )

    def start(self, waits=()):
        units = self.units()
        ahead = 2
        waits = list(waits) + [()] * 3
        for at, unit in enumerate(units[:ahead]):
            for made in waits[at]:
                made.wait()
            self.to_core(*unit)
        for made in waits[2]:
            made.wait()
        for at, unit in enumerate(units):
            self.to_links(*unit)
            if at + ahead < len(units):
                self.to_core(*units[at + ahead])

    def turn(self):
        for side in range(2):
            came, goes = 3 * side, 3 * side + 2
            self.send[came].wait_recv()

            def each(_, at):
                self.out[goes, :, at] = low(self.wait[side, :, at] + wide(self.come[came, :, at]))

            self.columns(side, each)
            self.send[goes].start()

    def finish(self):
        for side in range(2):
            for n in (1, 2):
                self.send[3 * side + n].wait_recv()
            cols = pl.ds(side * self.half, self.half)
            self.total[:, cols] = self.total[:, cols] + wide(self.come[3 * side + 1]) + wide(self.come[3 * side + 2])
        self.links.drain()


def gather_plane(place, links, mine, full, part):
    half = mine.shape[1] // 2
    left, right = pl.ds(0, half), pl.ds(half, half)
    own, other = place.tp, 1 - place.tp

    def rows(block, tp):
        return aligned((block * 2 + tp) * part, part)

    y_left = links.copy(mine.at[:, left], full.at[rows(0, own), left], place.y)
    x_right = links.copy(mine.at[:, right], full.at[rows(1, own), right], place.x)
    y_right = links.copy(mine.at[:, right], full.at[rows(0, own), right], place.y)
    x_left = links.copy(mine.at[:, left], full.at[rows(1, own), left], place.x)
    core = [links.copy(mine, full.at[rows(2, own)], place.core)]
    for made in (y_left, x_right, y_right, x_left, core[0]):
        made.start()

    def relay(come, block, tp, cols, onward=None):
        come.wait_recv()
        here = full.at[rows(block, tp), cols]
        if onward == "x":
            made = links.copy(here, full.at[rows(1, tp), cols], place.x)
        elif onward == "y":
            made = links.copy(here, full.at[rows(block, tp), cols], place.y)
        if onward:
            made.start()
        over = links.copy(here, full.at[rows(block + 2, tp), cols], place.core)
        over.start()
        core.append(over)
        return made if onward else None

    far_left = relay(y_left, 0, other, left, "x")
    far_right = relay(x_right, 1, own, right, "y")
    relay(y_right, 0, other, right)
    relay(x_left, 1, own, left)
    relay(far_left, 1, other, left)
    relay(far_right, 1, other, right)
    for made in core:
        made.wait_recv()


def load(sems, pairs):
    made = [pltpu.make_async_copy(src, dst, sems.at[n]) for n, (src, dst) in enumerate(pairs)]
    for copy in made:
        copy.start()
    return made


def forward_mid_kernel(mixed, weight, hidden, gain, full, resid_out, mine, *refs):
    place = Place()
    scatter_refs, (send, recv, local_sem) = refs[:-3], refs[-3:]
    count = mixed.shape[0]
    part = count // 8
    meet([place.x, place.core, place.y])
    scatter = Scatter(place, lambda rows, cols: contract_cols(mixed[rows, :], weight[cols, weight.shape[1] - mixed.shape[1] :]), count, scatter_refs)
    scatter.start()
    scatter.turn()
    scatter.finish()
    step = STEP

    def some(n, _):
        rows = aligned(n * step, step)
        values = wide(hidden[aligned(place.tp * part + n * step, step), :]) + scatter.total[rows, :]
        resid_out[rows, :] = values
        scale = lax.rsqrt(jnp.mean(values * values, axis=1, keepdims=True) + EPS)
        mine[rows, :] = low(values * scale * gain[...])
        return 0

    lax.fori_loop(0, part // step, some, 0)
    stay = pltpu.make_async_copy(mine, full.at[aligned(place.tp * part, part)], local_sem)
    stay.start()
    links = Links(send, recv)
    gather_plane(place, links, mine, full, part)
    links.drain()
    stay.wait()


def mid_scratch(count, width):
    return [pltpu.VMEM((count // 8, width), jnp.bfloat16)] + scatter_scratch(count, width) + [
        pltpu.SemaphoreType.DMA((16,)),
        pltpu.SemaphoreType.DMA((16,)),
        pltpu.SemaphoreType.DMA,
    ]


def forward_mid(mixed, weight, hidden, gain):
    count, width = mixed.shape[0], weight.shape[0]
    vmem = pl.BlockSpec(memory_space=pltpu.VMEM)
    return pl.pallas_call(
        forward_mid_kernel,
        in_specs=[vmem] * 4,
        out_specs=[pl.BlockSpec(memory_space=pl.ANY), vmem],
        out_shape=[jax.ShapeDtypeStruct((count, width), jnp.bfloat16), jax.ShapeDtypeStruct((count // 8, width), jnp.float32)],
        scratch_shapes=mid_scratch(count, width),
        compiler_params=pltpu.CompilerParams(collective_id=1, has_side_effects=True, vmem_limit_bytes=VMEM_LIMIT),
        cost_estimate=pl.CostEstimate(flops=0, bytes_accessed=300_000_000, transcendentals=0),
    )(mixed, weight, hidden, gain[None, :])


def norm_back(values, scale, gain, cot):
    scaled = cot * gain
    lean = jnp.mean(values * scaled, axis=1, keepdims=True)
    return scale * scaled - values * (scale * scale * scale) * lean, cot * (values * scale)


def backward_mid_kernel(
    hidden_hbm, weights_hbm, resid_hbm, grads_hbm, gain, full, cot_out, gain_out,
    hidden_cot, weights, resid, grads, sems, mine, *refs
):
    place = Place()
    scatter_refs, (send, recv, local_sem) = refs[:-3], refs[-3:]
    count = hidden_cot.shape[0]
    part = count // 8
    width = weights.shape[0]
    lower, upper = pl.ds(0, count // 2), pl.ds(count // 2, count // 2)
    left, right = pl.ds(0, width // 2), pl.ds(width // 2, width // 2)
    loads = load(
        sems,
        [
            (weights_hbm.at[left], weights.at[left]),
            (hidden_hbm.at[upper], hidden_cot.at[upper]),
            (weights_hbm.at[right], weights.at[right]),
            (hidden_hbm.at[lower], hidden_cot.at[lower]),
            (resid_hbm, resid),
            (grads_hbm.at[aligned(place.tp * part, part)], grads),
        ],
    )
    meet([place.x, place.core, place.y])

    def make(rows, cols):
        return contract_cols(hidden_cot[rows, :], weights[cols, :])

    scatter = Scatter(place, make, count, scatter_refs)
    scatter.start((loads[:2], loads[2:3], loads[3:4]))
    scatter.turn()
    scatter.finish()
    for made in loads[4:]:
        made.wait()
    step = STEP

    def some(n, sums):
        rows = aligned(n * step, step)
        values = resid[rows, :]
        scale = lax.rsqrt(jnp.mean(values * values, axis=1, keepdims=True) + EPS)
        back, terms = norm_back(values, scale, gain[...], scatter.total[rows, :])
        cot = wide(grads[rows, :]) + back
        cot_out[rows, :] = cot
        mine[rows, :] = low(cot)
        return sums + jnp.sum(terms, axis=0, keepdims=True)

    gain_out[...] = lax.fori_loop(0, part // step, some, jnp.zeros(gain.shape, jnp.float32))
    stay = pltpu.make_async_copy(mine, full.at[aligned(place.tp * part, part)], local_sem)
    stay.start()
    links = Links(send, recv)
    gather_plane(place, links, mine, full, part)
    links.drain()
    stay.wait()


def backward_mid(hidden_cot, weights, resid, grads, gain):
    count, width = hidden_cot.shape[0], weights.shape[0]
    vmem = pl.BlockSpec(memory_space=pltpu.VMEM)
    hbm = pl.BlockSpec(memory_space=pl.ANY)
    return pl.pallas_call(
        backward_mid_kernel,
        in_specs=[hbm] * 4 + [vmem],
        out_specs=[pl.BlockSpec(memory_space=pl.ANY), vmem, vmem],
        out_shape=[
            jax.ShapeDtypeStruct((count, width), jnp.bfloat16),
            jax.ShapeDtypeStruct((count // 8, width), jnp.float32),
            jax.ShapeDtypeStruct((1, width), jnp.float32),
        ],
        scratch_shapes=[
            pltpu.VMEM(hidden_cot.shape, jnp.bfloat16),
            pltpu.VMEM(weights.shape, jnp.bfloat16),
            pltpu.VMEM(resid.shape, jnp.float32),
            pltpu.VMEM(resid.shape, jnp.bfloat16),
            pltpu.SemaphoreType.DMA((6,)),
        ]
        + mid_scratch(count, width),
        compiler_params=pltpu.CompilerParams(collective_id=2, has_side_effects=True, vmem_limit_bytes=VMEM_LIMIT),
        cost_estimate=pl.CostEstimate(flops=0, bytes_accessed=300_000_000, transcendentals=0),
    )(hidden_cot, weights, resid, grads, gain[None, :])


def input_kernel(cots, weights, cot_hbm, hidden_hbm, gain, grad_out, gain_out, resid_cot, hidden, sems, *refs):
    place = Place()
    count = cots.shape[0]
    part = count // 8
    loads = load(sems, [(cot_hbm, resid_cot), (hidden_hbm.at[aligned(place.tp * part, part)], hidden)])
    meet([place.x, place.core, place.y])
    scatter = Scatter(place, lambda rows, cols: contract_cols(cots[rows, :], weights[cols, : cots.shape[1]]), count, refs, ("y", "y"))
    scatter.start()
    scatter.turn()
    scatter.finish()
    for made in loads:
        made.wait()
    step = STEP

    def some(n, total):
        rows = aligned(n * step, step)
        values = wide(hidden[rows, :])
        scale = lax.rsqrt(jnp.mean(values * values, axis=1, keepdims=True) + EPS)
        back, terms = norm_back(values, scale, gain[...], scatter.total[rows, :])
        grad_out[rows, :] = low(resid_cot[rows, :] + back)
        return total + jnp.sum(terms, axis=0, keepdims=True)

    gain_out[...] = lax.fori_loop(0, part // step, some, jnp.zeros(gain.shape, jnp.float32))


def gain_kernel(gain_one, gain_two, gains_out, sums, come, send, recv):
    place, links = Place(), Links(send, recv)
    stages = place.plane(), place.others("fsdp")
    meet(stages[0] + stages[1])
    sums[0, 0:1, :] = gain_one[...]
    sums[0, 1:2, :] = gain_two[...]
    total = sums[0]
    for stage, devices in enumerate(stages):
        at = stage * len(stages[0])
        made = [links.copy(sums.at[stage], come.at[at + n], device) for n, device in enumerate(devices)]
        for copy in made:
            copy.start()
        for n, copy in enumerate(made):
            copy.wait_recv()
            total = total + come[at + n]
        if stage == 0:
            sums[1] = total
    gains_out[...] = total
    links.drain()


def gain_sum(gain_one, gain_two):
    width = gain_one.shape[1]
    copies = 6 + lax.axis_size("fsdp")
    vmem = pl.BlockSpec(memory_space=pltpu.VMEM)
    return pl.pallas_call(
        gain_kernel,
        in_specs=[vmem] * 2,
        out_specs=vmem,
        out_shape=jax.ShapeDtypeStruct((2, width), jnp.float32),
        scratch_shapes=[
            pltpu.VMEM((2, 2, width), jnp.float32),
            pltpu.VMEM((copies, 2, width), jnp.float32),
            pltpu.SemaphoreType.DMA((copies,)),
            pltpu.SemaphoreType.DMA((copies,)),
        ],
        compiler_params=pltpu.CompilerParams(collective_id=5, has_side_effects=True, vmem_limit_bytes=VMEM_LIMIT),
        cost_estimate=pl.CostEstimate(flops=0, bytes_accessed=20_000_000, transcendentals=0),
    )(gain_one, gain_two)


def input_exchange(cots, weights, resid_cot, hidden, gain):
    count, width = cots.shape[0], weights.shape[0]
    vmem = pl.BlockSpec(memory_space=pltpu.VMEM)
    return pl.pallas_call(
        input_kernel,
        in_specs=[vmem] * 2 + [pl.BlockSpec(memory_space=pl.ANY)] * 2 + [vmem],
        out_specs=[vmem, vmem],
        out_shape=[jax.ShapeDtypeStruct((count // 8, width), jnp.bfloat16), jax.ShapeDtypeStruct((1, width), jnp.float32)],
        scratch_shapes=[
            pltpu.VMEM(resid_cot.shape, jnp.float32),
            pltpu.VMEM(resid_cot.shape, jnp.bfloat16),
            pltpu.SemaphoreType.DMA((2,)),
        ]
        + scatter_scratch(count, width),
        compiler_params=pltpu.CompilerParams(collective_id=3, has_side_effects=True, vmem_limit_bytes=VMEM_LIMIT),
        cost_estimate=pl.CostEstimate(flops=0, bytes_accessed=180_000_000, transcendentals=0),
    )(cots, weights, resid_cot, hidden, gain[None, :])


def attention_output_kernel(
    rot_hbm, cos_hbm, sin_hbm, seg_col, seg_row, cot_hbm, mixed_hbm, lse, hidden_act, down, resid_hbm, cots, out,
    rot, cos, sin, cot, mixed, resid, sems, delta, dq, *refs
):
    place = Place()
    count = hidden_act.shape[0]
    me = lax.axis_index("ctx")
    blocks = count // BLOCK
    per = count // 4 // BLOCK

    def at(block):
        n = block // per
        return (((me // 2 + n % 2) % 2) * 2 + (me % 2 + n // 2) % 2) * per + block % per

    def follows(i, j):
        return (at(j) < at(i)) & (at(i) - at(j) <= blocks // 2)

    loads = load(
        sems, [(rot_hbm, rot), (cos_hbm, cos), (sin_hbm, sin), (cot_hbm, cot), (mixed_hbm, mixed), (resid_hbm, resid)]
    )
    meet([place.x, place.core, place.y])
    scatter = Scatter(place, lambda rows, cols: product(hidden_act[rows, :], down[:, cols]), count, refs, ("y", "y"))
    scatter.start()
    for made in loads:
        made.wait()
    pairs = rot.shape[1] // (3 * PAIR)
    steps = pairs * blocks

    def step(n, _):
        back = Backward(n // blocks, rot, cos, sin, seg_col, seg_row, cot, mixed, lse, cots, delta, dq, follows)

        @pl.when(n % blocks == 0)
        def _():
            back.prepare()

        back.column(n % blocks)

        @pl.when(n % blocks == blocks - 1)
        def _():
            back.finish()

        @pl.when(n == steps // 4 - 1)
        def _():
            scatter.turn()

        return 0

    lax.fori_loop(0, steps, step, 0)
    scatter.finish()
    out[...] = low(resid[...] + scatter.total[...])


def attention_output(rot, cos, sin, seg_col, seg_row, cot, mixed, lse, hidden_act, down, resid):
    count, width = hidden_act.shape[0], down.shape[1]
    vmem = pl.BlockSpec(memory_space=pltpu.VMEM)
    hbm = pl.BlockSpec(memory_space=pl.ANY)
    return pl.pallas_call(
        attention_output_kernel,
        in_specs=[hbm] * 3 + [vmem] * 2 + [hbm] * 2 + [vmem] * 3 + [hbm],
        out_specs=[vmem, vmem],
        out_shape=[
            jax.ShapeDtypeStruct(rot.shape, jnp.bfloat16),
            jax.ShapeDtypeStruct((count // 8, width), jnp.bfloat16),
        ],
        scratch_shapes=[pltpu.VMEM(array.shape, array.dtype) for array in (rot, cos, sin, cot, mixed, resid)]
        + [
            pltpu.SemaphoreType.DMA((6,)),
            pltpu.VMEM((2, count), jnp.float32),
            pltpu.VMEM((count, PAIR), jnp.float32),
        ]
        + scatter_scratch(count, width),
        compiler_params=pltpu.CompilerParams(collective_id=4, has_side_effects=True, vmem_limit_bytes=VMEM_LIMIT),
        cost_estimate=pl.CostEstimate(flops=0, bytes_accessed=220_000_000, transcendentals=0),
    )(rot, cos, sin, seg_col, seg_row, cot, mixed, lse, hidden_act, down, resid)


def hidden_cot_kernel(cot, down, gate_slope, up_slope, out):
    cols = down.shape[0]

    def some(n, _):
        at = aligned(n * TILE, TILE)
        back = contract_cols(cot[...], down[at, :])
        out[:, at] = low(back * gate_slope[:, at])
        out[:, aligned(cols + n * TILE, TILE)] = low(back * up_slope[:, at])
        return 0

    lax.fori_loop(0, cols // TILE, some, 0)


def hidden_cots(cot, down, gate_slope, up_slope):
    count, width = cot.shape
    cols = down.shape[0]
    rows = 512
    side = pl.BlockSpec((rows, cols), lambda n: (n, 0))
    return pl.pallas_call(
        hidden_cot_kernel,
        grid=(count // rows,),
        in_specs=[pl.BlockSpec((rows, width), lambda n: (n, 0)), pl.BlockSpec((cols, width), lambda n: (0, 0)), side, side],
        out_specs=pl.BlockSpec((rows, 2 * cols), lambda n: (n, 0)),
        out_shape=jax.ShapeDtypeStruct((count, 2 * cols), jnp.bfloat16),
        compiler_params=pltpu.CompilerParams(vmem_limit_bytes=VMEM_LIMIT),
        cost_estimate=pl.CostEstimate(flops=2 * count * width * cols, bytes_accessed=2 * count * (width + 4 * cols), transcendentals=0),
    )(cot, down, gate_slope, up_slope)


def take_attention_kernel(at, query, key, value, out, taken):
    pairs = query.shape[1] // PAIR
    for p in range(pairs):
        for n, part in enumerate((query, key, value)):
            taken[:, (3 * p + n) * PAIR : (3 * p + n + 1) * PAIR] = part[:, p * PAIR : (p + 1) * PAIR]
    taken[:, 3 * pairs * PAIR :] = out[...].T


def take_attention(me, query, key, value, out, count):
    depth = query.shape[0]
    block = pl.BlockSpec((depth, count), lambda n, at: (0, at[0]))
    return pl.pallas_call(
        take_attention_kernel,
        grid_spec=pltpu.PrefetchScalarGridSpec(
            num_scalar_prefetch=1,
            grid=(1,),
            in_specs=[block] * 3 + [pl.BlockSpec((count, depth), lambda n, at: (at[0], 0))],
            out_specs=pl.BlockSpec((depth, 4 * count), lambda n, at: (0, 0)),
        ),
        out_shape=jax.ShapeDtypeStruct((depth, 4 * count), query.dtype),
        compiler_params=pltpu.CompilerParams(vmem_limit_bytes=VMEM_LIMIT),
    )(me, query, key, value, out)


def take_hidden_kernel(at, gate, up, down, both, rows):
    count = gate.shape[1]
    both[:, :count] = gate[...]
    both[:, count:] = up[...]
    rows[...] = down[...]


def take_hidden(me, gate, up, down, count):
    depth = gate.shape[0]
    block = pl.BlockSpec((depth, count), lambda n, at: (0, at[0]))
    return pl.pallas_call(
        take_hidden_kernel,
        grid_spec=pltpu.PrefetchScalarGridSpec(
            num_scalar_prefetch=1,
            grid=(1,),
            in_specs=[block] * 2 + [pl.BlockSpec((count, depth), lambda n, at: (at[0], 0))],
            out_specs=[pl.BlockSpec((depth, 2 * count), lambda n, at: (0, 0)), pl.BlockSpec((count, depth), lambda n, at: (0, 0))],
        ),
        out_shape=[jax.ShapeDtypeStruct((depth, 2 * count), gate.dtype), jax.ShapeDtypeStruct((count, depth), down.dtype)],
        compiler_params=pltpu.CompilerParams(vmem_limit_bytes=VMEM_LIMIT),
    )(me, gate, up, down)


def first_swaps(block):
    pieces = [block]
    for mask in masks(lax.axis_size("ctx"))[:-1]:
        pieces = pieces + [swap(piece, "ctx", mask) for piece in pieces]
    return pieces


def last_swap(pieces):
    return pieces + [swap(piece, "ctx", 1) for piece in pieces]


def order_of_pieces():
    return lax.axis_index("ctx") ^ jnp.array(offsets(lax.axis_size("ctx")), jnp.int32)


def place_kernel(at, *refs):
    out = refs[-1]
    for n, piece in enumerate(refs[:-1]):

        @pl.when(pl.program_id(0) == n)
        def _():
            out[...] = wide(piece[...])


def place_pieces(pieces, axis):
    block = pieces[0].shape
    shape = list(block)
    shape[axis] *= len(pieces)
    return pl.pallas_call(
        place_kernel,
        grid_spec=pltpu.PrefetchScalarGridSpec(
            num_scalar_prefetch=1,
            grid=(len(pieces),),
            in_specs=[pl.BlockSpec(block, lambda n, at: (0, 0))] * len(pieces),
            out_specs=pl.BlockSpec(block, lambda n, at: (at[n], 0) if axis == 0 else (0, at[n])),
        ),
        out_shape=jax.ShapeDtypeStruct(shape, jnp.float32),
        compiler_params=pltpu.CompilerParams(vmem_limit_bytes=VMEM_LIMIT),
        cost_estimate=pl.CostEstimate(flops=0, bytes_accessed=6 * math.prod(shape), transcendentals=0),
    )(order_of_pieces(), *pieces)


def join_kernel(at, *refs):
    outs = refs[-2:]
    for n in range(2):

        @pl.when(pl.program_id(0) == n)
        def _():
            for m, out in enumerate(outs):
                out[...] = refs[2 * m + n][...]


def join_rows(first, second):
    rows, width = first[0].shape
    me = lax.axis_index("tp")
    whole = pl.BlockSpec((rows, width), lambda n, at: (0, 0))
    return pl.pallas_call(
        join_kernel,
        grid_spec=pltpu.PrefetchScalarGridSpec(
            num_scalar_prefetch=1,
            grid=(2,),
            in_specs=[whole] * 4,
            out_specs=[pl.BlockSpec((rows, width), lambda n, at: (at[n], 0))] * 2,
        ),
        out_shape=[jax.ShapeDtypeStruct((2 * rows, width), first[0].dtype)] * 2,
        compiler_params=pltpu.CompilerParams(vmem_limit_bytes=VMEM_LIMIT),
        cost_estimate=pl.CostEstimate(flops=0, bytes_accessed=16 * rows * width, transcendentals=0),
    )(jnp.stack([me, 1 - me]), *first, *second)


def place_gate_up_kernel(at, *refs):
    pieces, (gate, up) = refs[:-2], refs[-2:]
    count = gate.shape[1]
    for n, piece in enumerate(pieces):

        @pl.when(pl.program_id(0) == n)
        def _():
            gate[...] = wide(piece[:, :count])
            up[...] = wide(piece[:, count:])


def place_gate_up(pieces):
    rows, cols = pieces[0].shape
    count, whole = cols // 2, cols // 2 * len(pieces)
    side = pl.BlockSpec((rows, count), lambda n, at: (0, at[n]))
    return pl.pallas_call(
        place_gate_up_kernel,
        grid_spec=pltpu.PrefetchScalarGridSpec(
            num_scalar_prefetch=1,
            grid=(len(pieces),),
            in_specs=[pl.BlockSpec((rows, cols), lambda n, at: (0, 0))] * len(pieces),
            out_specs=[side] * 2,
        ),
        out_shape=[jax.ShapeDtypeStruct((rows, whole), jnp.float32)] * 2,
        compiler_params=pltpu.CompilerParams(vmem_limit_bytes=VMEM_LIMIT),
        cost_estimate=pl.CostEstimate(flops=0, bytes_accessed=12 * rows * whole, transcendentals=0),
    )(order_of_pieces(), *pieces)


def place_attention_kernel(at, *refs):
    pieces, outs = refs[:-4], refs[-4:]
    count = outs[0].shape[1]
    pairs = count // PAIR
    for n, piece in enumerate(pieces):

        @pl.when(pl.program_id(0) == n)
        def _():
            for p in range(pairs):
                for m in range(3):
                    outs[m][:, p * PAIR : (p + 1) * PAIR] = wide(piece[:, (3 * p + m) * PAIR : (3 * p + m + 1) * PAIR])
            outs[3][...] = wide(piece[:, 3 * count :]).T


def place_attention(pieces):
    depth, count = pieces[0].shape[0], pieces[0].shape[1] // 4
    whole = len(pieces) * count
    side = pl.BlockSpec((depth, count), lambda n, at: (0, at[n]))
    return pl.pallas_call(
        place_attention_kernel,
        grid_spec=pltpu.PrefetchScalarGridSpec(
            num_scalar_prefetch=1,
            grid=(len(pieces),),
            in_specs=[pl.BlockSpec(pieces[0].shape, lambda n, at: (0, 0))] * len(pieces),
            out_specs=[side] * 3 + [pl.BlockSpec((count, depth), lambda n, at: (at[n], 0))],
        ),
        out_shape=[jax.ShapeDtypeStruct((depth, whole), jnp.float32)] * 3 + [jax.ShapeDtypeStruct((whole, depth), jnp.float32)],
        compiler_params=pltpu.CompilerParams(vmem_limit_bytes=VMEM_LIMIT),
        cost_estimate=pl.CostEstimate(flops=0, bytes_accessed=24 * depth * whole, transcendentals=0),
    )(order_of_pieces(), *pieces)


def local(
    hidden_in,
    out_grad,
    segment_ids,
    attn_gain,
    w_query,
    w_key,
    w_value,
    w_out,
    mlp_gain,
    w_gate,
    w_up,
    w_down,
):
    group = lax.axis_size("ctx")
    me = lax.axis_index("ctx")
    local_rows = hidden_in.shape[1]
    tokens = local_rows * group
    head_cols = w_query.shape[1] // group
    ff_cols = w_gate.shape[1] // group

    def gather(weight, axis):
        return lax.all_gather(weight, "fsdp", axis=axis, tiled=True)

    def settle(part, axis):
        return lax.psum_scatter(part, "fsdp", scatter_dimension=axis, tiled=True)

    at = me[None]
    w_attn = gather(take_attention(at, w_query, w_key, w_value, w_out, head_cols), 0)
    qkv_cols = 3 * head_cols
    w_qkv, w_out_t = w_attn[:, :qkv_cols], w_attn[:, qkv_cols:]
    own_gate_up, own_down = take_hidden(at, w_gate, w_up, w_down, ff_cols)
    full_gate_up = gather(own_gate_up, 0)
    full_down = gather(own_down, 1)

    kernels = fits_kernels()
    if kernels:
        attn_in, branch_cot, segments, gains = start_exchange(hidden_in[0], out_grad[0], segment_ids[0], attn_gain, mlp_gain)
        gain_one, gain_two = gains[0], gains[1]
    else:
        gains = wide(gather(jnp.stack([attn_gain, mlp_gain]), 1))
        gain_one, gain_two = gains[0], gains[1]
        rows_in = wide(hidden_in[0])
        r1 = lax.rsqrt(jnp.mean(rows_in * rows_in, axis=-1, keepdims=True) + EPS)
        attn_in = gather_rows(low(rows_in * r1 * gain_one), "ctx")
        segments = gather_rows(segment_ids[0], "ctx")
        branch_cot = gather_rows(out_grad[0], "ctx")

    firsts = jnp.stack([(me ^ at) * local_rows for at in offsets(group)])
    positions = (firsts[:, None] + jnp.arange(local_rows, dtype=jnp.int32)[None, :]).reshape(tokens)
    exponents = jnp.arange(0, HEAD_DIM, 2).astype(jnp.float32) / HEAD_DIM
    inverse = jnp.float32(ROPE_BASE) ** (-exponents)
    angles = positions.astype(jnp.float32)[:, None] * inverse[None, :]
    cos = jnp.tile(jnp.cos(angles), (1, 4))
    sin = jnp.tile(jnp.sin(angles), (1, 4))
    info = jnp.stack([positions[::BLOCK], segments[::BLOCK], segments[BLOCK - 1 :: BLOCK]])
    seg_col, seg_row = segments[:, None], segments[None, :]

    qkv = product(attn_in, w_qkv)
    rot, mixed, mixed_wide, lse = attention_forward(info, qkv, cos, sin, seg_col, seg_row)

    own_in = wide(own_part(hidden_in[0]))
    if kernels:
        mlp_in, resid = forward_mid(mixed, w_attn, hidden_in[0], gain_two)
    else:
        part = scatter_both(lambda lo, hi: contract_cols(mixed[lo:hi], w_out_t), tokens)
        resid = own_in + part
        r2 = lax.rsqrt(jnp.mean(resid * resid, axis=-1, keepdims=True) + EPS)
        mlp_in = gather_rows(join_tp(low(resid * r2 * gain_two)), "ctx")
    acts = product(mlp_in, full_gate_up)
    gate_act, up_act = acts[:, :ff_cols], acts[:, ff_cols:]
    sigmoid = jax.nn.sigmoid(gate_act)
    hidden = low(gate_act * sigmoid * up_act)
    gate_slope = low(up_act * sigmoid * (1.0 + gate_act * (1.0 - sigmoid)))
    up_slope = low(gate_act * sigmoid)
    hidden, gate_slope, up_slope = lax.optimization_barrier((hidden, gate_slope, up_slope))
    down_part = low(contract_rows(hidden, branch_cot))
    down_part, full_down, branch_cot = lax.optimization_barrier((down_part, full_down, branch_cot))
    down_own = settle(down_part, 1)

    hidden_cot = hidden_cots(branch_cot, full_down, gate_slope, up_slope)
    gate_up_part = low(contract_rows(mlp_in, hidden_cot))
    gate_up_own = settle(gate_up_part, 0)
    if kernels:
        hidden_cot, gate_up_part = lax.optimization_barrier((hidden_cot, gate_up_part))
        attn_cot, resid_cot, gain_two_part = backward_mid(hidden_cot, full_gate_up, resid, out_grad[0], gain_two)
    else:
        mlp_in_cot = scatter_both(lambda lo, hi: contract_cols(hidden_cot[lo:hi], full_gate_up), tokens)
        back, terms = norm_back(resid, r2, gain_two, mlp_in_cot)
        gain_two_part = jnp.sum(terms, axis=0, keepdims=True)
        resid_cot = wide(own_part(out_grad[0])) + back
        attn_cot = gather_rows(join_tp(low(resid_cot)), "ctx")
    mixed_cot = low(product(attn_cot, w_out_t))
    out_part = low(contract_rows(attn_cot, mixed))
    mixed_cot, out_part, down_own = lax.optimization_barrier((mixed_cot, out_part, down_own))
    down_pieces = first_swaps(down_own)
    if kernels:
        cots, output = attention_output(rot, cos, sin, seg_col, seg_row, mixed_cot, mixed_wide, lse, hidden, full_down, resid)
        other_output = swap(output, "tp", 1)
    else:
        cots = attention_backward(info, rot, cos, sin, seg_col, seg_row, mixed_cot, mixed_wide, lse)
    cots, *down_pieces = lax.optimization_barrier((cots, *down_pieces))
    qkv_part = low(contract_rows(attn_in, cots))
    attn_part = jnp.concatenate([qkv_part, out_part], axis=1)
    attn_own = settle(attn_part, 0)
    if kernels:
        cots, attn_part, gate_up_own = lax.optimization_barrier((cots, attn_part, gate_up_own))
        gate_up_pieces = first_swaps(gate_up_own)
        input_grad, gain_one_part = input_exchange(cots, w_attn, resid_cot, hidden_in[0], gain_one)
        gain_sums = gain_sum(gain_one_part, gain_two_part)
        input_grad, gain_sums, *gate_up_pieces = lax.optimization_barrier((input_grad, gain_sums, *gate_up_pieces))
        other_input = swap(input_grad, "tp", 1)
        output, input_grad = join_rows((output, other_output), (input_grad, other_input))
    else:
        gate_up_pieces = first_swaps(gate_up_own)
        out_sum = scatter_both(lambda lo, hi: product(hidden[lo:hi], full_down), tokens)
        output = join_tp(low(resid + out_sum))
        attn_in_cot = scatter_both(lambda lo, hi: contract_cols(cots[lo:hi], w_qkv), tokens)
        back, terms = norm_back(own_in, own_part(r1), gain_one, attn_in_cot)
        input_grad = join_tp(low(resid_cot + back))
        gain_sums = lax.psum(jnp.concatenate([jnp.sum(terms, axis=0, keepdims=True), gain_two_part]), ("fsdp", "ctx", "tp"))
    attn_pieces = first_swaps(attn_own)
    down_pieces = last_swap(down_pieces)
    down_grad = place_pieces(down_pieces, 0)
    gate_up_pieces = last_swap(gate_up_pieces)
    gate_grad, up_grad = place_gate_up(gate_up_pieces)
    down_grad, gate_grad, up_grad, *attn_pieces = lax.optimization_barrier((down_grad, gate_grad, up_grad, *attn_pieces))
    query_grad, key_grad, value_grad, out_proj_grad = place_attention(last_swap(attn_pieces))

    gain_sums = lax.dynamic_slice_in_dim(gain_sums, lax.axis_index("fsdp") * attn_gain.shape[0], attn_gain.shape[0], 1)
    return (
        output[None],
        input_grad[None],
        gain_sums[0],
        query_grad,
        key_grad,
        value_grad,
        out_proj_grad,
        gain_sums[1],
        gate_grad,
        up_grad,
        down_grad,
    )


def solution(mesh):
    weight, gain = P("fsdp", "tp"), P("fsdp")
    rows = P("fsdp", "ctx", None)
    in_specs = (rows, rows, P("fsdp", "ctx"), gain, weight, weight, weight, P("tp", "fsdp"), gain, weight, weight, P("tp", "fsdp"))
    out_specs = (rows, rows, gain, weight, weight, weight, P("tp", "fsdp"), gain, weight, weight, P("tp", "fsdp"))
    return jax.shard_map(local, mesh=mesh, in_specs=in_specs, out_specs=out_specs, check_vma=False)
```
